32 devices in a mesh: dp: 1 (over z), heads: 4 (over y), ctx: 8 (over x, core).
Axes of the slice: x: 4, y: 4, z: 1, core: 2. Of those that a mesh axis runs over, the one named last changes fastest.
The devices are a block of a 4x4x8 slice.
Arguments:
- hidden: bfloat16 [512, 5120], P(('dp', 'ctx'))
- w_query: bfloat16 [5120, 4096], P(None, 'heads')
- w_key: bfloat16 [5120, 1024], P(None, 'heads')
- w_value: bfloat16 [5120, 1024], P(None, 'heads')
- w_out: bfloat16 [4096, 5120], P('heads')
- prefix_k: bfloat16 [8192, 8, 128], P(('dp', 'ctx'), 'heads')
- prefix_v: bfloat16 [8192, 8, 128], P(('dp', 'ctx'), 'heads')
- suffix_k: bfloat16 [512, 512, 8, 128], P(('dp', 'ctx'), None, 'heads')
- suffix_v: bfloat16 [512, 512, 8, 128], P(('dp', 'ctx'), None, 'heads')
- seq_lens: int32 [512], P(('dp', 'ctx'))
Outputs:
- output: bfloat16 [512, 5120], P(('dp', 'ctx'))
All inputs are finite; a program needn't handle non-finite values.
Results may differ from the reference program's by a relative error of at most 0.00452898.
Values are sent between devices in bfloat16 or wider.
A program may use at most 768 MiB of HBM per device.

```python
import math
import jax
import jax.numpy as jnp
from jax import lax

D = 5120
HEADS = 32
KV_HEADS = 8
HEAD = 128
SEQS = 512
PREFIX = 8192
SUFFIX = 512
SEG_LEN = 1024


def draw_lens(lens_key):
    raw_lens = jax.random.randint(lens_key, (SEQS,), 0, SUFFIX, jnp.int32)
    row_ids = jnp.arange(SEQS)
    return jnp.where(row_ids == 0, SUFFIX - 1, jnp.where(row_ids == 1, 0, raw_lens)).astype(jnp.int32)


def setup_inputs(seed: int = 0, part: int = 0) -> dict:
    base_key = jax.random.key(seed)
    shared = jax.random.split(base_key, 4)
    own_keys = jax.random.split(jax.random.fold_in(base_key, part), 8)
    q_width = HEADS * HEAD
    kv_width = KV_HEADS * HEAD
    log_mass = math.log(PREFIX) + 4.0
    n_seg = PREFIX // SEG_LEN
    w_query = jax.random.normal(shared[0], (D, q_width), jnp.float32) * D ** -0.5
    w_key = jax.random.normal(shared[1], (D, kv_width), jnp.float32) * (log_mass * D ** -0.5)
    w_value = jax.random.normal(shared[2], (D, kv_width), jnp.float32) * D ** -0.5
    w_out = jax.random.normal(shared[3], (q_width, D), jnp.float32) * q_width ** -0.5
    hidden = jax.random.normal(own_keys[0], (SEQS, D), jnp.float32)
    seg_dir = jax.random.normal(own_keys[1], (n_seg, 1, KV_HEADS, HEAD), jnp.float32)
    key_noise = jax.random.normal(own_keys[2], (n_seg, SEG_LEN, KV_HEADS, HEAD), jnp.float32)
    seg_val = jax.random.normal(own_keys[3], (n_seg, 1, KV_HEADS, HEAD), jnp.float32)
    val_noise = jax.random.normal(own_keys[4], (n_seg, SEG_LEN, KV_HEADS, HEAD), jnp.float32)
    prefix_k = (key_noise + 2.0 * seg_dir).reshape(PREFIX, KV_HEADS, HEAD)
    prefix_v = (val_noise + seg_val).reshape(PREFIX, KV_HEADS, HEAD)
    suffix_k = jax.random.normal(own_keys[5], (SEQS, SUFFIX, KV_HEADS, HEAD), jnp.float32) * (log_mass / 2.5)
    suffix_v = jax.random.normal(own_keys[6], (SEQS, SUFFIX, KV_HEADS, HEAD), jnp.float32)
    seq_lens = draw_lens(own_keys[7])
    return {'hidden': hidden.astype(jnp.bfloat16), 'w_query': w_query.astype(jnp.bfloat16), 'w_key': w_key.astype(jnp.bfloat16), 'w_value': w_value.astype(jnp.bfloat16), 'w_out': w_out.astype(jnp.bfloat16), 'prefix_k': prefix_k.astype(jnp.bfloat16), 'prefix_v': prefix_v.astype(jnp.bfloat16), 'suffix_k': suffix_k.astype(jnp.bfloat16), 'suffix_v': suffix_v.astype(jnp.bfloat16), 'seq_lens': seq_lens}


def reference(hidden, w_query, w_key, w_value, w_out, prefix_k, prefix_v, suffix_k, suffix_v, seq_lens):
    q_group = HEADS // KV_HEADS
    score_scale = HEAD ** -0.5
    queries = jnp.dot(hidden, w_query, preferred_element_type=jnp.float32).astype(jnp.bfloat16).reshape(SEQS, KV_HEADS, q_group, HEAD)
    key_new = jnp.dot(hidden, w_key, preferred_element_type=jnp.float32).astype(jnp.bfloat16).reshape(SEQS, KV_HEADS, HEAD)
    val_new = jnp.dot(hidden, w_value, preferred_element_type=jnp.float32).astype(jnp.bfloat16).reshape(SEQS, KV_HEADS, HEAD)
    pre_k = prefix_k.astype(jnp.float32)
    pre_v = prefix_v.astype(jnp.float32)
    slot_ids = jnp.arange(SUFFIX)

    def one_seq(seq_item):
        q_row, k_row, v_row, cache_k, cache_v, length = seq_item
        at_slot = (slot_ids == length)[:, None, None]
        suf_keys = jnp.where(at_slot, k_row[None], cache_k).astype(jnp.float32)
        suf_vals = jnp.where(at_slot, v_row[None], cache_v).astype(jnp.float32)
        q_float = q_row.astype(jnp.float32)
        score_pre = jnp.einsum('kgd,pkd->kgp', q_float, pre_k) * score_scale
        score_suf = jnp.einsum('kgd,skd->kgs', q_float, suf_keys) * score_scale
        score_suf = jnp.where(slot_ids <= length, score_suf, -jnp.inf)
        row_max = jnp.maximum(jnp.max(score_pre, axis=-1), jnp.max(score_suf, axis=-1))[..., None]
        exp_pre = jnp.exp(score_pre - row_max)
        exp_suf = jnp.exp(score_suf - row_max)
        denominator = jnp.sum(exp_pre, axis=-1) + jnp.sum(exp_suf, axis=-1)
        numerator = jnp.einsum('kgp,pkd->kgd', exp_pre.astype(jnp.bfloat16).astype(jnp.float32), pre_v) + jnp.einsum('kgs,skd->kgd', exp_suf.astype(jnp.bfloat16).astype(jnp.float32), suf_vals)
        return (numerator / denominator[..., None]).astype(jnp.bfloat16).reshape(HEADS * HEAD)

    attended = lax.map(one_seq, (queries, key_new, val_new, suffix_k, suffix_v, seq_lens))
    mixed_out = jnp.dot(attended, w_out, preferred_element_type=jnp.float32)
    return (hidden.astype(jnp.float32) + mixed_out).astype(jnp.bfloat16)
```

```python
import functools
import math
import jax
import jax.numpy as jnp
from jax import lax
from jax.experimental import pallas as pl
from jax.experimental.pallas import tpu as pltpu
from jax.sharding import PartitionSpec as P

MESH = pl.DeviceIdType.MESH
F32 = jnp.float32
BF16 = jnp.bfloat16
LOW = -3.0e38
SEQ_CHUNK = 8
RING = 5
POS_CHUNK = 512


def dot_nt(a, b):
    return lax.dot_general(a, b, (((1,), (1,)), ((), ())), preferred_element_type=F32)


def dot_nn(a, b):
    return lax.dot_general(a, b, (((1,), (0,)), ((), ())), preferred_element_type=F32)


def pack_stats(row_max, row_sum):
    rows = row_max.shape[0]
    lane = lax.broadcasted_iota(jnp.int32, (rows, 128), 1)
    both = jnp.where(lane == 0, row_max, jnp.where(lane == 1, row_sum, 0.0))
    return jnp.transpose(both)[:8]


def unpack_stats(packed):
    rows = packed.shape[1]
    both = jnp.transpose(jnp.concatenate([packed, jnp.zeros((120, rows), F32)], axis=0))
    return both[:, 0:1], both[:, 1:2]


def merge(one, two):
    (num_a, max_a, sum_a), (num_b, max_b, sum_b) = one, two
    top = jnp.maximum(max_a, max_b)
    fac_a, fac_b = jnp.exp2(max_a - top), jnp.exp2(max_b - top)
    return num_a * fac_a + num_b * fac_b, top, sum_a * fac_a + sum_b * fac_b


def kernel(dims, hid_h, wq_h, wk_h, wv_h, wo_h, pk_h, pv_h, sk_h, sv_h, lens, out_h,
           hid, wq, wk, wv, wo, raw, flat, kpre, vpre, qg, q8, knew, vnew,
           ring_k, ring_v, scores, own_num, own_max, own_sum, hold_num, hold_max, hold_sum,
           so8, sm8, sl8, xs_num, xs_st, xr_num, xr_st, att, ys, yr, yblk, ygat,
           s_hid, s_wq, s_wkv, s_wo, s_raw, s_rawsend, s_rawrecv, s_ring,
           s_qs, s_qr, s_xs, s_xr, s_xst, s_xrt, s_ys, s_yr, s_gs, s_gr, s_out):
    n_ctx, n_y, kv_n, grp = dims
    rows = hid.shape[0]
    width = hid.shape[1]
    head = kpre.shape[-1]
    per_kv = grp * head
    heads = kv_n * grp
    local_pos = raw.shape[2] // kv_n
    scale = head ** -0.5 * math.log2(math.e)
    blk = width // n_y
    half = blk // 2

    ctx = lax.axis_index('ctx')
    ypos = lax.axis_index('heads')
    right = {'ctx': lax.rem(ctx + 2, n_ctx)}
    left = {'ctx': lax.rem(ctx + n_ctx - 2, n_ctx)}
    partner = {'ctx': ctx + 1 - 2 * lax.rem(ctx, 2)}
    up = {'heads': lax.rem(ypos + 1, n_y)}
    down = {'heads': lax.rem(ypos + n_y - 1, n_y)}

    def remote(src, dst, send, recv, where):
        return pltpu.make_async_remote_copy(src_ref=src, dst_ref=dst, send_sem=send, recv_sem=recv,
                                            device_id=where, device_id_type=MESH)

    c_hid = pltpu.make_async_copy(hid_h, hid, s_hid)
    c_hid.start()
    n_q = heads // 2
    c_wq = [pltpu.make_async_copy(wq_h.at[:, pl.ds(i * 2 * head, 2 * head)], wq.at[i], s_wq.at[i]) for i in range(n_q)]
    c_raw = [pltpu.make_async_copy(src, raw.at[0, i], s_raw.at[i]) for i, src in enumerate((pk_h, pv_h))]
    c_wq[0].start()
    for c in c_raw:
        c.start()
    for c in c_wq[1:]:
        c.start()

    barrier = pltpu.get_barrier_semaphore()
    for where in (partner, left, right, up, down):
        pl.semaphore_signal(barrier, inc=1, device_id=where, device_id_type=MESH)
    pl.semaphore_wait(barrier, 5)

    c_swap = [remote(src, raw.at[1, i], s_rawsend.at[i], s_rawrecv.at[i], partner) for i, src in enumerate((pk_h, pv_h))]
    for c in c_swap:
        c.start()
    c_wkv = [pltpu.make_async_copy(src, dst, s_wkv.at[i]) for i, (src, dst) in enumerate(((wk_h, wk), (wv_h, wv)))]
    for c in c_wkv:
        c.start()

    def deinterleave(which):
        for i, dst in enumerate((kpre, vpre)):
            flat[...] = raw[which, i].astype(F32)
            for kv in range(kv_n):
                dst[kv, pl.ds(which * local_pos, local_pos), :] = flat[pl.ds(kv, local_pos, stride=kv_n), :].astype(BF16)

    def ring_copies(chunk, slot):
        seqs = pl.ds(chunk * SEQ_CHUNK, SEQ_CHUNK)
        return (pltpu.make_async_copy(sk_h.at[seqs], ring_k.at[slot], s_ring.at[slot, 0]),
                pltpu.make_async_copy(sv_h.at[seqs], ring_v.at[slot], s_ring.at[slot, 1]))

    n_chunks = rows // SEQ_CHUNK

    for c in c_raw:
        c.wait()
    deinterleave(0)

    c_hid.wait()
    q_copies = []
    for kv in range(kv_n):
        for j in range(grp // 2):
            i = kv * (grp // 2) + j
            c_wq[i].wait()
            part = dot_nn(hid[...], wq[i]).astype(BF16)
            qg[0, kv, :, pl.ds(j * 2 * head, 2 * head)] = part
            for g in range(2):
                h = kv * grp + j * 2 + g
                q8[pl.ds(h, rows, stride=heads), :] = part[:, g * head:(g + 1) * head].astype(F32)
        to_right = remote(qg.at[0, kv], qg.at[1, kv], s_qs.at[0, kv], s_qr.at[1, kv], right)
        to_left = remote(qg.at[0, kv], qg.at[2, kv], s_qs.at[1, kv], s_qr.at[2, kv], left)
        to_right.start()
        to_left.start()
        q_copies.append((to_right, to_left))
        if kv == 0:
            for chunk in range(RING):
                for c in ring_copies(chunk, chunk):
                    c.start()
    c_wo = []
    for r in range(2 * n_y):
        dest = lax.rem(ypos + r // 2, n_y)
        col = pl.multiple_of(dest * blk + (r % 2) * half, 128)
        c_wo.append(pltpu.make_async_copy(wo_h.at[:, pl.ds(col, half)], wo.at[r], s_wo.at[r]))
    for c in c_wo:
        c.start()

    for c in c_wkv:
        c.wait()
    knew[...] = dot_nn(hid[...], wk[...]).astype(BF16).astype(F32)
    vnew[...] = dot_nn(hid[...], wv[...]).astype(BF16).astype(F32)

    for c in c_swap:
        c.wait()
    deinterleave(1)

    n_pos = kpre.shape[1]

    def prefix_part(slot, kv):
        queries = jnp.concatenate([qg[slot, kv, :, pl.ds(g * head, head)] for g in range(grp)], axis=0)
        run = None
        for c in range(n_pos // POS_CHUNK):
            at = pl.ds(c * POS_CHUNK, POS_CHUNK)
            s = dot_nt(queries, kpre[kv, at, :])
            scores[:, at] = s
            for t in range(POS_CHUNK // 128):
                piece = s[:, t * 128:(t + 1) * 128]
                run = piece if run is None else jnp.maximum(run, piece)
        row_max = jnp.max(run, axis=1, keepdims=True) * scale
        wide_max = jnp.broadcast_to(row_max, (grp * rows, 128))
        wide_max = jnp.concatenate([wide_max] * (POS_CHUNK // 128), axis=1)
        total, num = None, None
        for c in range(n_pos // POS_CHUNK):
            at = pl.ds(c * POS_CHUNK, POS_CHUNK)
            p = jnp.exp2(scores[:, at] * scale - wide_max)
            for t in range(POS_CHUNK // 128):
                piece = p[:, t * 128:(t + 1) * 128]
                total = piece if total is None else total + piece
            term = dot_nn(p.astype(BF16), vpre[kv, at, :])
            num = term if num is None else num + term
        return num, row_max, jnp.sum(total, axis=1, keepdims=True)

    def post(state, i, where):
        xs_num[i] = state[0]
        xs_st[i] = pack_stats(state[1], state[2])
        out = (remote(xs_num.at[i], xr_num.at[i], s_xs.at[i], s_xr.at[i], where),
               remote(xs_st.at[i], xr_st.at[i], s_xst.at[i], s_xrt.at[i], where))
        for c in out:
            c.start()
        return out

    def received(i, where):
        for c in (remote(xs_num.at[i], xr_num.at[i], s_xs.at[i], s_xr.at[i], where),
                  remote(xs_st.at[i], xr_st.at[i], s_xst.at[i], s_xrt.at[i], where)):
            c.wait_recv()
        return (xr_num[i],) + unpack_stats(xr_st[i])

    def suffix_chunks(first, last):
        lane = lax.broadcasted_iota(jnp.int32, (heads, ring_k.shape[2]), 1)
        line = lax.broadcasted_iota(jnp.int32, (heads, ring_k.shape[2]), 0)
        mine = lax.rem(lane, kv_n) == line // grp
        place = jnp.where(mine, lane // kv_n, ring_k.shape[2])

        @pl.loop(first, last)
        def _(chunk):
            slot = lax.rem(chunk, RING)
            for c in ring_copies(chunk, slot):
                c.wait()
            for i in range(SEQ_CHUNK):
                b = chunk * SEQ_CHUNK + i
                at = pl.ds(pl.multiple_of(b * heads, heads), heads)
                qb = q8[at, :].astype(BF16)
                s = dot_nt(qb, ring_k[slot, i]) * scale
                s = jnp.where(place < lens[b], s, -jnp.inf)
                m = jnp.maximum(jnp.max(s, axis=1, keepdims=True), LOW)
                p = jnp.exp2(s - m)
                so8[at, :] = dot_nn(p.astype(BF16), ring_v[slot, i])
                sm8[at, :] = jnp.broadcast_to(m, (heads, head))
                sl8[at, :] = jnp.broadcast_to(jnp.sum(p, axis=1, keepdims=True), (heads, head))

            @pl.when(chunk + RING < n_chunks)
            def _():
                for c in ring_copies(chunk + RING, slot):
                    c.start()

    def keep(refs, i, state):
        for ref, val in zip(refs, state):
            ref[i] = val if val.shape == ref.shape[1:] else jnp.broadcast_to(val, ref.shape[1:])

    def kept(refs, i):
        return refs[0][i], refs[1][i][:, 0:1], refs[2][i][:, 0:1]

    own = (own_num, own_max, own_sum)
    hold = (hold_num, hold_max, hold_sum)

    keep(own, 0, prefix_part(0, 0))
    q_copies[0][0].wait_recv()
    fwd_right = remote(qg.at[1, 0], qg.at[3, 0], s_qs.at[2, 0], s_qr.at[3, 0], right)
    fwd_right.start()
    keep(own, 1, prefix_part(0, 1))
    q_copies[1][1].wait_recv()
    fwd_left = remote(qg.at[2, 1], qg.at[3, 1], s_qs.at[2, 1], s_qr.at[3, 1], left)
    fwd_left.start()

    sent = []
    q_copies[1][0].wait_recv()
    q_copies[0][1].wait_recv()
    sent += post(prefix_part(2, 1), 0, right)
    sent += post(prefix_part(1, 0), 1, left)
    fwd_right.wait_recv()
    sent += post(prefix_part(3, 0), 2, right)
    fwd_left.wait_recv()
    sent += post(prefix_part(3, 1), 3, left)
    keep(hold, 0, prefix_part(2, 0))
    keep(hold, 1, prefix_part(1, 1))
    suffix_chunks(0, 2)
    sent += post(merge(received(2, right), kept(hold, 0)), 4, right)
    sent += post(merge(received(3, left), kept(hold, 1)), 5, left)
    suffix_chunks(2, n_chunks)

    for kv in range(kv_n):
        states = [kept(own, kv)]
        if kv == 0:
            states += [received(1, left), received(4, right)]
        else:
            states += [received(0, right), received(5, left)]
        state = functools.reduce(merge, states)
        for g in range(grp):
            h = kv * grp + g
            at = slice(g * rows, (g + 1) * rows)
            every = pl.ds(h, rows, stride=heads)
            qh = q8[every, :]
            kn = knew[:, kv * head:(kv + 1) * head]
            vn = vnew[:, kv * head:(kv + 1) * head]
            s_new = jnp.sum(qh * kn, axis=1, keepdims=True) * scale
            full = merge((state[0][at], state[1][at], state[2][at]), (so8[every, :], sm8[every, :], sl8[every, :]))
            full = merge(full, (vn, s_new, jnp.ones_like(s_new)))
            att[:, h * head:(h + 1) * head] = (full[0] / full[2]).astype(BF16)

    ysent = []

    def y_part(r):
        c_wo[r].wait()
        return dot_nn(att[...], wo[r])

    def y_copy(i, where):
        return remote(ys.at[i], yr.at[i], s_ys.at[i], s_yr.at[i], where)

    def y_post(val, i, where):
        ys[i] = val
        c = y_copy(i, where)
        c.start()
        ysent.append(c)

    far, near_up, near_down = 2 * (n_y // 2), 2, 2 * (n_y - 1)
    y_post(y_part(far), 0, up)
    y_post(y_part(far + 1), 1, down)
    y_post(y_part(near_up + 1), 2, up)
    y_post(y_part(near_down), 3, down)
    part_up = y_part(near_up)
    part_down = y_part(near_down + 1)
    y_copy(0, up).wait_recv()
    y_post(part_up + yr[0], 4, up)
    y_copy(1, down).wait_recv()
    y_post(part_down + yr[1], 5, down)
    low, high = y_part(0), y_part(1)
    me_col = pl.multiple_of(ypos * blk, 128)
    y_copy(3, down).wait_recv()
    low = low + yr[3]
    y_copy(2, up).wait_recv()
    high = high + yr[2]
    y_copy(4, up).wait_recv()
    low = low + yr[4] + hid[:, pl.ds(me_col, half)].astype(F32)
    yblk[0] = low.astype(BF16)
    y_copy(5, down).wait_recv()
    high = high + yr[5] + hid[:, pl.ds(pl.multiple_of(me_col + half, 128), half)].astype(F32)
    yblk[1] = high.astype(BF16)

    gsend = []

    def g_copy(src, slot, part, sem, where):
        c = remote(src, ygat.at[slot, part], s_gs.at[sem], s_gr.at[slot, part], where)
        gsend.append(c)
        return c

    g_up = [g_copy(yblk.at[p], 0, p, p, up) for p in range(2)]
    g_down = [g_copy(yblk.at[p], 1, p, 2 + p, down) for p in range(2)]
    for p in range(2):
        g_up[p].start()
        g_down[1 - p].start()

    outs = []

    def put(src, dest, part):
        col = pl.multiple_of(dest * blk + part * half, 128)
        c = pltpu.make_async_copy(src, out_h.at[:, pl.ds(col, half)], s_out.at[len(outs)])
        c.start()
        outs.append(c)

    put(yblk.at[0], ypos, 0)
    put(yblk.at[1], ypos, 1)
    g_up[0].wait_recv()
    f_up = g_copy(ygat.at[0, 0], 2, 0, 4, up)
    f_up.start()
    g_down[1].wait_recv()
    f_down = g_copy(ygat.at[1, 1], 2, 1, 5, down)
    f_down.start()
    below, above = lax.rem(ypos + n_y - 1, n_y), lax.rem(ypos + 1, n_y)
    put(ygat.at[0, 0], below, 0)
    put(ygat.at[1, 1], above, 1)
    g_up[1].wait_recv()
    put(ygat.at[0, 1], below, 1)
    g_down[0].wait_recv()
    put(ygat.at[1, 0], above, 0)
    opposite = lax.rem(ypos + n_y // 2, n_y)
    f_up.wait_recv()
    put(ygat.at[2, 0], opposite, 0)
    f_down.wait_recv()
    put(ygat.at[2, 1], opposite, 1)

    for pair in q_copies:
        for c in pair:
            c.wait_send()
    for c in [fwd_right, fwd_left] + sent + ysent + gsend:
        c.wait_send()
    for c in outs:
        c.wait()


def solution(mesh):
    n_ctx, n_y = mesh.shape['ctx'], mesh.shape['heads']
    row_spec = P(('dp', 'ctx'), None)
    col_spec = P(None, 'heads')
    pre_spec = P(('dp', 'ctx'), 'heads', None)
    suf_spec = P(('dp', 'ctx'), None, 'heads', None)

    def local_step(hidden, w_query, w_key, w_value, w_out, prefix_k, prefix_v, suffix_k, suffix_v, seq_lens):
        rows, width = hidden.shape
        pos, kv_n, head = prefix_k.shape
        slots = suffix_k.shape[1]
        grp = w_query.shape[1] // (kv_n * head)
        heads = kv_n * grp
        blk = width // n_y
        stack = grp * rows
        dma = pltpu.SemaphoreType.DMA
        scratch = dict(
            hid=pltpu.VMEM((rows, width), BF16),
            wq=pltpu.VMEM((heads // 2, width, 2 * head), BF16),
            wk=pltpu.VMEM((width, kv_n * head), BF16),
            wv=pltpu.VMEM((width, kv_n * head), BF16),
            wo=pltpu.VMEM((2 * n_y, heads * head, blk // 2), BF16),
            raw=pltpu.VMEM((2, 2, pos * kv_n, head), BF16),
            flat=pltpu.VMEM((pos * kv_n, head), F32),
            kpre=pltpu.VMEM((kv_n, 2 * pos, head), BF16),
            vpre=pltpu.VMEM((kv_n, 2 * pos, head), BF16),
            qg=pltpu.VMEM((4, kv_n, rows, grp * head), BF16),
            q8=pltpu.VMEM((rows * heads, head), F32),
            knew=pltpu.VMEM((rows, kv_n * head), F32),
            vnew=pltpu.VMEM((rows, kv_n * head), F32),
            ring_k=pltpu.VMEM((RING, SEQ_CHUNK, slots * kv_n, head), BF16),
            ring_v=pltpu.VMEM((RING, SEQ_CHUNK, slots * kv_n, head), BF16),
            scores=pltpu.VMEM((stack, 2 * pos), F32),
            own_num=pltpu.VMEM((kv_n, stack, head), F32),
            own_max=pltpu.VMEM((kv_n, stack, 128), F32),
            own_sum=pltpu.VMEM((kv_n, stack, 128), F32),
            hold_num=pltpu.VMEM((2, stack, head), F32),
            hold_max=pltpu.VMEM((2, stack, 128), F32),
            hold_sum=pltpu.VMEM((2, stack, 128), F32),
            so8=pltpu.VMEM((rows * heads, head), F32),
            sm8=pltpu.VMEM((rows * heads, head), F32),
            sl8=pltpu.VMEM((rows * heads, head), F32),
            xs_num=pltpu.VMEM((6, stack, head), F32),
            xs_st=pltpu.VMEM((6, 8, stack), F32),
            xr_num=pltpu.VMEM((6, stack, head), F32),
            xr_st=pltpu.VMEM((6, 8, stack), F32),
            att=pltpu.VMEM((rows, heads * head), BF16),
            ys=pltpu.VMEM((6, rows, blk // 2), F32),
            yr=pltpu.VMEM((6, rows, blk // 2), F32),
            yblk=pltpu.VMEM((2, rows, blk // 2), BF16),
            ygat=pltpu.VMEM((3, 2, rows, blk // 2), BF16),
            s_hid=dma(()), s_wq=dma((heads // 2,)), s_wkv=dma((2,)), s_wo=dma((2 * n_y,)),
            s_raw=dma((2,)), s_rawsend=dma((2,)), s_rawrecv=dma((2,)), s_ring=dma((RING, 2)),
            s_qs=dma((3, kv_n)), s_qr=dma((4, kv_n)),
            s_xs=dma((6,)), s_xr=dma((6,)), s_xst=dma((6,)), s_xrt=dma((6,)),
            s_ys=dma((6,)), s_yr=dma((6,)), s_gs=dma((6,)), s_gr=dma((3, 2)), s_out=dma((8,)),
        )
        hbm = pl.BlockSpec(memory_space=pl.ANY)
        return pl.pallas_call(
            functools.partial(kernel, (n_ctx, n_y, kv_n, grp)),
            out_shape=jax.ShapeDtypeStruct((rows, width), BF16),
            in_specs=[hbm] * 9 + [pl.BlockSpec(memory_space=pltpu.SMEM)],
            out_specs=hbm,
            scratch_shapes=list(scratch.values()),
            compiler_params=pltpu.CompilerParams(collective_id=0, has_side_effects=True, vmem_limit_bytes=67043328),
        )(hidden, w_query, w_key, w_value, w_out,
          prefix_k.reshape(pos * kv_n, head), prefix_v.reshape(pos * kv_n, head),
          suffix_k.reshape(rows, slots * kv_n, head), suffix_v.reshape(rows, slots * kv_n, head), seq_lens)

    return jax.shard_map(local_step, mesh=mesh, in_specs=(row_spec, col_spec, col_spec, col_spec, P('heads', None), pre_spec, pre_spec, suf_spec, suf_spec, P(('dp', 'ctx'))), out_specs=row_spec, check_vma=False)
```

```python
import functools
import math
import jax
import jax.numpy as jnp
from jax import lax
from jax.experimental import pallas as pl
from jax.experimental.pallas import tpu as pltpu
from jax.sharding import PartitionSpec as P

MESH = pl.DeviceIdType.MESH
F32 = jnp.float32
BF16 = jnp.bfloat16
LOW = -3.0e38
GROUP = 16
RING = 2
POS_CHUNK = 512


def dot_nt(a, b):
    return lax.dot_general(a, b, (((1,), (1,)), ((), ())), preferred_element_type=F32)


def dot_nn(a, b):
    return lax.dot_general(a, b, (((1,), (0,)), ((), ())), preferred_element_type=F32)


def pack_stats(row_max, row_sum):
    rows = row_max.shape[0]
    lane = lax.broadcasted_iota(jnp.int32, (rows, 128), 1)
    both = jnp.where(lane == 0, row_max, jnp.where(lane == 1, row_sum, 0.0))
    return jnp.transpose(both)[:8]


def unpack_stats(packed):
    rows = packed.shape[1]
    both = jnp.transpose(jnp.concatenate([packed, jnp.zeros((120, rows), F32)], axis=0))
    return both[:, 0:1], both[:, 1:2]


def merge(one, two):
    (num_a, max_a, sum_a), (num_b, max_b, sum_b) = one, two
    top = jnp.maximum(max_a, max_b)
    fac_a, fac_b = jnp.exp2(max_a - top), jnp.exp2(max_b - top)
    return num_a * fac_a + num_b * fac_b, top, sum_a * fac_a + sum_b * fac_b


def kernel(dims, hid_h, wq_h, wk_h, wv_h, wo_h, pk_h, pv_h, sk_h, sv_h, lens, out_h,
           hid, wq, wk, wv, wo, raw, flat, kpre, vpre, qg, q8, knew, vnew,
           ring_k, ring_v, qbd, sufs, sufp, scores, own_num, own_st, hold_num, hold_st,
           so8, sst8, xs_num, xs_st, xr_num, xr_st, att, yhold, ys, yr, yblk, ygat,
           s_hid, s_wq, s_wkv, s_wo, s_raw, s_rawsend, s_rawrecv, s_ring,
           s_qs, s_qr, s_xs, s_xr, s_xst, s_xrt, s_ys, s_yr, s_gs, s_gr, s_out):
    n_ctx, n_y, kv_n, grp = dims
    rows = hid.shape[0]
    width = hid.shape[1]
    head = kpre.shape[-1]
    heads = kv_n * grp
    local_pos = raw.shape[2] // kv_n
    scale = head ** -0.5 * math.log2(math.e)
    blk = width // n_y
    half = blk // 2
    part_rows = rows // 2
    stack = grp * part_rows

    ctx = lax.axis_index('ctx')
    ypos = lax.axis_index('heads')
    right = {'ctx': lax.rem(ctx + 2, n_ctx)}
    left = {'ctx': lax.rem(ctx + n_ctx - 2, n_ctx)}
    partner = {'ctx': ctx + 1 - 2 * lax.rem(ctx, 2)}
    up = {'heads': lax.rem(ypos + 1, n_y)}
    down = {'heads': lax.rem(ypos + n_y - 1, n_y)}
    below, above, opposite = lax.rem(ypos + n_y - 1, n_y), lax.rem(ypos + 1, n_y), lax.rem(ypos + n_y // 2, n_y)

    def remote(src, dst, send, recv, where):
        return pltpu.make_async_remote_copy(src_ref=src, dst_ref=dst, send_sem=send, recv_sem=recv,
                                            device_id=where, device_id_type=MESH)

    c_hid = pltpu.make_async_copy(hid_h, hid, s_hid)
    c_raw = [pltpu.make_async_copy(src, raw.at[0, i], s_raw.at[i]) for i, src in enumerate((pk_h, pv_h))]
    c_wq = [pltpu.make_async_copy(wq_h.at[:, pl.ds(kv * grp * head, grp * head)], wq.at[kv], s_wq.at[kv]) for kv in range(kv_n)]
    c_wkv = [pltpu.make_async_copy(src, dst, s_wkv.at[i]) for i, (src, dst) in enumerate(((wk_h, wk), (wv_h, wv)))]
    c_wo = []
    for r in range(2 * n_y):
        dest = lax.rem(ypos + r // 2, n_y)
        col = pl.multiple_of(dest * blk + (r % 2) * half, 128)
        c_wo.append(pltpu.make_async_copy(wo_h.at[:, pl.ds(col, half)], wo.at[r], s_wo.at[r]))
    n_groups = rows // GROUP

    def ring_copies(group):
        seqs = pl.ds(group * GROUP, GROUP)
        slot = group % RING
        return (pltpu.make_async_copy(sk_h.at[seqs], ring_k.at[slot], s_ring.at[slot, 0]),
                pltpu.make_async_copy(sv_h.at[seqs], ring_v.at[slot], s_ring.at[slot, 1]))

    def start(copies):
        for c in copies:
            c.start()

    def wait(copies):
        for c in copies:
            c.wait()

    c_hid.start()
    c_wq[0].start()
    start(c_raw)

    barrier = pltpu.get_barrier_semaphore()
    for where in (partner, left, right, up, down):
        pl.semaphore_signal(barrier, inc=1, device_id=where, device_id_type=MESH)

    def deinterleave(which):
        for i, dst in enumerate((kpre, vpre)):
            flat[...] = raw[which, i].astype(F32)
            for kv in range(kv_n):
                dst[kv, pl.ds(which * local_pos, local_pos), :] = flat[pl.ds(kv, local_pos, stride=kv_n), :].astype(BF16)

    def queries(kv):
        part = dot_nn(hid[...], wq[kv]).astype(BF16)
        qg[0, kv] = part
        for g in range(grp):
            q8[pl.ds(kv * grp + g, rows, stride=heads), :] = part[:, g * head:(g + 1) * head].astype(F32)

    def send_queries(kv):
        pair = (remote(qg.at[0, kv], qg.at[1, kv], s_qs.at[0, kv], s_qr.at[1, kv], right),
                remote(qg.at[0, kv], qg.at[2, kv], s_qs.at[1, kv], s_qr.at[2, kv], left))
        start(pair)
        return pair

    c_hid.wait()
    c_wq[0].wait()
    c_wq[1].start()
    start(c_wkv)
    queries(0)
    wait(c_raw)
    deinterleave(0)
    pl.semaphore_wait(barrier, 5)
    q_copies = [send_queries(0)]
    c_swap = [remote(src, raw.at[1, i], s_rawsend.at[i], s_rawrecv.at[i], partner) for i, src in enumerate((pk_h, pv_h))]
    start(c_swap)
    c_wq[1].wait()
    start(ring_copies(0))
    queries(1)
    q_copies.append(send_queries(1))
    start(ring_copies(1))
    start(c_wo)

    wait(c_wkv)
    knew[...] = dot_nn(hid[...], wk[...]).astype(BF16).astype(F32)
    vnew[...] = dot_nn(hid[...], wv[...]).astype(BF16).astype(F32)

    wait(c_swap)
    deinterleave(1)

    n_pos = kpre.shape[1]

    def prefix_pair(slot_a, slot_b, kv, chunk, buf):
        at_rows = pl.ds(chunk * part_rows, part_rows)
        stacked = jnp.concatenate([qg[slot, kv, at_rows, pl.ds(g * head, head)]
                                   for slot in (slot_a, slot_b) for g in range(grp)], axis=0)
        run = None
        for c in range(n_pos // POS_CHUNK):
            at = pl.ds(c * POS_CHUNK, POS_CHUNK)
            s = dot_nt(stacked, kpre[kv, at, :])
            scores[buf, :, at] = s
            for t in range(POS_CHUNK // 128):
                piece = s[:, t * 128:(t + 1) * 128]
                run = piece if run is None else jnp.maximum(run, piece)
        row_max = jnp.max(run, axis=1, keepdims=True) * scale
        wide_max = jnp.broadcast_to(row_max, (2 * stack, 128))
        wide_max = jnp.concatenate([wide_max] * (POS_CHUNK // 128), axis=1)
        total, num = None, None
        for c in range(n_pos // POS_CHUNK):
            at = pl.ds(c * POS_CHUNK, POS_CHUNK)
            p = jnp.exp2(scores[buf, :, at] * scale - wide_max)
            for t in range(POS_CHUNK // 128):
                piece = p[:, t * 128:(t + 1) * 128]
                total = piece if total is None else total + piece
            term = dot_nn(p.astype(BF16), vpre[kv, at, :])
            num = term if num is None else num + term
        row_sum = jnp.sum(total, axis=1, keepdims=True)
        return ((num[:stack], row_max[:stack], row_sum[:stack]), (num[stack:], row_max[stack:], row_sum[stack:]))

    sent = []

    def x_copies(i, where):
        return (remote(xs_num.at[i], xr_num.at[i], s_xs.at[i], s_xr.at[i], where),
                remote(xs_st.at[i], xr_st.at[i], s_xst.at[i], s_xrt.at[i], where))

    def post(state, i, where):
        xs_num[i] = state[0]
        xs_st[i] = pack_stats(state[1], state[2])
        out = x_copies(i, where)
        start(out)
        sent.extend(out)

    def received(i, where):
        for c in x_copies(i, where):
            c.wait_recv()
        return (xr_num[i],) + unpack_stats(xr_st[i])

    def keep(refs, i, state):
        refs[0][i] = state[0]
        lane = lax.broadcasted_iota(jnp.int32, state[0].shape, 1)
        refs[1][i] = jnp.where(lane == 0, state[1], state[2])

    def kept(refs, i):
        return refs[0][i], refs[1][i][:, 0:1], refs[1][i][:, 1:2]

    own = (own_num, own_st)
    hold = (hold_num, hold_st)

    def prefix_near(chunk):
        base = 6 * chunk
        on_right, on_left = prefix_pair(2, 1, 1, chunk, 0)
        post(on_right, base, right)
        keep(hold, 1, on_left)
        on_right, on_left = prefix_pair(2, 1, 0, chunk, 1)
        post(on_left, base + 1, left)
        keep(hold, 0, on_right)

    def prefix_far(chunk):
        base = 6 * chunk
        across, mine = prefix_pair(3, 0, 0, chunk, 0)
        post(across, base + 2, right)
        keep(own, 0, mine)
        across, mine = prefix_pair(3, 0, 1, chunk, 1)
        post(across, base + 3, left)
        keep(own, 1, mine)

    def relay(chunk):
        base = 6 * chunk
        post(merge(received(base + 2, right), kept(hold, 0)), base + 4, right)
        post(merge(received(base + 3, left), kept(hold, 1)), base + 5, left)

    lines = GROUP * heads
    span = ring_k.shape[2]
    tile = span // 4

    def suffix_group(group):
        slot = group % RING
        lane = lax.broadcasted_iota(jnp.int32, (head, lines), 1)
        q_t = jnp.transpose(q8[pl.ds(group * lines, lines), :])
        for j in range(GROUP // 2):
            both = [jnp.where(lane // heads == 2 * j + e, q_t, 0.0) for e in range(2)]
            qbd[j] = jnp.concatenate(both, axis=0).astype(BF16)
        one = lax.broadcasted_iota(jnp.int32, (1, lines), 1)
        length = jnp.zeros((1, lines), jnp.int32)
        for b in range(GROUP):
            length = jnp.where(one // heads == b, lens[group * GROUP + b], length)
        line = lax.broadcasted_iota(jnp.int32, (tile, lines), 0)
        lane = lax.broadcasted_iota(jnp.int32, (tile, lines), 1)
        mine = lax.rem(line, kv_n) == lax.rem(lane, heads) // grp
        place = jnp.where(mine, line // kv_n, span)
        wait(ring_copies(group))
        run = jnp.full((1, lines), LOW, F32)
        for c in range(4):
            at = pl.ds(c * tile, tile)
            s = None
            for j in range(GROUP // 2):
                keys = jnp.concatenate([ring_k[slot, 2 * j, at, :], ring_k[slot, 2 * j + 1, at, :]], axis=1)
                term = dot_nn(keys, qbd[j])
                s = term if s is None else s + term
            s = jnp.where(place < length - c * (tile // kv_n), s * scale, -jnp.inf)
            sufs[at, :] = s
            run = jnp.maximum(run, jnp.max(s, axis=0, keepdims=True))
        total = jnp.zeros((1, lines), F32)
        for c in range(4):
            p = jnp.exp2(sufs[pl.ds(c * tile, tile), :] - run)
            total = total + jnp.sum(p, axis=0, keepdims=True)
            sufp[:, pl.ds(c * tile, tile)] = jnp.transpose(p).astype(BF16)
        stats = jnp.concatenate([run, total, jnp.zeros((head - 2, lines), F32)], axis=0)
        sst8[pl.ds(group * lines, lines), :] = jnp.transpose(stats)
        for j in range(GROUP // 2):
            weights = sufp[pl.ds(2 * j * heads, 2 * heads), :]
            for e in range(2):
                o = dot_nn(weights, ring_v[slot, 2 * j + e])
                so8[pl.ds(group * lines + (2 * j + e) * heads, heads), :] = o[e * heads:(e + 1) * heads]
        if group + RING < n_groups:
            start(ring_copies(group + RING))

    def combine(chunk):
        base = 6 * chunk
        for kv in range(kv_n):
            states = [kept(own, kv)]
            if kv == 0:
                states += [received(base + 1, left), received(base + 4, right)]
            else:
                states += [received(base, right), received(base + 5, left)]
            state = functools.reduce(merge, states)
            rest = []
            for g in range(grp):
                every = pl.ds(chunk * part_rows * heads + kv * grp + g, part_rows, stride=heads)
                stats = sst8[every, :]
                rest.append((so8[every, :], stats[:, 0:1], stats[:, 1:2], q8[every, :]))
            num, top, tot, qs = (jnp.concatenate(list(v), axis=0) for v in zip(*rest))
            state = merge(state, (num, top, tot))
            at_rows = pl.ds(chunk * part_rows, part_rows)
            kn = jnp.concatenate([knew[at_rows, pl.ds(kv * head, head)]] * grp, axis=0)
            vn = jnp.concatenate([vnew[at_rows, pl.ds(kv * head, head)]] * grp, axis=0)
            s_new = jnp.sum(qs * kn, axis=1, keepdims=True) * scale
            state = merge(state, (vn, s_new, jnp.ones_like(s_new)))
            res = (state[0] / state[2]).astype(BF16)
            for g in range(grp):
                att[chunk, :, pl.ds((kv * grp + g) * head, head)] = res[g * part_rows:(g + 1) * part_rows]

    ysent = []

    def y_part(chunk, r):
        if chunk == 0:
            c_wo[r].wait()
        return dot_nn(att[chunk], wo[r])

    def y_copy(i, where):
        return remote(ys.at[i], yr.at[i], s_ys.at[i], s_yr.at[i], where)

    def y_post(val, i, where):
        ys[i] = val
        c = y_copy(i, where)
        c.start()
        ysent.append(c)

    far, near_up, near_down = 2 * (n_y // 2), 2, 2 * (n_y - 1)

    def project(chunk):
        base = 6 * chunk
        y_post(y_part(chunk, far), base, up)
        y_post(y_part(chunk, far + 1), base + 1, down)
        y_post(y_part(chunk, near_up + 1), base + 2, up)
        y_post(y_part(chunk, near_down), base + 3, down)
        yhold[0] = y_part(chunk, near_up)
        yhold[1] = y_part(chunk, near_down + 1)
        yhold[2] = y_part(chunk, 0)
        yhold[3] = y_part(chunk, 1)

    def y_relay(chunk):
        base = 6 * chunk
        y_copy(base, up).wait_recv()
        y_post(yhold[0] + yr[base], base + 4, up)
        y_copy(base + 1, down).wait_recv()
        y_post(yhold[1] + yr[base + 1], base + 5, down)

    gsend = []

    def g_copy(src, chunk, slot, part, sem, where):
        return remote(src, ygat.at[chunk, slot, part], s_gs.at[chunk, sem], s_gr.at[chunk, slot, part], where)

    outs = []

    def put(src, chunk, dest, part):
        col = pl.multiple_of(dest * blk + part * half, 128)
        c = pltpu.make_async_copy(src, out_h.at[pl.ds(chunk * part_rows, part_rows), pl.ds(col, half)], s_out.at[len(outs)])
        c.start()
        outs.append(c)

    def g_out(chunk, slot, part, where, sem):
        src = yblk.at[chunk, part] if slot < 2 else ygat.at[chunk, 0 if part == 0 else 1, part]
        return g_copy(src, chunk, slot, part, sem, where)

    def finish(chunk):
        base = 6 * chunk
        at_rows = pl.ds(chunk * part_rows, part_rows)
        for part, (near, merged) in enumerate(((base + 3, base + 4), (base + 2, base + 5))):
            val = yhold[2 + part]
            for i in (near, merged):
                y_copy(i, up if i % 2 == 0 else down).wait_recv()
                val = val + yr[i]
            col = pl.multiple_of(ypos * blk + part * half, 128)
            yblk[chunk, part] = (val + hid[at_rows, pl.ds(col, half)].astype(F32)).astype(BF16)
            first, second = ((0, up, part), (1, down, 2 + part)) if part == 0 else ((1, down, 2 + part), (0, up, part))
            for slot, where, sem in (first, second):
                c = g_out(chunk, slot, part, where, sem)
                c.start()
                gsend.append(c)
            put(yblk.at[chunk, part], chunk, ypos, part)

    def forward(chunk):
        g_out(chunk, 0, 0, up, 0).wait_recv()
        c = g_out(chunk, 2, 0, up, 4)
        c.start()
        gsend.append(c)
        g_out(chunk, 1, 1, down, 3).wait_recv()
        c = g_out(chunk, 2, 1, down, 5)
        c.start()
        gsend.append(c)
        put(ygat.at[chunk, 0, 0], chunk, below, 0)
        put(ygat.at[chunk, 1, 1], chunk, above, 1)

    def collect(chunk):
        g_out(chunk, 0, 1, up, 1).wait_recv()
        put(ygat.at[chunk, 0, 1], chunk, below, 1)
        g_out(chunk, 1, 0, down, 2).wait_recv()
        put(ygat.at[chunk, 1, 0], chunk, above, 0)
        g_out(chunk, 2, 0, up, 4).wait_recv()
        put(ygat.at[chunk, 2, 0], chunk, opposite, 0)
        g_out(chunk, 2, 1, down, 5).wait_recv()
        put(ygat.at[chunk, 2, 1], chunk, opposite, 1)

    q_copies[0][0].wait_recv()
    fwd_right = remote(qg.at[1, 0], qg.at[3, 0], s_qs.at[2, 0], s_qr.at[3, 0], right)
    fwd_right.start()
    q_copies[1][1].wait_recv()
    fwd_left = remote(qg.at[2, 1], qg.at[3, 1], s_qs.at[2, 1], s_qr.at[3, 1], left)
    fwd_left.start()
    q_copies[1][0].wait_recv()
    q_copies[0][1].wait_recv()

    per_part = n_groups // 2
    prefix_near(0)
    fwd_right.wait_recv()
    fwd_left.wait_recv()
    prefix_far(0)
    for group in range(per_part // 2):
        suffix_group(group)
    relay(0)
    for group in range(per_part // 2, per_part):
        suffix_group(group)
    combine(0)
    project(0)

    prefix_near(1)
    y_relay(0)
    prefix_far(1)
    for group in range(per_part, per_part + per_part // 2):
        suffix_group(group)
    finish(0)
    relay(1)
    for group in range(per_part + per_part // 2, n_groups):
        suffix_group(group)
    forward(0)
    combine(1)
    project(1)
    collect(0)
    y_relay(1)
    finish(1)
    forward(1)
    collect(1)

    for pair in q_copies:
        for c in pair:
            c.wait_send()
    for c in [fwd_right, fwd_left] + sent + ysent + gsend:
        c.wait_send()
    wait(outs)


def solution(mesh):
    n_ctx, n_y = mesh.shape['ctx'], mesh.shape['heads']
    row_spec = P(('dp', 'ctx'), None)
    col_spec = P(None, 'heads')
    pre_spec = P(('dp', 'ctx'), 'heads', None)
    suf_spec = P(('dp', 'ctx'), None, 'heads', None)

    def local_step(hidden, w_query, w_key, w_value, w_out, prefix_k, prefix_v, suffix_k, suffix_v, seq_lens):
        rows, width = hidden.shape
        pos, kv_n, head = prefix_k.shape
        slots = suffix_k.shape[1]
        grp = w_query.shape[1] // (kv_n * head)
        heads = kv_n * grp
        blk = width // n_y
        half_rows = rows // 2
        stack = grp * half_rows
        lines = GROUP * heads
        dma = pltpu.SemaphoreType.DMA
        scratch = dict(
            hid=pltpu.VMEM((rows, width), BF16),
            wq=pltpu.VMEM((kv_n, width, grp * head), BF16),
            wk=pltpu.VMEM((width, kv_n * head), BF16),
            wv=pltpu.VMEM((width, kv_n * head), BF16),
            wo=pltpu.VMEM((2 * n_y, heads * head, blk // 2), BF16),
            raw=pltpu.VMEM((2, 2, pos * kv_n, head), BF16),
            flat=pltpu.VMEM((pos * kv_n, head), F32),
            kpre=pltpu.VMEM((kv_n, 2 * pos, head), BF16),
            vpre=pltpu.VMEM((kv_n, 2 * pos, head), BF16),
            qg=pltpu.VMEM((4, kv_n, rows, grp * head), BF16),
            q8=pltpu.VMEM((rows * heads, head), F32),
            knew=pltpu.VMEM((rows, kv_n * head), F32),
            vnew=pltpu.VMEM((rows, kv_n * head), F32),
            ring_k=pltpu.VMEM((RING, GROUP, slots * kv_n, head), BF16),
            ring_v=pltpu.VMEM((RING, GROUP, slots * kv_n, head), BF16),
            qbd=pltpu.VMEM((GROUP // 2, 2 * head, lines), BF16),
            sufs=pltpu.VMEM((slots * kv_n, lines), F32),
            sufp=pltpu.VMEM((lines, slots * kv_n), BF16),
            scores=pltpu.VMEM((2, 2 * stack, 2 * pos), F32),
            own_num=pltpu.VMEM((kv_n, stack, head), F32),
            own_st=pltpu.VMEM((kv_n, stack, 128), F32),
            hold_num=pltpu.VMEM((2, stack, head), F32),
            hold_st=pltpu.VMEM((2, stack, 128), F32),
            so8=pltpu.VMEM((rows * heads, head), F32),
            sst8=pltpu.VMEM((rows * heads, head), F32),
            xs_num=pltpu.VMEM((12, stack, head), F32),
            xs_st=pltpu.VMEM((12, 8, stack), F32),
            xr_num=pltpu.VMEM((12, stack, head), F32),
            xr_st=pltpu.VMEM((12, 8, stack), F32),
            att=pltpu.VMEM((2, half_rows, heads * head), BF16),
            yhold=pltpu.VMEM((4, half_rows, blk // 2), F32),
            ys=pltpu.VMEM((12, half_rows, blk // 2), F32),
            yr=pltpu.VMEM((12, half_rows, blk // 2), F32),
            yblk=pltpu.VMEM((2, 2, half_rows, blk // 2), BF16),
            ygat=pltpu.VMEM((2, 3, 2, half_rows, blk // 2), BF16),
            s_hid=dma(()), s_wq=dma((kv_n,)), s_wkv=dma((2,)), s_wo=dma((2 * n_y,)),
            s_raw=dma((2,)), s_rawsend=dma((2,)), s_rawrecv=dma((2,)), s_ring=dma((RING, 2)),
            s_qs=dma((3, kv_n)), s_qr=dma((4, kv_n)),
            s_xs=dma((12,)), s_xr=dma((12,)), s_xst=dma((12,)), s_xrt=dma((12,)),
            s_ys=dma((12,)), s_yr=dma((12,)), s_gs=dma((2, 6)), s_gr=dma((2, 3, 2)), s_out=dma((16,)),
        )
        hbm = pl.BlockSpec(memory_space=pl.ANY)
        return pl.pallas_call(
            functools.partial(kernel, (n_ctx, n_y, kv_n, grp)),
            out_shape=jax.ShapeDtypeStruct((rows, width), BF16),
            in_specs=[hbm] * 9 + [pl.BlockSpec(memory_space=pltpu.SMEM)],
            out_specs=hbm,
            scratch_shapes=list(scratch.values()),
            compiler_params=pltpu.CompilerParams(collective_id=0, has_side_effects=True, vmem_limit_bytes=67043328),
        )(hidden, w_query, w_key, w_value, w_out,
          prefix_k.reshape(pos * kv_n, head), prefix_v.reshape(pos * kv_n, head),
          suffix_k.reshape(rows, slots * kv_n, head), suffix_v.reshape(rows, slots * kv_n, head), seq_lens)

    return jax.shard_map(local_step, mesh=mesh, in_specs=(row_spec, col_spec, col_spec, col_spec, P('heads', None), pre_spec, pre_spec, suf_spec, suf_spec, P(('dp', 'ctx'))), out_specs=row_spec, check_vma=False)
```

```python
import functools
import math
import jax
import jax.numpy as jnp
from jax import lax
from jax.experimental import pallas as pl
from jax.experimental.pallas import tpu as pltpu
from jax.sharding import PartitionSpec as P

MESH = pl.DeviceIdType.MESH
F32 = jnp.float32
BF16 = jnp.bfloat16
LOW = -3.0e38
GROUP = 16
RING = 2
POS_CHUNK = 512
PIECES = 4
VMEM_BYTES = 66000000


def dot_nt(a, b):
    return lax.dot_general(a, b, (((1,), (1,)), ((), ())), preferred_element_type=F32)


def dot_nn(a, b):
    return lax.dot_general(a, b, (((1,), (0,)), ((), ())), preferred_element_type=F32)


def pack_stats(row_max, row_sum):
    rows = row_max.shape[0]
    lane = lax.broadcasted_iota(jnp.int32, (rows, 128), 1)
    both = jnp.where(lane == 0, row_max, jnp.where(lane == 1, row_sum, 0.0))
    return jnp.transpose(both)[:8]


def unpack_stats(packed):
    rows = packed.shape[1]
    both = jnp.transpose(jnp.concatenate([packed, jnp.zeros((120, rows), F32)], axis=0))
    return both[:, 0:1], both[:, 1:2]


def merge(one, two):
    (num_a, max_a, sum_a), (num_b, max_b, sum_b) = one, two
    top = jnp.maximum(max_a, max_b)
    fac_a, fac_b = jnp.exp2(max_a - top), jnp.exp2(max_b - top)
    return num_a * fac_a + num_b * fac_b, top, sum_a * fac_a + sum_b * fac_b


def kernel(dims, hid_h, wq_h, wk_h, wv_h, wo_h, pk_h, pv_h, sk_h, sv_h, lens, out_v,
           hid, wq, wk, wv, wo, raw, flat, kpre, vpre, qg, q8, knew, vnew,
           ring_k, ring_v, qbd, sufs, sufp, scores, own_num, own_st, hold_num, hold_st,
           so8, sst8, xs_num, xs_st, xr_num, xr_st, att, yhold, ys, yr,
           s_hid, s_wq, s_wkv, s_wo, s_raw, s_rawsend, s_rawrecv, s_ring,
           s_qs, s_qr, s_xs, s_xr, s_xst, s_xrt, s_ys, s_yr, s_gs, s_gr):
    n_ctx, n_y, kv_n, grp = dims
    rows = hid.shape[0]
    width = hid.shape[1]
    head = kpre.shape[-1]
    heads = kv_n * grp
    local_pos = raw.shape[2] // kv_n
    scale = head ** -0.5 * math.log2(math.e)
    blk = width // n_y
    half = blk // 2
    part_rows = rows // 2
    stack = grp * part_rows

    ctx = lax.axis_index('ctx')
    ypos = lax.axis_index('heads')
    right = {'ctx': lax.rem(ctx + 2, n_ctx)}
    left = {'ctx': lax.rem(ctx + n_ctx - 2, n_ctx)}
    partner = {'ctx': ctx + 1 - 2 * lax.rem(ctx, 2)}
    up = {'heads': lax.rem(ypos + 1, n_y)}
    down = {'heads': lax.rem(ypos + n_y - 1, n_y)}
    below, above = lax.rem(ypos + n_y - 1, n_y), lax.rem(ypos + 1, n_y)

    def remote(src, dst, send, recv, where):
        return pltpu.make_async_remote_copy(src_ref=src, dst_ref=dst, send_sem=send, recv_sem=recv,
                                            device_id=where, device_id_type=MESH)

    c_hid = pltpu.make_async_copy(hid_h, hid, s_hid)
    c_raw = [pltpu.make_async_copy(src, raw.at[0, i], s_raw.at[i]) for i, src in enumerate((pk_h, pv_h))]
    deep = width // PIECES
    c_wq = [pltpu.make_async_copy(wq_h.at[pl.ds(k * deep, deep), pl.ds(kv * grp * head, grp * head)],
                                  wq.at[kv, pl.ds(k * deep, deep), :], s_wq.at[kv, k])
            for kv in range(kv_n) for k in range(PIECES)]
    c_wkv = [pltpu.make_async_copy(src, dst, s_wkv.at[i]) for i, (src, dst) in enumerate(((wk_h, wk), (wv_h, wv)))]
    c_wo = []
    for r in range(2 * n_y):
        dest = lax.rem(ypos + r // 2, n_y)
        col = pl.multiple_of(dest * blk + (r % 2) * half, 128)
        c_wo.append(pltpu.make_async_copy(wo_h.at[:, pl.ds(col, half)], wo.at[r], s_wo.at[r]))
    n_groups = rows // GROUP

    def ring_copies(group):
        seqs = pl.ds(group * GROUP, GROUP)
        slot = group % RING
        return (pltpu.make_async_copy(sk_h.at[seqs], ring_k.at[slot], s_ring.at[slot, 0]),
                pltpu.make_async_copy(sv_h.at[seqs], ring_v.at[slot], s_ring.at[slot, 1]))

    def start(copies):
        for c in copies:
            c.start()

    def wait(copies):
        for c in copies:
            c.wait()

    queue = c_wq + c_raw + c_wkv

    def advance():
        if queue:
            queue.pop(0).start()

    c_hid.start()
    for _ in range(3):
        advance()

    barrier = pltpu.get_barrier_semaphore()
    for where in (partner, left, right, up, down):
        pl.semaphore_signal(barrier, inc=1, device_id=where, device_id_type=MESH)

    def deinterleave(which):
        for i, dst in enumerate((kpre, vpre)):
            flat[...] = raw[which, i].astype(F32)
            for kv in range(kv_n):
                dst[kv, pl.ds(which * local_pos, local_pos), :] = flat[pl.ds(kv, local_pos, stride=kv_n), :].astype(BF16)

    def queries(kv):
        total = None
        for k in range(PIECES):
            c_wq[kv * PIECES + k].wait()
            advance()
            at = pl.ds(k * deep, deep)
            term = dot_nn(hid[:, at], wq[kv, at, :])
            total = term if total is None else total + term
        part = total.astype(BF16)
        qg[0, kv] = part
        for g in range(grp):
            q8[pl.ds(kv * grp + g, rows, stride=heads), :] = part[:, g * head:(g + 1) * head].astype(F32)

    def send_queries(kv):
        pair = (remote(qg.at[0, kv], qg.at[1, kv], s_qs.at[0, kv], s_qr.at[1, kv], right),
                remote(qg.at[0, kv], qg.at[2, kv], s_qs.at[1, kv], s_qr.at[2, kv], left))
        start(pair)
        return pair

    c_hid.wait()
    queries(0)
    pl.semaphore_wait(barrier, 5)
    q_copies = [send_queries(0)]
    c_swap = [remote(src, raw.at[1, i], s_rawsend.at[i], s_rawrecv.at[i], partner) for i, src in enumerate((pk_h, pv_h))]
    start(c_swap)
    queries(1)
    q_copies.append(send_queries(1))
    while queue:
        advance()
    wait(c_raw)
    deinterleave(0)

    wait(c_wkv)
    start(ring_copies(0))
    knew[...] = dot_nn(hid[...], wk[...]).astype(BF16).astype(F32)
    vnew[...] = dot_nn(hid[...], wv[...]).astype(BF16).astype(F32)

    wait(c_swap)
    deinterleave(1)
    start(ring_copies(1))
    for r in (4, 5, 3, 6, 2, 7, 0, 1):
        c_wo[r].start()

    n_pos = kpre.shape[1]

    n_pieces = n_pos // POS_CHUNK
    part_lanes = POS_CHUNK // 128

    def prefix_states(jobs):
        stacked, run, out = [None] * len(jobs), [None] * len(jobs), []

        def score(i, c):
            sources, kv = jobs[i]
            if c == 0:
                stacked[i] = jnp.concatenate([qg[slot, kv, pl.ds(chunk * part_rows, part_rows), pl.ds(g * head, head)]
                                              for slot, chunk in sources for g in range(grp)], axis=0)
            at = pl.ds(c * POS_CHUNK, POS_CHUNK)
            s = dot_nt(stacked[i], kpre[kv, at, :])
            scores[i % 2, :, at] = s
            for t in range(part_lanes):
                piece = s[:, t * 128:(t + 1) * 128]
                run[i] = piece if run[i] is None else jnp.maximum(run[i], piece)

        for c in range(n_pieces):
            score(0, c)
        for i, (sources, kv) in enumerate(jobs):
            row_max = jnp.max(run[i], axis=1, keepdims=True) * scale
            wide_max = jnp.broadcast_to(row_max, (2 * stack, 128))
            wide_max = jnp.concatenate([wide_max] * part_lanes, axis=1)
            total, num = None, None
            for c in range(n_pieces):
                if i + 1 < len(jobs):
                    score(i + 1, c)
                at = pl.ds(c * POS_CHUNK, POS_CHUNK)
                p = jnp.exp2(scores[i % 2, :, at] * scale - wide_max)
                for t in range(part_lanes):
                    piece = p[:, t * 128:(t + 1) * 128]
                    total = piece if total is None else total + piece
                term = dot_nn(p.astype(BF16), vpre[kv, at, :])
                num = term if num is None else num + term
            row_sum = jnp.sum(total, axis=1, keepdims=True)
            out += [(num[:stack], row_max[:stack], row_sum[:stack]), (num[stack:], row_max[stack:], row_sum[stack:])]
        return out

    sent = []

    def x_copies(i, where):
        return (remote(xs_num.at[i], xr_num.at[i], s_xs.at[i], s_xr.at[i], where),
                remote(xs_st.at[i], xr_st.at[i], s_xst.at[i], s_xrt.at[i], where))

    def post(state, i, where):
        xs_num[i] = state[0]
        xs_st[i] = pack_stats(state[1], state[2])
        out = x_copies(i, where)
        start(out)
        sent.extend(out)

    def received(i, where):
        for c in x_copies(i, where):
            c.wait_recv()
        return (xr_num[i],) + unpack_stats(xr_st[i])

    def keep(refs, i, state):
        refs[0][i] = state[0]
        lane = lax.broadcasted_iota(jnp.int32, state[0].shape, 1)
        refs[1][i] = jnp.where(lane == 0, state[1], state[2])

    def kept(refs, i):
        return refs[0][i], refs[1][i][:, 0:1], refs[1][i][:, 1:2]

    own = (own_num, own_st)
    hold = (hold_num, hold_st)

    def prefix_near(chunk):
        base = 6 * chunk
        both = ((2, chunk), (1, chunk))
        right_1, left_1, right_0, left_0 = prefix_states([(both, 1), (both, 0)])
        post(right_1, base, right)
        post(left_0, base + 1, left)
        keep(hold, 1, left_1)
        keep(hold, 0, right_0)

    def prefix_far():
        both = ((3, 0), (3, 1))
        states = prefix_states([(both, 0), (both, 1)])
        for chunk in range(2):
            post(states[chunk], 6 * chunk + 2, right)
            post(states[2 + chunk], 6 * chunk + 3, left)

    def prefix_own():
        both = ((0, 0), (0, 1))
        for i, state in enumerate(prefix_states([(both, 0), (both, 1)])):
            keep(own, i, state)

    def relay(chunk):
        base = 6 * chunk
        post(merge(received(base + 2, right), kept(hold, 0)), base + 4, right)
        post(merge(received(base + 3, left), kept(hold, 1)), base + 5, left)

    lines = GROUP * heads
    span = ring_k.shape[2]
    tile = span // 4

    def suffix_group(group):
        slot = group % RING
        lane = lax.broadcasted_iota(jnp.int32, (head, lines), 1)
        q_t = jnp.transpose(q8[pl.ds(group * lines, lines), :])
        for j in range(GROUP // 2):
            both = [jnp.where(lane // heads == 2 * j + e, q_t, 0.0) for e in range(2)]
            qbd[j] = jnp.concatenate(both, axis=0).astype(BF16)
        one = lax.broadcasted_iota(jnp.int32, (1, lines), 1)
        length = jnp.zeros((1, lines), jnp.int32)
        for b in range(GROUP):
            length = jnp.where(one // heads == b, lens[group * GROUP + b], length)
        line = lax.broadcasted_iota(jnp.int32, (tile, lines), 0)
        lane = lax.broadcasted_iota(jnp.int32, (tile, lines), 1)
        mine = lax.rem(line, kv_n) == lax.rem(lane, heads) // grp
        place = jnp.where(mine, line // kv_n, span)
        wait(ring_copies(group))
        run = jnp.full((1, lines), LOW, F32)
        for c in range(4):
            at = pl.ds(c * tile, tile)
            s = None
            for j in range(GROUP // 2):
                keys = jnp.concatenate([ring_k[slot, 2 * j, at, :], ring_k[slot, 2 * j + 1, at, :]], axis=1)
                term = dot_nn(keys, qbd[j])
                s = term if s is None else s + term
            s = jnp.where(place < length - c * (tile // kv_n), s * scale, -jnp.inf)
            sufs[at, :] = s
            run = jnp.maximum(run, jnp.max(s, axis=0, keepdims=True))
        total = jnp.zeros((1, lines), F32)
        for c in range(4):
            p = jnp.exp2(sufs[pl.ds(c * tile, tile), :] - run)
            total = total + jnp.sum(p, axis=0, keepdims=True)
            sufp[:, pl.ds(c * tile, tile)] = jnp.transpose(p).astype(BF16)
        stats = jnp.concatenate([run, total, jnp.zeros((head - 2, lines), F32)], axis=0)
        sst8[pl.ds(group * lines, lines), :] = jnp.transpose(stats)
        for j in range(GROUP // 2):
            weights = sufp[pl.ds(2 * j * heads, 2 * heads), :]
            for e in range(2):
                o = dot_nn(weights, ring_v[slot, 2 * j + e])
                so8[pl.ds(group * lines + (2 * j + e) * heads, heads), :] = o[e * heads:(e + 1) * heads]
        if group + RING < n_groups:
            start(ring_copies(group + RING))

    def combine(chunk):
        base = 6 * chunk
        for kv in range(kv_n):
            states = [kept(own, 2 * kv + chunk)]
            if kv == 0:
                states += [received(base + 1, left), received(base + 4, right)]
            else:
                states += [received(base, right), received(base + 5, left)]
            state = functools.reduce(merge, states)
            rest = []
            for g in range(grp):
                every = pl.ds(chunk * part_rows * heads + kv * grp + g, part_rows, stride=heads)
                stats = sst8[every, :]
                rest.append((so8[every, :], stats[:, 0:1], stats[:, 1:2], q8[every, :]))
            num, top, tot, qs = (jnp.concatenate(list(v), axis=0) for v in zip(*rest))
            state = merge(state, (num, top, tot))
            at_rows = pl.ds(chunk * part_rows, part_rows)
            kn = jnp.concatenate([knew[at_rows, pl.ds(kv * head, head)]] * grp, axis=0)
            vn = jnp.concatenate([vnew[at_rows, pl.ds(kv * head, head)]] * grp, axis=0)
            s_new = jnp.sum(qs * kn, axis=1, keepdims=True) * scale
            state = merge(state, (vn, s_new, jnp.ones_like(s_new)))
            res = (state[0] / state[2]).astype(BF16)
            for g in range(grp):
                att[chunk, :, pl.ds((kv * grp + g) * head, head)] = res[g * part_rows:(g + 1) * part_rows]

    ysent = []

    def y_part(chunk, r):
        if chunk == 0:
            c_wo[r].wait()
        return dot_nn(att[chunk], wo[r])

    def y_copy(i, where):
        return remote(ys.at[i], yr.at[i], s_ys.at[i], s_yr.at[i], where)

    def y_post(val, i, where):
        ys[i] = val
        c = y_copy(i, where)
        c.start()
        ysent.append(c)

    far, near_up, near_down = 2 * (n_y // 2), 2, 2 * (n_y - 1)

    def project(chunk):
        base = 6 * chunk
        y_post(y_part(chunk, far), base, up)
        y_post(y_part(chunk, far + 1), base + 1, down)
        y_post(y_part(chunk, near_up + 1), base + 2, up)
        y_post(y_part(chunk, near_down), base + 3, down)
        yhold[0] = y_part(chunk, near_up)
        yhold[1] = y_part(chunk, near_down + 1)
        yhold[2] = y_part(chunk, 0)
        yhold[3] = y_part(chunk, 1)

    def y_relay(chunk):
        base = 6 * chunk
        y_copy(base, up).wait_recv()
        y_post(yhold[0] + yr[base], base + 4, up)
        y_copy(base + 1, down).wait_recv()
        y_post(yhold[1] + yr[base + 1], base + 5, down)

    gsend = []

    def g_out(chunk, slot, part, where, sem):
        dest = ypos if slot < 2 else (below if part == 0 else above)
        at = (pl.ds(chunk * part_rows, part_rows), pl.ds(pl.multiple_of(dest * blk + part * half, 128), half))
        return remote(out_v.at[at], out_v.at[at], s_gs.at[chunk, sem], s_gr.at[chunk, slot, part], where)

    def finish(chunk):
        base = 6 * chunk
        at_rows = pl.ds(chunk * part_rows, part_rows)
        for part, (near, merged) in enumerate(((base + 3, base + 4), (base + 2, base + 5))):
            val = yhold[2 + part]
            for i in (near, merged):
                y_copy(i, up if i % 2 == 0 else down).wait_recv()
                val = val + yr[i]
            col = pl.multiple_of(ypos * blk + part * half, 128)
            out_v[at_rows, pl.ds(col, half)] = (val + hid[at_rows, pl.ds(col, half)].astype(F32)).astype(BF16)
            first, second = ((0, up, part), (1, down, 2 + part)) if part == 0 else ((1, down, 2 + part), (0, up, part))
            for slot, where, sem in (first, second):
                c = g_out(chunk, slot, part, where, sem)
                c.start()
                gsend.append(c)

    def forward(chunk):
        g_out(chunk, 0, 0, up, 0).wait_recv()
        c = g_out(chunk, 2, 0, up, 4)
        c.start()
        gsend.append(c)
        g_out(chunk, 1, 1, down, 3).wait_recv()
        c = g_out(chunk, 2, 1, down, 5)
        c.start()
        gsend.append(c)

    def collect(chunk):
        g_out(chunk, 0, 1, up, 1).wait_recv()
        g_out(chunk, 1, 0, down, 2).wait_recv()
        g_out(chunk, 2, 0, up, 4).wait_recv()
        g_out(chunk, 2, 1, down, 5).wait_recv()

    prefix_own()
    q_copies[0][0].wait_recv()
    fwd_right = remote(qg.at[1, 0], qg.at[3, 0], s_qs.at[2, 0], s_qr.at[3, 0], right)
    fwd_right.start()
    q_copies[1][1].wait_recv()
    fwd_left = remote(qg.at[2, 1], qg.at[3, 1], s_qs.at[2, 1], s_qr.at[3, 1], left)
    fwd_left.start()
    q_copies[1][0].wait_recv()
    q_copies[0][1].wait_recv()

    per_part = n_groups // 2
    prefix_near(0)
    fwd_right.wait_recv()
    fwd_left.wait_recv()
    prefix_far()
    for group in range(per_part):
        suffix_group(group)
    relay(0)
    prefix_near(1)
    combine(0)
    project(0)

    suffix_group(per_part)
    y_relay(0)
    relay(1)
    for group in range(per_part + 1, n_groups):
        suffix_group(group)
    finish(0)
    combine(1)
    project(1)
    forward(0)
    collect(0)
    y_relay(1)
    finish(1)
    forward(1)
    collect(1)

    for pair in q_copies:
        for c in pair:
            c.wait_send()
    for c in [fwd_right, fwd_left] + sent + ysent + gsend:
        c.wait_send()


def store(src, dst, sem):
    c = pltpu.make_async_copy(src, dst, sem)
    c.start()
    c.wait()


def solution(mesh):
    n_ctx, n_y = mesh.shape['ctx'], mesh.shape['heads']
    row_spec = P(('dp', 'ctx'), None)
    col_spec = P(None, 'heads')
    pre_spec = P(('dp', 'ctx'), 'heads', None)
    suf_spec = P(('dp', 'ctx'), None, 'heads', None)

    def local_step(hidden, w_query, w_key, w_value, w_out, prefix_k, prefix_v, suffix_k, suffix_v, seq_lens):
        rows, width = hidden.shape
        pos, kv_n, head = prefix_k.shape
        slots = suffix_k.shape[1]
        grp = w_query.shape[1] // (kv_n * head)
        heads = kv_n * grp
        blk = width // n_y
        half_rows = rows // 2
        stack = grp * half_rows
        lines = GROUP * heads
        dma = pltpu.SemaphoreType.DMA
        scratch = dict(
            hid=pltpu.VMEM((rows, width), BF16),
            wq=pltpu.VMEM((kv_n, width, grp * head), BF16),
            wk=pltpu.VMEM((width, kv_n * head), BF16),
            wv=pltpu.VMEM((width, kv_n * head), BF16),
            wo=pltpu.VMEM((2 * n_y, heads * head, blk // 2), BF16),
            raw=pltpu.VMEM((2, 2, pos * kv_n, head), BF16),
            flat=pltpu.VMEM((pos * kv_n, head), F32),
            kpre=pltpu.VMEM((kv_n, 2 * pos, head), BF16),
            vpre=pltpu.VMEM((kv_n, 2 * pos, head), BF16),
            qg=pltpu.VMEM((4, kv_n, rows, grp * head), BF16),
            q8=pltpu.VMEM((rows * heads, head), F32),
            knew=pltpu.VMEM((rows, kv_n * head), F32),
            vnew=pltpu.VMEM((rows, kv_n * head), F32),
            ring_k=pltpu.VMEM((RING, GROUP, slots * kv_n, head), BF16),
            ring_v=pltpu.VMEM((RING, GROUP, slots * kv_n, head), BF16),
            qbd=pltpu.VMEM((GROUP // 2, 2 * head, lines), BF16),
            sufs=pltpu.VMEM((slots * kv_n, lines), F32),
            sufp=pltpu.VMEM((lines, slots * kv_n), BF16),
            scores=pltpu.VMEM((2, 2 * stack, 2 * pos), F32),
            own_num=pltpu.VMEM((2 * kv_n, stack, head), F32),
            own_st=pltpu.VMEM((2 * kv_n, stack, 128), F32),
            hold_num=pltpu.VMEM((2, stack, head), F32),
            hold_st=pltpu.VMEM((2, stack, 128), F32),
            so8=pltpu.VMEM((rows * heads, head), F32),
            sst8=pltpu.VMEM((rows * heads, head), F32),
            xs_num=pltpu.VMEM((12, stack, head), F32),
            xs_st=pltpu.VMEM((12, 8, stack), F32),
            xr_num=pltpu.VMEM((12, stack, head), F32),
            xr_st=pltpu.VMEM((12, 8, stack), F32),
            att=pltpu.VMEM((2, half_rows, heads * head), BF16),
            yhold=pltpu.VMEM((4, half_rows, blk // 2), F32),
            ys=pltpu.VMEM((12, half_rows, blk // 2), F32),
            yr=pltpu.VMEM((12, half_rows, blk // 2), F32),
            s_hid=dma(()), s_wq=dma((kv_n, PIECES)), s_wkv=dma((2,)), s_wo=dma((2 * n_y,)),
            s_raw=dma((2,)), s_rawsend=dma((2,)), s_rawrecv=dma((2,)), s_ring=dma((RING, 2)),
            s_qs=dma((3, kv_n)), s_qr=dma((4, kv_n)),
            s_xs=dma((12,)), s_xr=dma((12,)), s_xst=dma((12,)), s_xrt=dma((12,)),
            s_ys=dma((12,)), s_yr=dma((12,)), s_gs=dma((2, 6)), s_gr=dma((2, 3, 2)),
        )
        hbm = pl.BlockSpec(memory_space=pl.ANY)
        out = pl.pallas_call(
            functools.partial(kernel, (n_ctx, n_y, kv_n, grp)),
            out_shape=pltpu.VMEM((rows, width), BF16),
            in_specs=[hbm] * 9 + [pl.BlockSpec(memory_space=pltpu.SMEM)],
            out_specs=pl.BlockSpec(memory_space=pltpu.VMEM),
            scratch_shapes=list(scratch.values()),
            compiler_params=pltpu.CompilerParams(collective_id=0, has_side_effects=True, vmem_limit_bytes=VMEM_BYTES),
        )(hidden, w_query, w_key, w_value, w_out,
          prefix_k.reshape(pos * kv_n, head), prefix_v.reshape(pos * kv_n, head),
          suffix_k.reshape(rows, slots * kv_n, head), suffix_v.reshape(rows, slots * kv_n, head), seq_lens)
        return pl.pallas_call(
            store,
            out_shape=jax.ShapeDtypeStruct((rows, width), BF16),
            in_specs=[pl.BlockSpec(memory_space=pltpu.VMEM)],
            out_specs=hbm,
            scratch_shapes=[dma(())],
            compiler_params=pltpu.CompilerParams(vmem_limit_bytes=1048576),
        )(out)

    return jax.shard_map(local_step, mesh=mesh, in_specs=(row_spec, col_spec, col_spec, col_spec, P('heads', None), pre_spec, pre_spec, suf_spec, suf_spec, P(('dp', 'ctx'))), out_specs=row_spec, check_vma=False)
```

```python
import functools
import math
import jax
import jax.numpy as jnp
from jax import lax
from jax.experimental import pallas as pl
from jax.experimental.pallas import tpu as pltpu
from jax.sharding import PartitionSpec as P

MESH = pl.DeviceIdType.MESH
F32 = jnp.float32
BF16 = jnp.bfloat16
LOW = -3.0e38
GROUP = 16
RING = 2
POS_CHUNK = 512
PIECES = 4
VMEM_BYTES = 66000000


def dot_nt(a, b):
    return lax.dot_general(a, b, (((1,), (1,)), ((), ())), preferred_element_type=F32)


def dot_nn(a, b):
    return lax.dot_general(a, b, (((1,), (0,)), ((), ())), preferred_element_type=F32)


def pack_stats(row_max, row_sum):
    rows = row_max.shape[0]
    lane = lax.broadcasted_iota(jnp.int32, (rows, 128), 1)
    both = jnp.where(lane == 0, row_max, jnp.where(lane == 1, row_sum, 0.0))
    return jnp.transpose(both)[:8]


def unpack_stats(packed):
    rows = packed.shape[1]
    both = jnp.transpose(jnp.concatenate([packed, jnp.zeros((120, rows), F32)], axis=0))
    return both[:, 0:1], both[:, 1:2]


def merge(one, two):
    (num_a, max_a, sum_a), (num_b, max_b, sum_b) = one, two
    top = jnp.maximum(max_a, max_b)
    fac_a, fac_b = jnp.exp2(max_a - top), jnp.exp2(max_b - top)
    return num_a * fac_a + num_b * fac_b, top, sum_a * fac_a + sum_b * fac_b


def kernel(dims, hid_h, wq_h, wk_h, wv_h, wo_h, pk_h, pv_h, sk_h, sv_h, lens, out_v,
           hid, wq, wk, wv, wo, raw, flat, kpre, vpre, qg, q8, knew, vnew,
           ring_k, ring_v, qbd, sufs, sufp, scores, own_num, own_st, hold_num, hold_st, xres,
           so8, sst8, xs_num, xs_st, xr_num, xr_st, att, yhold, ys, yr, yblk,
           s_hid, s_wq, s_wkv, s_wo, s_raw, s_rawsend, s_rawrecv, s_ring, s_res, s_ress, s_resr, s_as, s_ar,
           s_qs, s_qr, s_xs, s_xr, s_xst, s_xrt, s_ys, s_yr, s_gs, s_gr):
    n_ctx, n_y, kv_n, grp = dims
    rows = hid.shape[0]
    width = hid.shape[1]
    head = kpre.shape[-1]
    heads = kv_n * grp
    local_pos = raw.shape[2] // kv_n
    scale = head ** -0.5 * math.log2(math.e)
    blk = width // n_y
    half = blk // 2
    part_rows = rows // 2
    stack = grp * part_rows

    ctx = lax.axis_index('ctx')
    ypos = lax.axis_index('heads')
    right = {'ctx': lax.rem(ctx + 2, n_ctx)}
    left = {'ctx': lax.rem(ctx + n_ctx - 2, n_ctx)}
    core = lax.rem(ctx, 2)
    partner = {'ctx': ctx + 1 - 2 * core}
    below, above = lax.rem(ypos + n_y - 1, n_y), lax.rem(ypos + 1, n_y)
    up, down = {'heads': above}, {'heads': below}
    up_cores = [{'heads': above, 'ctx': ctx - core + c} for c in range(2)]
    down_cores = [{'heads': below, 'ctx': ctx - core + c} for c in range(2)]
    up_other = {'heads': above, 'ctx': ctx + 1 - 2 * core}
    down_other = {'heads': below, 'ctx': ctx + 1 - 2 * core}
    chunks = ((0, rows // 2), (rows // 2, rows // 4), (3 * rows // 4, rows // 4))

    def remote(src, dst, send, recv, where):
        return pltpu.make_async_remote_copy(src_ref=src, dst_ref=dst, send_sem=send, recv_sem=recv,
                                            device_id=where, device_id_type=MESH)

    c_hid = pltpu.make_async_copy(hid_h, hid, s_hid)
    c_raw = [pltpu.make_async_copy(src, raw.at[0, i], s_raw.at[i]) for i, src in enumerate((pk_h, pv_h))]
    deep = width // PIECES
    c_wq = [pltpu.make_async_copy(wq_h.at[pl.ds(k * deep, deep), pl.ds(kv * grp * head, grp * head)],
                                  wq.at[kv, pl.ds(k * deep, deep), :], s_wq.at[kv, k])
            for kv in range(kv_n) for k in range(PIECES)]
    c_wkv = [pltpu.make_async_copy(src, dst, s_wkv.at[i]) for i, (src, dst) in enumerate(((wk_h, wk), (wv_h, wv)))]
    c_wo = []
    for r in range(n_y):
        col = pl.multiple_of(lax.rem(ypos + r, n_y) * blk + core * half, 128)
        c_wo.append(pltpu.make_async_copy(wo_h.at[:, pl.ds(col, half)], wo.at[r], s_wo.at[r]))
    n_groups = rows // GROUP

    def ring_copies(group):
        seqs = pl.ds(group * GROUP, GROUP)
        slot = group % RING
        return (pltpu.make_async_copy(sk_h.at[seqs], ring_k.at[slot], s_ring.at[slot, 0]),
                pltpu.make_async_copy(sv_h.at[seqs], ring_v.at[slot], s_ring.at[slot, 1]))

    def start(copies):
        for c in copies:
            c.start()

    def wait(copies):
        for c in copies:
            c.wait()

    queue = c_wq + c_raw + c_wkv

    def advance():
        if queue:
            queue.pop(0).start()

    c_hid.start()
    for _ in range(6):
        advance()

    barrier = pltpu.get_barrier_semaphore()
    for where in (partner, left, right, up, down, up_other, down_other):
        pl.semaphore_signal(barrier, inc=1, device_id=where, device_id_type=MESH)

    def deinterleave(which):
        for i, dst in enumerate((kpre, vpre)):
            flat[...] = raw[which, i].astype(F32)
            for kv in range(kv_n):
                dst[kv, pl.ds(which * local_pos, local_pos), :] = flat[pl.ds(kv, local_pos, stride=kv_n), :].astype(BF16)

    def queries(kv):
        total = None
        for k in range(PIECES):
            c_wq[kv * PIECES + k].wait()
            advance()
            at = pl.ds(k * deep, deep)
            term = dot_nn(hid[:, at], wq[kv, at, :])
            total = term if total is None else total + term
        part = total.astype(BF16)
        qg[0, kv] = part
        for g in range(grp):
            q8[pl.ds(kv * grp + g, rows, stride=heads), :] = part[:, g * head:(g + 1) * head].astype(F32)

    def send_queries(kv):
        pair = (remote(qg.at[0, kv], qg.at[1, kv], s_qs.at[0, kv], s_qr.at[1, kv], right),
                remote(qg.at[0, kv], qg.at[2, kv], s_qs.at[1, kv], s_qr.at[2, kv], left))
        start(pair)
        return pair

    with jax.named_scope('w_c_hidwait'):
        c_hid.wait()
    with jax.named_scope('queries_'+str(0)):
        queries(0)
    with jax.named_scope('w_plsemaphore_wa'):
        pl.semaphore_wait(barrier, 7)
    q_copies = [send_queries(0)]
    c_swap = [remote(src, raw.at[1, i], s_rawsend.at[i], s_rawrecv.at[i], partner) for i, src in enumerate((pk_h, pv_h))]
    start(c_swap)
    c_res = [pltpu.make_async_copy(hid_h.at[:, pl.ds(pl.multiple_of(ypos * blk + core * half, 128), half)], xres.at[core], s_res),
             remote(hid_h.at[:, pl.ds(pl.multiple_of(ypos * blk + (1 - core) * half, 128), half)], xres.at[core], s_ress, s_resr, partner)]
    start(c_res)
    with jax.named_scope('queries_'+str(1)):
        queries(1)
    q_copies.append(send_queries(1))
    while queue:
        advance()
    with jax.named_scope('w_waitc_raw'):
        wait(c_raw)
    with jax.named_scope('deinterleave_'+str(0)):
        deinterleave(0)

    with jax.named_scope('w_waitc_wkv'):
        wait(c_wkv)
    start(ring_copies(0))
    with jax.named_scope('kv'):
        knew[...] = dot_nn(hid[...], wk[...]).astype(BF16).astype(F32)
    with jax.named_scope('kv'):
        vnew[...] = dot_nn(hid[...], wv[...]).astype(BF16).astype(F32)

    with jax.named_scope('w_waitc_swap'):
        wait(c_swap)
    with jax.named_scope('deinterleave_'+str(1)):
        deinterleave(1)
    start(ring_copies(1))
    for r in (n_y // 2, 1, n_y - 1, 0):
        c_wo[r].start()

    n_pos = kpre.shape[1]

    n_pieces = n_pos // POS_CHUNK
    part_lanes = POS_CHUNK // 128

    def prefix_states(jobs):
        stacked, run, out = [None] * len(jobs), [None] * len(jobs), []

        def score(i, c):
            sources, kv = jobs[i]
            if c == 0:
                stacked[i] = jnp.concatenate([qg[slot, kv, pl.ds(chunk * part_rows, part_rows), pl.ds(g * head, head)]
                                              for slot, chunk in sources for g in range(grp)], axis=0)
            at = pl.ds(c * POS_CHUNK, POS_CHUNK)
            s = dot_nt(stacked[i], kpre[kv, at, :])
            scores[i % 2, :, at] = s
            for t in range(part_lanes):
                piece = s[:, t * 128:(t + 1) * 128]
                run[i] = piece if run[i] is None else jnp.maximum(run[i], piece)

        for c in range(n_pieces):
            score(0, c)
        for i, (sources, kv) in enumerate(jobs):
            row_max = jnp.max(run[i], axis=1, keepdims=True) * scale
            wide_max = jnp.broadcast_to(row_max, (2 * stack, 128))
            wide_max = jnp.concatenate([wide_max] * part_lanes, axis=1)
            total, num = None, None
            for c in range(n_pieces):
                if i + 1 < len(jobs):
                    score(i + 1, c)
                at = pl.ds(c * POS_CHUNK, POS_CHUNK)
                p = jnp.exp2(scores[i % 2, :, at] * scale - wide_max)
                for t in range(part_lanes):
                    piece = p[:, t * 128:(t + 1) * 128]
                    total = piece if total is None else total + piece
                term = dot_nn(p.astype(BF16), vpre[kv, at, :])
                num = term if num is None else num + term
            row_sum = jnp.sum(total, axis=1, keepdims=True)
            out += [(num[:stack], row_max[:stack], row_sum[:stack]), (num[stack:], row_max[stack:], row_sum[stack:])]
        return out

    sent = []

    def x_copies(i, where):
        return (remote(xs_num.at[i], xr_num.at[i], s_xs.at[i], s_xr.at[i], where),
                remote(xs_st.at[i], xr_st.at[i], s_xst.at[i], s_xrt.at[i], where))

    def post(state, i, where):
        xs_num[i] = state[0]
        xs_st[i] = pack_stats(state[1], state[2])
        out = x_copies(i, where)
        start(out)
        sent.extend(out)

    def arrived(i):
        return (xr_num[i],) + unpack_stats(xr_st[i])

    def keep(refs, i, state):
        refs[0][i] = state[0]
        lane = lax.broadcasted_iota(jnp.int32, state[0].shape, 1)
        refs[1][i] = jnp.where(lane == 0, state[1], state[2])

    def kept(refs, i):
        return refs[0][i], refs[1][i][:, 0:1], refs[1][i][:, 1:2]

    own = (own_num, own_st)
    hold = (hold_num, hold_st)

    def prefix_near(chunk):
        base = 6 * chunk
        both = ((2, chunk), (1, chunk))
        right_1, left_1, right_0, left_0 = prefix_states([(both, 1), (both, 0)])
        post(right_1, base, right)
        post(left_0, base + 1, left)
        keep(hold, 1, left_1)
        keep(hold, 0, right_0)

    def prefix_far():
        both = ((3, 0), (3, 1))
        states = prefix_states([(both, 0), (both, 1)])
        for chunk in range(2):
            post(states[chunk], 6 * chunk + 2, right)
            post(states[2 + chunk], 6 * chunk + 3, left)

    def prefix_own():
        both = ((0, 0), (0, 1))
        for i, state in enumerate(prefix_states([(both, 0), (both, 1)])):
            keep(own, i, state)

    def relay(chunk):
        base = 6 * chunk
        for i, where in ((base + 2, right), (base + 3, left)):
            for c in x_copies(i, where):
                c.wait_recv()
        to_right, to_left = (merge(arrived(base + 2 + i), kept(hold, i)) for i in range(2))
        post(to_right, base + 4, right)
        post(to_left, base + 5, left)

    lines = GROUP * heads
    span = ring_k.shape[2]
    tile = span // 4

    def suffix_group(group):
        slot = group % RING
        lane = lax.broadcasted_iota(jnp.int32, (head, lines), 1)
        q_t = jnp.transpose(q8[pl.ds(group * lines, lines), :])
        for j in range(GROUP // 2):
            both = [jnp.where(lane // heads == 2 * j + e, q_t, 0.0) for e in range(2)]
            qbd[j] = jnp.concatenate(both, axis=0).astype(BF16)
        one = lax.broadcasted_iota(jnp.int32, (1, lines), 1)
        length = jnp.zeros((1, lines), jnp.int32)
        for b in range(GROUP):
            length = jnp.where(one // heads == b, lens[group * GROUP + b], length)
        line = lax.broadcasted_iota(jnp.int32, (tile, lines), 0)
        lane = lax.broadcasted_iota(jnp.int32, (tile, lines), 1)
        mine = lax.rem(line, kv_n) == lax.rem(lane, heads) // grp
        place = jnp.where(mine, line // kv_n, span)
        wait(ring_copies(group))
        run = jnp.full((1, lines), LOW, F32)
        for c in range(4):
            at = pl.ds(c * tile, tile)
            s = None
            for j in range(GROUP // 2):
                keys = jnp.concatenate([ring_k[slot, 2 * j, at, :], ring_k[slot, 2 * j + 1, at, :]], axis=1)
                term = dot_nn(keys, qbd[j])
                s = term if s is None else s + term
            s = jnp.where(place < length - c * (tile // kv_n), s * scale, -jnp.inf)
            sufs[at, :] = s
            run = jnp.maximum(run, jnp.max(s, axis=0, keepdims=True))
        total = jnp.zeros((1, lines), F32)
        for c in range(4):
            p = jnp.exp2(sufs[pl.ds(c * tile, tile), :] - run)
            total = total + jnp.sum(p, axis=0, keepdims=True)
            sufp[:, pl.ds(c * tile, tile)] = jnp.transpose(p).astype(BF16)
        stats = jnp.concatenate([run, total, jnp.zeros((head - 2, lines), F32)], axis=0)
        sst8[pl.ds(group * lines, lines), :] = jnp.transpose(stats)
        for j in range(GROUP // 2):
            weights = sufp[pl.ds(2 * j * heads, 2 * heads), :]
            for e in range(2):
                o = dot_nn(weights, ring_v[slot, 2 * j + e])
                so8[pl.ds(group * lines + (2 * j + e) * heads, heads), :] = o[e * heads:(e + 1) * heads]
        if group + RING < n_groups:
            start(ring_copies(group + RING))

    def merge_prefix(chunk):
        base = 6 * chunk
        for i, where in ((base + 1, left), (base + 4, right), (base, right), (base + 5, left)):
            for c in x_copies(i, where):
                c.wait_recv()
        merged = [functools.reduce(merge, [kept(own, chunk), arrived(base + 1), arrived(base + 4)]),
                  functools.reduce(merge, [kept(own, 2 + chunk), arrived(base), arrived(base + 5)])]
        for kv in range(kv_n):
            keep(own, 2 * kv + chunk, merged[kv])

    def att_copy(chunk):
        first, n = chunks[chunk]
        ref = att.at[core, pl.ds(first, n), :]
        return remote(ref, ref, s_as.at[chunk], s_ar.at[chunk], partner)

    def combine(chunk):
        first, n = chunks[chunk]
        at_rows = pl.ds(first, n)
        which, off = first // part_rows, first % part_rows
        for kv in range(kv_n):
            rest = []
            for g in range(grp):
                every = pl.ds(first * heads + kv * grp + g, n, stride=heads)
                stats = sst8[every, :]
                pre_at = pl.ds(g * part_rows + off, n)
                pre = own_st[2 * kv + which, pre_at, :]
                rest.append((so8[every, :], stats[:, 0:1], stats[:, 1:2], q8[every, :],
                             own_num[2 * kv + which, pre_at, :], pre[:, 0:1], pre[:, 1:2]))
            num, top, tot, qs, pre_num, pre_top, pre_tot = (jnp.concatenate(list(v), axis=0) for v in zip(*rest))
            state = merge((pre_num, pre_top, pre_tot), (num, top, tot))
            kn = jnp.concatenate([knew[at_rows, pl.ds(kv * head, head)]] * grp, axis=0)
            vn = jnp.concatenate([vnew[at_rows, pl.ds(kv * head, head)]] * grp, axis=0)
            s_new = jnp.sum(qs * kn, axis=1, keepdims=True) * scale
            state = merge(state, (vn, s_new, jnp.ones_like(s_new)))
            res = (state[0] / state[2]).astype(BF16)
            for g in range(grp):
                att[core, at_rows, pl.ds((kv * grp + g) * head, head)] = res[g * n:(g + 1) * n]
        c = att_copy(chunk)
        c.start()
        sent.append(c)

    ysent = []

    def y_copy(chunk, i, where):
        at = pl.ds(0, chunks[chunk][1])
        return remote(ys.at[i, at], yr.at[i, at], s_ys.at[i], s_yr.at[i], where)

    def y_post(chunk, val, i, where):
        ys[i, :val.shape[0]] = val
        c = y_copy(chunk, i, where)
        c.start()
        ysent.append(c)

    def project(chunk):
        base = 6 * chunk
        first, n = chunks[chunk]
        att_copy(chunk).wait_recv()
        both = jnp.concatenate([att[c, pl.ds(first, n), :] for c in range(2)], axis=0)

        def y_part(r):
            if chunk == 0:
                c_wo[r].wait()
            val = dot_nn(both, wo[r])
            return val[:n], val[n:]

        one, two = y_part(n_y // 2)
        y_post(chunk, one, base, up)
        y_post(chunk, two, base + 1, down)
        one, two = y_part(1)
        y_post(chunk, two, base + 2, up)
        yhold[chunk, 0, :n] = one
        one, two = y_part(n_y - 1)
        y_post(chunk, one, base + 3, down)
        yhold[chunk, 1, :n] = two
        one, two = y_part(0)
        yhold[chunk, 2, :n] = one
        yhold[chunk, 3, :n] = two

    def y_relay(chunk):
        base = 6 * chunk
        n = chunks[chunk][1]
        y_copy(chunk, base, up).wait_recv()
        y_post(chunk, yhold[chunk, 0, :n] + yr[base, :n], base + 4, up)
        y_copy(chunk, base + 1, down).wait_recv()
        y_post(chunk, yhold[chunk, 1, :n] + yr[base + 1, :n], base + 5, down)

    gsend = []

    def region(chunk, dest, which):
        first, n = chunks[chunk]
        return out_v.at[pl.ds(first, n), pl.ds(pl.multiple_of(dest * blk + which * half, 128), half)]

    def g_start(src, dst, chunk, slot, which, sem, where):
        c = remote(src, dst, s_gs.at[chunk, sem], s_gr.at[chunk, slot, which], where)
        c.start()
        gsend.append(c)

    def g_wait(chunk, slot, which):
        ref = region(chunk, ypos, 0)
        remote(ref, ref, s_gs.at[chunk, 0], s_gr.at[chunk, slot, which], up).wait_recv()

    def finish(chunk):
        base = 6 * chunk
        first, n = chunks[chunk]
        mine = region(chunk, ypos, core)
        done = []
        for c, (near, merged) in enumerate(((base + 3, base + 4), (base + 2, base + 5))):
            val = yhold[chunk, 2 + c, :n]
            for i in (near, merged):
                y_copy(chunk, i, up if i % 2 == 0 else down).wait_recv()
                val = val + yr[i, :n]
            val = (val + xres[c, pl.ds(first, n), :].astype(F32)).astype(BF16)
            yblk[chunk, c, :n] = val
            src = yblk.at[chunk, c, pl.ds(0, n)]
            order = ((0, up_cores[c]), (1, down_cores[c]))
            for slot, where in (order if c == 0 else order[::-1]):
                g_start(src, mine, chunk, slot, core, 2 * c + slot, where)
            done.append(val)
        col = pl.multiple_of(ypos * blk + core * half, 128)
        out_v[pl.ds(first, n), pl.ds(col, half)] = jnp.where(core == 0, done[0], done[1])
        g_start(yblk.at[chunk, 1 - core, pl.ds(0, n)], mine, chunk, 3, core, 4, partner)

    def forward(chunk):
        g_wait(chunk, 0, 0)
        ref = region(chunk, below, 0)
        g_start(ref, ref, chunk, 2, 0, 5, up)
        g_wait(chunk, 1, 1)
        ref = region(chunk, above, 1)
        g_start(ref, ref, chunk, 2, 1, 6, down)

    def collect(chunk):
        g_wait(chunk, 0, 1)
        g_wait(chunk, 1, 0)
        g_wait(chunk, 3, 1 - core)
        g_wait(chunk, 2, 0)
        g_wait(chunk, 2, 1)

    with jax.named_scope('prefix_own_'+str('')):
        prefix_own()
    with jax.named_scope('w_q_copies00wait'):
        q_copies[0][0].wait_recv()
    fwd_right = remote(qg.at[1, 0], qg.at[3, 0], s_qs.at[2, 0], s_qr.at[3, 0], right)
    fwd_right.start()
    with jax.named_scope('w_q_copies11wait'):
        q_copies[1][1].wait_recv()
    fwd_left = remote(qg.at[2, 1], qg.at[3, 1], s_qs.at[2, 1], s_qr.at[3, 1], left)
    fwd_left.start()
    with jax.named_scope('w_q_copies10wait'):
        q_copies[1][0].wait_recv()
    with jax.named_scope('w_q_copies01wait'):
        q_copies[0][1].wait_recv()

    per_part = n_groups // 2
    with jax.named_scope('prefix_near_'+str(0)):
        prefix_near(0)
    with jax.named_scope('w_fwd_rightwait_'):
        fwd_right.wait_recv()
    with jax.named_scope('w_fwd_leftwait_r'):
        fwd_left.wait_recv()
    with jax.named_scope('prefix_far_'+str('')):
        prefix_far()
    for group in range(per_part):
        with jax.named_scope('suffix_group_'+str(group)):
            suffix_group(group)
    with jax.named_scope('relay_'+str(0)):
        relay(0)
    with jax.named_scope('prefix_near_'+str(1)):
        prefix_near(1)
    with jax.named_scope('merge_prefix_'+str(0)):
        merge_prefix(0)
    with jax.named_scope('combine_'+str(0)):
        combine(0)
    with jax.named_scope('relay_'+str(1)):
        relay(1)
    with jax.named_scope('w_waitc_res'):
        wait(c_res)
    with jax.named_scope('project_'+str(0)):
        project(0)

    with jax.named_scope('suffix_group_'+str(per_part)):
        suffix_group(per_part)
    with jax.named_scope('merge_prefix_'+str(1)):
        merge_prefix(1)
    with jax.named_scope('combine_'+str(1)):
        combine(1)
    with jax.named_scope('y_relay_'+str(0)):
        y_relay(0)
    with jax.named_scope('suffix_group_'+str(per_part + 1)):
        suffix_group(per_part + 1)
    with jax.named_scope('project_'+str(1)):
        project(1)
    with jax.named_scope('finish_'+str(0)):
        finish(0)
    with jax.named_scope('combine_'+str(2)):
        combine(2)
    with jax.named_scope('y_relay_'+str(1)):
        y_relay(1)
    with jax.named_scope('forward_'+str(0)):
        forward(0)
    with jax.named_scope('project_'+str(2)):
        project(2)
    with jax.named_scope('finish_'+str(1)):
        finish(1)
    with jax.named_scope('y_relay_'+str(2)):
        y_relay(2)
    with jax.named_scope('forward_'+str(1)):
        forward(1)
    with jax.named_scope('finish_'+str(2)):
        finish(2)
    with jax.named_scope('forward_'+str(2)):
        forward(2)
    with jax.named_scope('collect_'+str(0)):
        collect(0)
    with jax.named_scope('collect_'+str(1)):
        collect(1)
    with jax.named_scope('collect_'+str(2)):
        collect(2)

    for pair in q_copies:
        for c in pair:
            c.wait_send()
    for c in [fwd_right, fwd_left] + sent + ysent + gsend:
        c.wait_send()


def store(src, dst, sem):
    c = pltpu.make_async_copy(src, dst, sem)
    c.start()
    c.wait()


def solution(mesh):
    n_ctx, n_y = mesh.shape['ctx'], mesh.shape['heads']
    row_spec = P(('dp', 'ctx'), None)
    col_spec = P(None, 'heads')
    pre_spec = P(('dp', 'ctx'), 'heads', None)
    suf_spec = P(('dp', 'ctx'), None, 'heads', None)

    def local_step(hidden, w_query, w_key, w_value, w_out, prefix_k, prefix_v, suffix_k, suffix_v, seq_lens):
        rows, width = hidden.shape
        pos, kv_n, head = prefix_k.shape
        slots = suffix_k.shape[1]
        grp = w_query.shape[1] // (kv_n * head)
        heads = kv_n * grp
        blk = width // n_y
        half_rows = rows // 2
        stack = grp * half_rows
        lines = GROUP * heads
        dma = pltpu.SemaphoreType.DMA
        scratch = dict(
            hid=pltpu.VMEM((rows, width), BF16),
            wq=pltpu.VMEM((kv_n, width, grp * head), BF16),
            wk=pltpu.VMEM((width, kv_n * head), BF16),
            wv=pltpu.VMEM((width, kv_n * head), BF16),
            wo=pltpu.VMEM((n_y, heads * head, blk // 2), BF16),
            raw=pltpu.VMEM((2, 2, pos * kv_n, head), BF16),
            flat=pltpu.VMEM((pos * kv_n, head), F32),
            kpre=pltpu.VMEM((kv_n, 2 * pos, head), BF16),
            vpre=pltpu.VMEM((kv_n, 2 * pos, head), BF16),
            qg=pltpu.VMEM((4, kv_n, rows, grp * head), BF16),
            q8=pltpu.VMEM((rows * heads, head), F32),
            knew=pltpu.VMEM((rows, kv_n * head), F32),
            vnew=pltpu.VMEM((rows, kv_n * head), F32),
            ring_k=pltpu.VMEM((RING, GROUP, slots * kv_n, head), BF16),
            ring_v=pltpu.VMEM((RING, GROUP, slots * kv_n, head), BF16),
            qbd=pltpu.VMEM((GROUP // 2, 2 * head, lines), BF16),
            sufs=pltpu.VMEM((slots * kv_n, lines), F32),
            sufp=pltpu.VMEM((lines, slots * kv_n), BF16),
            scores=pltpu.VMEM((2, 2 * stack, 2 * pos), F32),
            own_num=pltpu.VMEM((2 * kv_n, stack, head), F32),
            own_st=pltpu.VMEM((2 * kv_n, stack, 128), F32),
            hold_num=pltpu.VMEM((2, stack, head), F32),
            hold_st=pltpu.VMEM((2, stack, 128), F32),
            xres=pltpu.VMEM((2, rows, blk // 2), BF16),
            so8=pltpu.VMEM((rows * heads, head), F32),
            sst8=pltpu.VMEM((rows * heads, head), F32),
            xs_num=pltpu.VMEM((12, stack, head), F32),
            xs_st=pltpu.VMEM((12, 8, stack), F32),
            xr_num=pltpu.VMEM((12, stack, head), F32),
            xr_st=pltpu.VMEM((12, 8, stack), F32),
            att=pltpu.VMEM((2, rows, heads * head), BF16),
            yhold=pltpu.VMEM((3, 4, half_rows, blk // 2), F32),
            ys=pltpu.VMEM((18, half_rows, blk // 2), F32),
            yr=pltpu.VMEM((18, half_rows, blk // 2), F32),
            yblk=pltpu.VMEM((3, 2, half_rows, blk // 2), BF16),
            s_hid=dma(()), s_wq=dma((kv_n, PIECES)), s_wkv=dma((2,)), s_wo=dma((n_y,)),
            s_raw=dma((2,)), s_rawsend=dma((2,)), s_rawrecv=dma((2,)), s_ring=dma((RING, 2)),
            s_res=dma(()), s_ress=dma(()), s_resr=dma(()), s_as=dma((3,)), s_ar=dma((3,)),
            s_qs=dma((3, kv_n)), s_qr=dma((4, kv_n)),
            s_xs=dma((12,)), s_xr=dma((12,)), s_xst=dma((12,)), s_xrt=dma((12,)),
            s_ys=dma((18,)), s_yr=dma((18,)), s_gs=dma((3, 7)), s_gr=dma((3, 4, 2)),
        )
        hbm = pl.BlockSpec(memory_space=pl.ANY)
        out = pl.pallas_call(
            functools.partial(kernel, (n_ctx, n_y, kv_n, grp)),
            out_shape=pltpu.VMEM((rows, width), BF16),
            in_specs=[hbm] * 9 + [pl.BlockSpec(memory_space=pltpu.SMEM)],
            out_specs=pl.BlockSpec(memory_space=pltpu.VMEM),
            scratch_shapes=list(scratch.values()),
            compiler_params=pltpu.CompilerParams(collective_id=0, has_side_effects=True, vmem_limit_bytes=VMEM_BYTES),
        )(hidden, w_query, w_key, w_value, w_out,
          prefix_k.reshape(pos * kv_n, head), prefix_v.reshape(pos * kv_n, head),
          suffix_k.reshape(rows, slots * kv_n, head), suffix_v.reshape(rows, slots * kv_n, head), seq_lens)
        return pl.pallas_call(
            store,
            out_shape=jax.ShapeDtypeStruct((rows, width), BF16),
            in_specs=[pl.BlockSpec(memory_space=pltpu.VMEM)],
            out_specs=hbm,
            scratch_shapes=[dma(())],
            compiler_params=pltpu.CompilerParams(vmem_limit_bytes=1048576),
        )(out)

    return jax.shard_map(local_step, mesh=mesh, in_specs=(row_spec, col_spec, col_spec, col_spec, P('heads', None), pre_spec, pre_spec, suf_spec, suf_spec, P(('dp', 'ctx'))), out_specs=row_spec, check_vma=False)
```

```python
import functools
import math
import jax
import jax.numpy as jnp
from jax import lax
from jax.experimental import pallas as pl
from jax.experimental.pallas import tpu as pltpu
from jax.sharding import PartitionSpec as P

MESH = pl.DeviceIdType.MESH
F32 = jnp.float32
BF16 = jnp.bfloat16
LOW = -3.0e38
GROUP = 16
RING = 2
POS_CHUNK = 512
PIECES = 5
IN_FLIGHT = 4
VMEM_BYTES = 66000000


def dot_nt(a, b):
    return lax.dot_general(a, b, (((1,), (1,)), ((), ())), preferred_element_type=F32)


def dot_nn(a, b):
    return lax.dot_general(a, b, (((1,), (0,)), ((), ())), preferred_element_type=F32)


def pack_stats(row_max, row_sum):
    rows = row_max.shape[0]
    lane = lax.broadcasted_iota(jnp.int32, (rows, 128), 1)
    both = jnp.where(lane == 0, row_max, jnp.where(lane == 1, row_sum, 0.0))
    return jnp.transpose(both)[:8]


def unpack_stats(packed):
    rows = packed.shape[1]
    both = jnp.transpose(jnp.concatenate([packed, jnp.zeros((120, rows), F32)], axis=0))
    return both[:, 0:1], both[:, 1:2]


def merge(one, two):
    (num_a, max_a, sum_a), (num_b, max_b, sum_b) = one, two
    top = jnp.maximum(max_a, max_b)
    fac_a, fac_b = jnp.exp2(max_a - top), jnp.exp2(max_b - top)
    return num_a * fac_a + num_b * fac_b, top, sum_a * fac_a + sum_b * fac_b


def kernel(dims, hid_h, wq_h, wk_h, wv_h, wo_h, pk_h, pv_h, sk_h, sv_h, lens, out_v,
           hid, wq, wk, wv, wo, raw, flat, kpre, vpre, qg, q8, knew, vnew,
           ring_k, ring_v, qbd, sufs, sufp, scores, own_num, own_st, hold_num, hold_st, xres,
           so8, sst8, xs_num, xs_st, xr_num, xr_st, att, yhold, ys, yr, yblk,
           s_hid, s_wq, s_wkv, s_wo, s_raw, s_rawsend, s_rawrecv, s_ring, s_res, s_ress, s_resr, s_as, s_ar,
           s_qs, s_qr, s_xs, s_xr, s_xst, s_xrt, s_ys, s_yr, s_gs, s_gr):
    n_ctx, n_y, kv_n, grp = dims
    rows = hid.shape[0]
    width = hid.shape[1]
    head = kpre.shape[-1]
    heads = kv_n * grp
    local_pos = raw.shape[2] // kv_n
    scale = head ** -0.5 * math.log2(math.e)
    blk = width // n_y
    half = blk // 2
    part_rows = rows // 2
    stack = grp * part_rows

    ctx = lax.axis_index('ctx')
    ypos = lax.axis_index('heads')
    right = {'ctx': lax.rem(ctx + 2, n_ctx)}
    left = {'ctx': lax.rem(ctx + n_ctx - 2, n_ctx)}
    core = lax.rem(ctx, 2)
    partner = {'ctx': ctx + 1 - 2 * core}
    below, above = lax.rem(ypos + n_y - 1, n_y), lax.rem(ypos + 1, n_y)
    up, down = {'heads': above}, {'heads': below}
    up_cores = [{'heads': above, 'ctx': ctx - core + c} for c in range(2)]
    down_cores = [{'heads': below, 'ctx': ctx - core + c} for c in range(2)]
    up_other = {'heads': above, 'ctx': ctx + 1 - 2 * core}
    down_other = {'heads': below, 'ctx': ctx + 1 - 2 * core}
    chunks = ((0, rows // 2), (rows // 2, rows // 4), (3 * rows // 4, rows // 4))

    def remote(src, dst, send, recv, where):
        return pltpu.make_async_remote_copy(src_ref=src, dst_ref=dst, send_sem=send, recv_sem=recv,
                                            device_id=where, device_id_type=MESH)

    c_hid = pltpu.make_async_copy(hid_h, hid, s_hid)
    c_raw = [pltpu.make_async_copy(src, raw.at[0, i], s_raw.at[i]) for i, src in enumerate((pk_h, pv_h))]
    deep = width // PIECES
    c_wq = [pltpu.make_async_copy(wq_h.at[pl.ds(k * deep, deep), pl.ds(kv * grp * head, grp * head)],
                                  wq.at[kv, pl.ds(k * deep, deep), :], s_wq.at[kv, k])
            for kv in range(kv_n) for k in range(PIECES)]
    c_wkv = [pltpu.make_async_copy(src, dst, s_wkv.at[i]) for i, (src, dst) in enumerate(((wk_h, wk), (wv_h, wv)))]
    c_wo = []
    for r in range(n_y):
        col = pl.multiple_of(lax.rem(ypos + r, n_y) * blk + core * half, 128)
        c_wo.append(pltpu.make_async_copy(wo_h.at[:, pl.ds(col, half)], wo.at[r], s_wo.at[r]))
    n_groups = rows // GROUP

    def ring_copies(group):
        seqs = pl.ds(group * GROUP, GROUP)
        slot = group % RING
        return (pltpu.make_async_copy(sk_h.at[seqs], ring_k.at[slot], s_ring.at[slot, 0]),
                pltpu.make_async_copy(sv_h.at[seqs], ring_v.at[slot], s_ring.at[slot, 1]))

    def start(copies):
        for c in copies:
            c.start()

    def wait(copies):
        for c in copies:
            c.wait()

    queue = c_wq + c_raw + c_wkv

    def advance():
        if queue:
            queue.pop(0).start()

    c_hid.start()
    for _ in range(IN_FLIGHT):
        advance()

    barrier = pltpu.get_barrier_semaphore()
    for where in (partner, left, right, up, down, up_other, down_other):
        pl.semaphore_signal(barrier, inc=1, device_id=where, device_id_type=MESH)

    def deinterleave(which):
        for i, dst in enumerate((kpre, vpre)):
            flat[...] = raw[which, i].astype(F32)
            for kv in range(kv_n):
                dst[kv, pl.ds(which * local_pos, local_pos), :] = flat[pl.ds(kv, local_pos, stride=kv_n), :].astype(BF16)

    def queries(kv):
        total = None
        for k in range(PIECES):
            c_wq[kv * PIECES + k].wait()
            advance()
            at = pl.ds(k * deep, deep)
            term = dot_nn(hid[:, at], wq[kv, at, :])
            total = term if total is None else total + term
        part = total.astype(BF16)
        qg[0, kv] = part
        for g in range(grp):
            q8[pl.ds(kv * grp + g, rows, stride=heads), :] = part[:, g * head:(g + 1) * head].astype(F32)

    def send_queries(kv):
        pair = (remote(qg.at[0, kv], qg.at[1, kv], s_qs.at[0, kv], s_qr.at[1, kv], right),
                remote(qg.at[0, kv], qg.at[2, kv], s_qs.at[1, kv], s_qr.at[2, kv], left))
        start(pair)
        return pair

    c_hid.wait()
    queries(0)
    pl.semaphore_wait(barrier, 7)
    q_copies = [send_queries(0)]
    c_swap = [remote(src, raw.at[1, i], s_rawsend.at[i], s_rawrecv.at[i], partner) for i, src in enumerate((pk_h, pv_h))]
    start(c_swap)
    c_res = [pltpu.make_async_copy(hid_h.at[:, pl.ds(pl.multiple_of(ypos * blk + core * half, 128), half)], xres.at[core], s_res),
             remote(hid_h.at[:, pl.ds(pl.multiple_of(ypos * blk + (1 - core) * half, 128), half)], xres.at[core], s_ress, s_resr, partner)]
    start(c_res)
    queries(1)
    q_copies.append(send_queries(1))
    while queue:
        advance()
    wait(c_raw)
    deinterleave(0)

    wait(c_swap)
    deinterleave(1)
    start(ring_copies(0))

    n_pos = kpre.shape[1]

    n_pieces = n_pos // POS_CHUNK
    part_lanes = POS_CHUNK // 128

    def prefix_states(jobs):
        stacked, run, out = [None] * len(jobs), [None] * len(jobs), []

        def score(i, c):
            sources, kv = jobs[i]
            if c == 0:
                stacked[i] = jnp.concatenate([qg[slot, kv, pl.ds(chunk * part_rows, part_rows), pl.ds(g * head, head)]
                                              for slot, chunk in sources for g in range(grp)], axis=0)
            at = pl.ds(c * POS_CHUNK, POS_CHUNK)
            s = dot_nt(stacked[i], kpre[kv, at, :])
            scores[i % 2, :, at] = s
            for t in range(part_lanes):
                piece = s[:, t * 128:(t + 1) * 128]
                run[i] = piece if run[i] is None else jnp.maximum(run[i], piece)

        for c in range(n_pieces):
            score(0, c)
        for i, (sources, kv) in enumerate(jobs):
            row_max = jnp.max(run[i], axis=1, keepdims=True) * scale
            wide_max = jnp.broadcast_to(row_max, (2 * stack, 128))
            wide_max = jnp.concatenate([wide_max] * part_lanes, axis=1)
            total, num = None, None
            for c in range(n_pieces):
                if i + 1 < len(jobs):
                    score(i + 1, c)
                at = pl.ds(c * POS_CHUNK, POS_CHUNK)
                p = jnp.exp2(scores[i % 2, :, at] * scale - wide_max)
                for t in range(part_lanes):
                    piece = p[:, t * 128:(t + 1) * 128]
                    total = piece if total is None else total + piece
                term = dot_nn(p.astype(BF16), vpre[kv, at, :])
                num = term if num is None else num + term
            row_sum = jnp.sum(total, axis=1, keepdims=True)
            out += [(num[:stack], row_max[:stack], row_sum[:stack]), (num[stack:], row_max[stack:], row_sum[stack:])]
        return out

    sent = []

    def x_copies(i, where):
        return (remote(xs_num.at[i], xr_num.at[i], s_xs.at[i], s_xr.at[i], where),
                remote(xs_st.at[i], xr_st.at[i], s_xst.at[i], s_xrt.at[i], where))

    def post(state, i, where):
        xs_num[i] = state[0]
        xs_st[i] = pack_stats(state[1], state[2])
        out = x_copies(i, where)
        start(out)
        sent.extend(out)

    def arrived(i):
        return (xr_num[i],) + unpack_stats(xr_st[i])

    def keep(refs, i, state):
        refs[0][i] = state[0]
        lane = lax.broadcasted_iota(jnp.int32, state[0].shape, 1)
        refs[1][i] = jnp.where(lane == 0, state[1], state[2])

    def kept(refs, i):
        return refs[0][i], refs[1][i][:, 0:1], refs[1][i][:, 1:2]

    own = (own_num, own_st)
    hold = (hold_num, hold_st)

    def prefix_near(chunk):
        base = 6 * chunk
        both = ((2, chunk), (1, chunk))
        right_1, left_1, right_0, left_0 = prefix_states([(both, 1), (both, 0)])
        post(right_1, base, right)
        post(left_0, base + 1, left)
        keep(hold, 2 * chunk + 1, left_1)
        keep(hold, 2 * chunk, right_0)

    def prefix_far():
        both = ((3, 0), (3, 1))
        states = prefix_states([(both, 0), (both, 1)])
        for chunk in range(2):
            post(states[chunk], 6 * chunk + 2, right)
            post(states[2 + chunk], 6 * chunk + 3, left)

    def prefix_own():
        both = ((0, 0), (0, 1))
        for i, state in enumerate(prefix_states([(both, 0), (both, 1)])):
            keep(own, i, state)

    def relay(chunk):
        base = 6 * chunk
        for i, where in ((base + 2, right), (base + 3, left)):
            for c in x_copies(i, where):
                c.wait_recv()
        to_right, to_left = (merge(arrived(base + 2 + i), kept(hold, 2 * chunk + i)) for i in range(2))
        post(to_right, base + 4, right)
        post(to_left, base + 5, left)

    lines = GROUP * heads
    span = ring_k.shape[2]
    tile = span // 4

    def suffix_group(group):
        slot = group % RING
        lane = lax.broadcasted_iota(jnp.int32, (head, lines), 1)
        q_t = jnp.transpose(q8[pl.ds(group * lines, lines), :])
        for j in range(GROUP // 2):
            both = [jnp.where(lane // heads == 2 * j + e, q_t, 0.0) for e in range(2)]
            qbd[j] = jnp.concatenate(both, axis=0).astype(BF16)
        one = lax.broadcasted_iota(jnp.int32, (1, lines), 1)
        length = jnp.zeros((1, lines), jnp.int32)
        for b in range(GROUP):
            length = jnp.where(one // heads == b, lens[group * GROUP + b], length)
        line = lax.broadcasted_iota(jnp.int32, (tile, lines), 0)
        lane = lax.broadcasted_iota(jnp.int32, (tile, lines), 1)
        mine = lax.rem(line, kv_n) == lax.rem(lane, heads) // grp
        place = jnp.where(mine, line // kv_n, span)
        wait(ring_copies(group))
        run = jnp.full((1, lines), LOW, F32)
        for c in range(4):
            at = pl.ds(c * tile, tile)
            s = None
            for j in range(GROUP // 2):
                keys = jnp.concatenate([ring_k[slot, 2 * j, at, :], ring_k[slot, 2 * j + 1, at, :]], axis=1)
                term = dot_nn(keys, qbd[j])
                s = term if s is None else s + term
            s = jnp.where(place < length - c * (tile // kv_n), s * scale, -jnp.inf)
            sufs[at, :] = s
            run = jnp.maximum(run, jnp.max(s, axis=0, keepdims=True))
        total = jnp.zeros((1, lines), F32)
        for c in range(4):
            p = jnp.exp2(sufs[pl.ds(c * tile, tile), :] - run)
            total = total + jnp.sum(p, axis=0, keepdims=True)
            sufp[:, pl.ds(c * tile, tile)] = jnp.transpose(p).astype(BF16)
        stats = jnp.concatenate([run, total, jnp.zeros((head - 2, lines), F32)], axis=0)
        sst8[pl.ds(group * lines, lines), :] = jnp.transpose(stats)
        for j in range(GROUP // 2):
            weights = sufp[pl.ds(2 * j * heads, 2 * heads), :]
            for e in range(2):
                o = dot_nn(weights, ring_v[slot, 2 * j + e])
                so8[pl.ds(group * lines + (2 * j + e) * heads, heads), :] = o[e * heads:(e + 1) * heads]
        if group + RING < n_groups:
            start(ring_copies(group + RING))

    def merge_prefix(chunk):
        base = 6 * chunk
        for i, where in ((base + 1, left), (base + 4, right), (base, right), (base + 5, left)):
            for c in x_copies(i, where):
                c.wait_recv()
        merged = [functools.reduce(merge, [kept(own, chunk), arrived(base + 1), arrived(base + 4)]),
                  functools.reduce(merge, [kept(own, 2 + chunk), arrived(base), arrived(base + 5)])]
        for kv in range(kv_n):
            keep(own, 2 * kv + chunk, merged[kv])

    def att_copy(chunk):
        first, n = chunks[chunk]
        ref = att.at[core, pl.ds(first, n), :]
        return remote(ref, ref, s_as.at[chunk], s_ar.at[chunk], partner)

    def combine(chunk):
        first, n = chunks[chunk]
        at_rows = pl.ds(first, n)
        which, off = first // part_rows, first % part_rows
        for kv in range(kv_n):
            rest = []
            for g in range(grp):
                every = pl.ds(first * heads + kv * grp + g, n, stride=heads)
                stats = sst8[every, :]
                pre_at = pl.ds(g * part_rows + off, n)
                pre = own_st[2 * kv + which, pre_at, :]
                rest.append((so8[every, :], stats[:, 0:1], stats[:, 1:2], q8[every, :],
                             own_num[2 * kv + which, pre_at, :], pre[:, 0:1], pre[:, 1:2]))
            num, top, tot, qs, pre_num, pre_top, pre_tot = (jnp.concatenate(list(v), axis=0) for v in zip(*rest))
            state = merge((pre_num, pre_top, pre_tot), (num, top, tot))
            kn = jnp.concatenate([knew[at_rows, pl.ds(kv * head, head)]] * grp, axis=0)
            vn = jnp.concatenate([vnew[at_rows, pl.ds(kv * head, head)]] * grp, axis=0)
            s_new = jnp.sum(qs * kn, axis=1, keepdims=True) * scale
            state = merge(state, (vn, s_new, jnp.ones_like(s_new)))
            res = (state[0] / state[2]).astype(BF16)
            for g in range(grp):
                att[core, at_rows, pl.ds((kv * grp + g) * head, head)] = res[g * n:(g + 1) * n]
        c = att_copy(chunk)
        c.start()
        sent.append(c)

    ysent = []

    def y_copy(chunk, i, where):
        at = pl.ds(0, chunks[chunk][1])
        return remote(ys.at[i, at], yr.at[i, at], s_ys.at[i], s_yr.at[i], where)

    def y_post(chunk, val, i, where):
        ys[i, :val.shape[0]] = val
        c = y_copy(chunk, i, where)
        c.start()
        ysent.append(c)

    def project(chunk):
        base = 6 * chunk
        first, n = chunks[chunk]
        att_copy(chunk).wait_recv()
        both = jnp.concatenate([att[c, pl.ds(first, n), :] for c in range(2)], axis=0)

        def y_part(r):
            if chunk == 0:
                c_wo[r].wait()
            val = dot_nn(both, wo[r])
            return val[:n], val[n:]

        one, two = y_part(n_y // 2)
        y_post(chunk, one, base, up)
        y_post(chunk, two, base + 1, down)
        one, two = y_part(1)
        y_post(chunk, two, base + 2, up)
        yhold[chunk, 0, :n] = one
        one, two = y_part(n_y - 1)
        y_post(chunk, one, base + 3, down)
        yhold[chunk, 1, :n] = two
        one, two = y_part(0)
        yhold[chunk, 2, :n] = one
        yhold[chunk, 3, :n] = two

    def y_relay(chunk):
        base = 6 * chunk
        n = chunks[chunk][1]
        y_copy(chunk, base, up).wait_recv()
        y_post(chunk, yhold[chunk, 0, :n] + yr[base, :n], base + 4, up)
        y_copy(chunk, base + 1, down).wait_recv()
        y_post(chunk, yhold[chunk, 1, :n] + yr[base + 1, :n], base + 5, down)

    gsend = []

    def region(chunk, dest, which):
        first, n = chunks[chunk]
        return out_v.at[pl.ds(first, n), pl.ds(pl.multiple_of(dest * blk + which * half, 128), half)]

    def g_start(src, dst, chunk, slot, which, sem, where):
        c = remote(src, dst, s_gs.at[chunk, sem], s_gr.at[chunk, slot, which], where)
        c.start()
        gsend.append(c)

    def g_wait(chunk, slot, which):
        ref = region(chunk, ypos, 0)
        remote(ref, ref, s_gs.at[chunk, 0], s_gr.at[chunk, slot, which], up).wait_recv()

    def finish(chunk):
        base = 6 * chunk
        first, n = chunks[chunk]
        mine = region(chunk, ypos, core)
        done = []
        for c, (near, merged) in enumerate(((base + 3, base + 4), (base + 2, base + 5))):
            val = yhold[chunk, 2 + c, :n]
            for i in (near, merged):
                y_copy(chunk, i, up if i % 2 == 0 else down).wait_recv()
                val = val + yr[i, :n]
            val = (val + xres[c, pl.ds(first, n), :].astype(F32)).astype(BF16)
            yblk[chunk, c, :n] = val
            src = yblk.at[chunk, c, pl.ds(0, n)]
            order = ((0, up_cores[c]), (1, down_cores[c]))
            for slot, where in (order if c == 0 else order[::-1]):
                g_start(src, mine, chunk, slot, core, 2 * c + slot, where)
            done.append(val)
        col = pl.multiple_of(ypos * blk + core * half, 128)
        out_v[pl.ds(first, n), pl.ds(col, half)] = jnp.where(core == 0, done[0], done[1])
        g_start(yblk.at[chunk, 1 - core, pl.ds(0, n)], mine, chunk, 3, core, 4, partner)

    def forward(chunk):
        g_wait(chunk, 0, 0)
        ref = region(chunk, below, 0)
        g_start(ref, ref, chunk, 2, 0, 5, up)
        g_wait(chunk, 1, 1)
        ref = region(chunk, above, 1)
        g_start(ref, ref, chunk, 2, 1, 6, down)

    def collect(chunk):
        g_wait(chunk, 0, 1)
        g_wait(chunk, 1, 0)
        g_wait(chunk, 3, 1 - core)
        g_wait(chunk, 2, 0)
        g_wait(chunk, 2, 1)

    prefix_own()
    q_copies[0][0].wait_recv()
    fwd_right = remote(qg.at[1, 0], qg.at[3, 0], s_qs.at[2, 0], s_qr.at[3, 0], right)
    fwd_right.start()
    wait(c_wkv)
    start(ring_copies(1))
    for r in (n_y // 2, 1, n_y - 1, 0):
        c_wo[r].start()
    knew[...] = dot_nn(hid[...], wk[...]).astype(BF16).astype(F32)
    vnew[...] = dot_nn(hid[...], wv[...]).astype(BF16).astype(F32)
    q_copies[1][1].wait_recv()
    fwd_left = remote(qg.at[2, 1], qg.at[3, 1], s_qs.at[2, 1], s_qr.at[3, 1], left)
    fwd_left.start()
    q_copies[1][0].wait_recv()
    q_copies[0][1].wait_recv()
    prefix_near(0)
    prefix_near(1)
    fwd_right.wait_recv()
    fwd_left.wait_recv()
    prefix_far()

    suffix_group(0)
    suffix_group(1)
    relay(0)
    relay(1)
    for group in range(2, n_groups):
        suffix_group(group)
    merge_prefix(0)
    combine(0)
    merge_prefix(1)
    combine(1)
    wait(c_res)
    project(0)
    combine(2)
    project(1)
    project(2)
    y_relay(0)
    y_relay(1)
    for c in [fwd_right, fwd_left] + sent:
        c.wait_send()
    for pair in q_copies:
        for c in pair:
            c.wait_send()
    y_relay(2)
    finish(0)
    finish(1)
    finish(2)
    for c in ysent:
        c.wait_send()
    forward(0)
    forward(1)
    forward(2)
    late = gsend[-2:]
    for c in gsend[:-2]:
        c.wait_send()
    collect(0)
    collect(1)
    collect(2)
    for c in late:
        c.wait_send()


def store(src, dst, sem):
    c = pltpu.make_async_copy(src, dst, sem)
    c.start()
    c.wait()


def solution(mesh):
    n_ctx, n_y = mesh.shape['ctx'], mesh.shape['heads']
    row_spec = P(('dp', 'ctx'), None)
    col_spec = P(None, 'heads')
    pre_spec = P(('dp', 'ctx'), 'heads', None)
    suf_spec = P(('dp', 'ctx'), None, 'heads', None)

    def local_step(hidden, w_query, w_key, w_value, w_out, prefix_k, prefix_v, suffix_k, suffix_v, seq_lens):
        rows, width = hidden.shape
        pos, kv_n, head = prefix_k.shape
        slots = suffix_k.shape[1]
        grp = w_query.shape[1] // (kv_n * head)
        heads = kv_n * grp
        blk = width // n_y
        half_rows = rows // 2
        stack = grp * half_rows
        lines = GROUP * heads
        dma = pltpu.SemaphoreType.DMA
        scratch = dict(
            hid=pltpu.VMEM((rows, width), BF16),
            wq=pltpu.VMEM((kv_n, width, grp * head), BF16),
            wk=pltpu.VMEM((width, kv_n * head), BF16),
            wv=pltpu.VMEM((width, kv_n * head), BF16),
            wo=pltpu.VMEM((n_y, heads * head, blk // 2), BF16),
            raw=pltpu.VMEM((2, 2, pos * kv_n, head), BF16),
            flat=pltpu.VMEM((pos * kv_n, head), F32),
            kpre=pltpu.VMEM((kv_n, 2 * pos, head), BF16),
            vpre=pltpu.VMEM((kv_n, 2 * pos, head), BF16),
            qg=pltpu.VMEM((4, kv_n, rows, grp * head), BF16),
            q8=pltpu.VMEM((rows * heads, head), F32),
            knew=pltpu.VMEM((rows, kv_n * head), F32),
            vnew=pltpu.VMEM((rows, kv_n * head), F32),
            ring_k=pltpu.VMEM((RING, GROUP, slots * kv_n, head), BF16),
            ring_v=pltpu.VMEM((RING, GROUP, slots * kv_n, head), BF16),
            qbd=pltpu.VMEM((GROUP // 2, 2 * head, lines), BF16),
            sufs=pltpu.VMEM((slots * kv_n, lines), F32),
            sufp=pltpu.VMEM((lines, slots * kv_n), BF16),
            scores=pltpu.VMEM((2, 2 * stack, 2 * pos), F32),
            own_num=pltpu.VMEM((2 * kv_n, stack, head), F32),
            own_st=pltpu.VMEM((2 * kv_n, stack, 128), F32),
            hold_num=pltpu.VMEM((4, stack, head), F32),
            hold_st=pltpu.VMEM((4, stack, 128), F32),
            xres=pltpu.VMEM((2, rows, blk // 2), BF16),
            so8=pltpu.VMEM((rows * heads, head), F32),
            sst8=pltpu.VMEM((rows * heads, head), F32),
            xs_num=pltpu.VMEM((12, stack, head), F32),
            xs_st=pltpu.VMEM((12, 8, stack), F32),
            xr_num=pltpu.VMEM((12, stack, head), F32),
            xr_st=pltpu.VMEM((12, 8, stack), F32),
            att=pltpu.VMEM((2, rows, heads * head), BF16),
            yhold=pltpu.VMEM((3, 4, half_rows, blk // 2), F32),
            ys=pltpu.VMEM((18, half_rows, blk // 2), F32),
            yr=pltpu.VMEM((18, half_rows, blk // 2), F32),
            yblk=pltpu.VMEM((3, 2, half_rows, blk // 2), BF16),
            s_hid=dma(()), s_wq=dma((kv_n, PIECES)), s_wkv=dma((2,)), s_wo=dma((n_y,)),
            s_raw=dma((2,)), s_rawsend=dma((2,)), s_rawrecv=dma((2,)), s_ring=dma((RING, 2)),
            s_res=dma(()), s_ress=dma(()), s_resr=dma(()), s_as=dma((3,)), s_ar=dma((3,)),
            s_qs=dma((3, kv_n)), s_qr=dma((4, kv_n)),
            s_xs=dma((12,)), s_xr=dma((12,)), s_xst=dma((12,)), s_xrt=dma((12,)),
            s_ys=dma((18,)), s_yr=dma((18,)), s_gs=dma((3, 7)), s_gr=dma((3, 4, 2)),
        )
        hbm = pl.BlockSpec(memory_space=pl.ANY)
        out = pl.pallas_call(
            functools.partial(kernel, (n_ctx, n_y, kv_n, grp)),
            out_shape=pltpu.VMEM((rows, width), BF16),
            in_specs=[hbm] * 9 + [pl.BlockSpec(memory_space=pltpu.SMEM)],
            out_specs=pl.BlockSpec(memory_space=pltpu.VMEM),
            scratch_shapes=list(scratch.values()),
            compiler_params=pltpu.CompilerParams(collective_id=0, has_side_effects=True, vmem_limit_bytes=VMEM_BYTES),
        )(hidden, w_query, w_key, w_value, w_out,
          prefix_k.reshape(pos * kv_n, head), prefix_v.reshape(pos * kv_n, head),
          suffix_k.reshape(rows, slots * kv_n, head), suffix_v.reshape(rows, slots * kv_n, head), seq_lens)
        return pl.pallas_call(
            store,
            out_shape=jax.ShapeDtypeStruct((rows, width), BF16),
            in_specs=[pl.BlockSpec(memory_space=pltpu.VMEM)],
            out_specs=hbm,
            scratch_shapes=[dma(())],
            compiler_params=pltpu.CompilerParams(vmem_limit_bytes=1048576),
        )(out)

    return jax.shard_map(local_step, mesh=mesh, in_specs=(row_spec, col_spec, col_spec, col_spec, P('heads', None), pre_spec, pre_spec, suf_spec, suf_spec, P(('dp', 'ctx'))), out_specs=row_spec, check_vma=False)
```

```python
import functools
import math
import jax
import jax.numpy as jnp
from jax import lax
from jax.experimental import pallas as pl
from jax.experimental.pallas import tpu as pltpu
from jax.sharding import PartitionSpec as P

MESH = pl.DeviceIdType.MESH
F32 = jnp.float32
BF16 = jnp.bfloat16
LOW = -3.0e38
GROUP = 16
RING = 2
POS_CHUNK = 512
PIECES = 5
IN_FLIGHT = 6
VMEM_BYTES = 66000000


def dot_nt(a, b):
    return lax.dot_general(a, b, (((1,), (1,)), ((), ())), preferred_element_type=F32)


def dot_nn(a, b):
    return lax.dot_general(a, b, (((1,), (0,)), ((), ())), preferred_element_type=F32)


def pack_stats(row_max, row_sum):
    rows = row_max.shape[0]
    lane = lax.broadcasted_iota(jnp.int32, (rows, 128), 1)
    both = jnp.where(lane == 0, row_max, jnp.where(lane == 1, row_sum, 0.0))
    return jnp.transpose(both)[:8]


def unpack_stats(packed):
    rows = packed.shape[1]
    both = jnp.transpose(jnp.concatenate([packed, jnp.zeros((120, rows), F32)], axis=0))
    return both[:, 0:1], both[:, 1:2]


def merge(one, two):
    (num_a, max_a, sum_a), (num_b, max_b, sum_b) = one, two
    top = jnp.maximum(max_a, max_b)
    fac_a, fac_b = jnp.exp2(max_a - top), jnp.exp2(max_b - top)
    return num_a * fac_a + num_b * fac_b, top, sum_a * fac_a + sum_b * fac_b


def kernel(dims, hid_h, wq_h, wk_h, wv_h, wo_h, pk_h, pv_h, sk_h, sv_h, lens, out_v,
           hid, wq, wk, wv, wo, raw, flat, kpre, vpre, qg, q8, knew, vnew,
           ring, qbd, sufs, sufp, scores, own_num, own_st, hold_num, hold_st, xres,
           so8, sst8, xs, xr, att, yhold, ys, yr, yblk,
           s_hid, s_wq, s_wkv, s_wo, s_raw, s_rawsend, s_rawrecv, s_ring, s_res, s_ress, s_resr, s_as, s_ar,
           s_qs, s_qr, s_xs, s_xr, s_ys, s_yr, s_gs, s_gr, s_gl):
    n_ctx, n_y, kv_n, grp = dims
    rows = hid.shape[0]
    width = hid.shape[1]
    head = kpre.shape[-1]
    heads = kv_n * grp
    local_pos = raw.shape[2] // kv_n
    scale = head ** -0.5 * math.log2(math.e)
    blk = width // n_y
    half = blk // 2
    part_rows = rows // 2
    stack = grp * part_rows

    ctx = lax.axis_index('ctx')
    ypos = lax.axis_index('heads')
    right = {'ctx': lax.rem(ctx + 2, n_ctx)}
    left = {'ctx': lax.rem(ctx + n_ctx - 2, n_ctx)}
    core = lax.rem(ctx, 2)
    partner = {'ctx': ctx + 1 - 2 * core}
    below, above = lax.rem(ypos + n_y - 1, n_y), lax.rem(ypos + 1, n_y)
    up, down = {'heads': above}, {'heads': below}
    up_cores = [{'heads': above, 'ctx': ctx - core + c} for c in range(2)]
    down_cores = [{'heads': below, 'ctx': ctx - core + c} for c in range(2)]
    up_other = {'heads': above, 'ctx': ctx + 1 - 2 * core}
    down_other = {'heads': below, 'ctx': ctx + 1 - 2 * core}
    chunks = ((0, rows // 2), (rows // 2, rows // 4), (3 * rows // 4, rows // 4))

    def remote(src, dst, send, recv, where):
        return pltpu.make_async_remote_copy(src_ref=src, dst_ref=dst, send_sem=send, recv_sem=recv,
                                            device_id=where, device_id_type=MESH)

    c_hid = pltpu.make_async_copy(hid_h, hid, s_hid)
    c_raw = [pltpu.make_async_copy(src, raw.at[0, i], s_raw) for i, src in enumerate((pk_h, pv_h))]
    deep = width // PIECES
    c_wq = [pltpu.make_async_copy(wq_h.at[pl.ds(k * deep, deep), pl.ds(kv * grp * head, grp * head)],
                                  wq.at[kv, pl.ds(k * deep, deep), :], s_wq.at[(kv * PIECES + k) % (IN_FLIGHT + 1)])
            for kv in range(kv_n) for k in range(PIECES)]
    c_wkv = [pltpu.make_async_copy(src, dst, s_wkv.at[i]) for i, (src, dst) in enumerate(((wk_h, wk), (wv_h, wv)))]
    c_wo = []
    for r in range(n_y):
        col = pl.multiple_of(lax.rem(ypos + r, n_y) * blk + core * half, 128)
        c_wo.append(pltpu.make_async_copy(wo_h.at[:, pl.ds(col, half)], wo.at[r], s_wo.at[r]))
    n_groups = rows // GROUP

    def ring_copies(group):
        seqs = pl.ds(group * GROUP, GROUP)
        slot = group % RING
        return [pltpu.make_async_copy(src.at[seqs], ring.at[slot, i], s_ring.at[slot]) for i, src in enumerate((sk_h, sv_h))]

    def start(copies):
        for c in copies:
            c.start()

    def wait(copies):
        for c in copies:
            c.wait()

    queue = c_wq + c_raw + c_wkv

    def advance():
        if queue:
            queue.pop(0).start()

    c_hid.start()
    for _ in range(IN_FLIGHT):
        advance()

    barrier = pltpu.get_barrier_semaphore()
    for where in (partner, left, right, up, down, up_other, down_other):
        pl.semaphore_signal(barrier, inc=1, device_id=where, device_id_type=MESH)

    def deinterleave(which):
        for i, dst in enumerate((kpre, vpre)):
            flat[...] = raw[which, i].astype(F32)
            for kv in range(kv_n):
                dst[kv, pl.ds(which * local_pos, local_pos), :] = flat[pl.ds(kv, local_pos, stride=kv_n), :].astype(BF16)

    def queries(kv):
        total = None
        for k in range(PIECES):
            c_wq[kv * PIECES + k].wait()
            advance()
            at = pl.ds(k * deep, deep)
            term = dot_nn(hid[:, at], wq[kv, at, :])
            total = term if total is None else total + term
        part = total.astype(BF16)
        qg[0, kv] = part
        for g in range(grp):
            q8[pl.ds(kv * grp + g, rows, stride=heads), :] = part[:, g * head:(g + 1) * head].astype(F32)

    def send_queries(kv):
        pair = (remote(qg.at[0, kv], qg.at[1, kv], s_qs, s_qr.at[0, kv], right),
                remote(qg.at[0, kv], qg.at[2, kv], s_qs, s_qr.at[1, kv], left))
        start(pair)
        return pair

    c_hid.wait()
    queries(0)
    pl.semaphore_wait(barrier, 7)
    q_copies = [send_queries(0)]
    c_swap = [remote(src, raw.at[1, i], s_rawsend, s_rawrecv, partner) for i, src in enumerate((pk_h, pv_h))]
    start(c_swap)
    c_res = [pltpu.make_async_copy(hid_h.at[:, pl.ds(pl.multiple_of(ypos * blk + core * half, 128), half)], xres.at[core], s_res),
             remote(hid_h.at[:, pl.ds(pl.multiple_of(ypos * blk + (1 - core) * half, 128), half)], xres.at[core], s_ress, s_resr, partner)]
    start(c_res)
    queries(1)
    q_copies.append(send_queries(1))
    while queue:
        advance()
    pltpu.make_async_copy(raw.at[0], raw.at[0], s_raw).wait()
    deinterleave(0)

    remote(raw.at[1], raw.at[1], s_rawsend, s_rawrecv, partner).wait()
    deinterleave(1)
    start(ring_copies(0))

    n_pos = kpre.shape[1]

    n_pieces = n_pos // POS_CHUNK
    part_lanes = POS_CHUNK // 128

    def prefix_states(jobs):
        stacked, run, out = [None] * len(jobs), [None] * len(jobs), []

        def score(i, c):
            sources, kv = jobs[i]
            if c == 0:
                stacked[i] = jnp.concatenate([qg[slot, kv, pl.ds(chunk * part_rows, part_rows), pl.ds(g * head, head)]
                                              for slot, chunk in sources for g in range(grp)], axis=0)
            at = pl.ds(c * POS_CHUNK, POS_CHUNK)
            s = dot_nt(stacked[i], kpre[kv, at, :])
            scores[i % 2, :, at] = s
            for t in range(part_lanes):
                piece = s[:, t * 128:(t + 1) * 128]
                run[i] = piece if run[i] is None else jnp.maximum(run[i], piece)

        for c in range(n_pieces):
            score(0, c)
        for i, (sources, kv) in enumerate(jobs):
            row_max = jnp.max(run[i], axis=1, keepdims=True) * scale
            wide_max = jnp.broadcast_to(row_max, (2 * stack, 128))
            wide_max = jnp.concatenate([wide_max] * part_lanes, axis=1)
            total, num = None, None
            for c in range(n_pieces):
                if i + 1 < len(jobs):
                    score(i + 1, c)
                at = pl.ds(c * POS_CHUNK, POS_CHUNK)
                p = jnp.exp2(scores[i % 2, :, at] * scale - wide_max)
                for t in range(part_lanes):
                    piece = p[:, t * 128:(t + 1) * 128]
                    total = piece if total is None else total + piece
                term = dot_nn(p.astype(BF16), vpre[kv, at, :])
                num = term if num is None else num + term
            row_sum = jnp.sum(total, axis=1, keepdims=True)
            out += [(num[:stack], row_max[:stack], row_sum[:stack]), (num[stack:], row_max[stack:], row_sum[stack:])]
        return out

    def x_copies(i, where):
        return remote(xs.at[i], xr.at[i], s_xs, s_xr.at[i], where)

    def post(state, i, where):
        xs[i, :stack] = state[0]
        xs[i, stack:, :stack] = pack_stats(state[1], state[2])
        x_copies(i, where).start()

    def arrived(i):
        return (xr[i, :stack],) + unpack_stats(xr[i, stack:, :stack])

    def keep(refs, i, state):
        refs[0][i] = state[0]
        lane = lax.broadcasted_iota(jnp.int32, state[0].shape, 1)
        refs[1][i] = jnp.where(lane == 0, state[1], state[2])

    def kept(refs, i):
        return refs[0][i], refs[1][i][:, 0:1], refs[1][i][:, 1:2]

    own = (own_num, own_st)
    hold = (hold_num, hold_st)

    def prefix_near(chunk):
        base = 6 * chunk
        both = ((2, chunk), (1, chunk))
        right_1, left_1, right_0, left_0 = prefix_states([(both, 1), (both, 0)])
        post(right_1, base, right)
        post(left_0, base + 1, left)
        keep(hold, 2 * chunk + 1, left_1)
        keep(hold, 2 * chunk, right_0)

    def prefix_far():
        both = ((3, 0), (3, 1))
        states = prefix_states([(both, 0), (both, 1)])
        for chunk in range(2):
            post(states[chunk], 6 * chunk + 2, right)
            post(states[2 + chunk], 6 * chunk + 3, left)

    def prefix_own():
        both = ((0, 0), (0, 1))
        for i, state in enumerate(prefix_states([(both, 0), (both, 1)])):
            keep(own, i, state)

    def relay(chunk):
        base = 6 * chunk
        for i, where in ((base + 2, right), (base + 3, left)):
            x_copies(i, where).wait_recv()
        to_right, to_left = (merge(arrived(base + 2 + i), kept(hold, 2 * chunk + i)) for i in range(2))
        post(to_right, base + 4, right)
        post(to_left, base + 5, left)

    lines = GROUP * heads
    span = ring.shape[3]
    tile = span // 4

    def suffix_group(group):
        slot = group % RING
        lane = lax.broadcasted_iota(jnp.int32, (head, lines), 1)
        q_t = jnp.transpose(q8[pl.ds(group * lines, lines), :])
        for j in range(GROUP // 2):
            both = [jnp.where(lane // heads == 2 * j + e, q_t, 0.0) for e in range(2)]
            qbd[j] = jnp.concatenate(both, axis=0).astype(BF16)
        one = lax.broadcasted_iota(jnp.int32, (1, lines), 1)
        length = jnp.zeros((1, lines), jnp.int32)
        for b in range(GROUP):
            length = jnp.where(one // heads == b, lens[group * GROUP + b], length)
        line = lax.broadcasted_iota(jnp.int32, (tile, lines), 0)
        lane = lax.broadcasted_iota(jnp.int32, (tile, lines), 1)
        mine = lax.rem(line, kv_n) == lax.rem(lane, heads) // grp
        place = jnp.where(mine, line // kv_n, span)
        pltpu.make_async_copy(ring.at[slot], ring.at[slot], s_ring.at[slot]).wait()
        run = jnp.full((1, lines), LOW, F32)
        for c in range(4):
            at = pl.ds(c * tile, tile)
            s = None
            for j in range(GROUP // 2):
                keys = jnp.concatenate([ring[slot, 0, 2 * j, at, :], ring[slot, 0, 2 * j + 1, at, :]], axis=1)
                term = dot_nn(keys, qbd[j])
                s = term if s is None else s + term
            s = jnp.where(place < length - c * (tile // kv_n), s * scale, -jnp.inf)
            sufs[at, :] = s
            run = jnp.maximum(run, jnp.max(s, axis=0, keepdims=True))
        total = jnp.zeros((1, lines), F32)
        for c in range(4):
            p = jnp.exp2(sufs[pl.ds(c * tile, tile), :] - run)
            total = total + jnp.sum(p, axis=0, keepdims=True)
            sufp[:, pl.ds(c * tile, tile)] = jnp.transpose(p).astype(BF16)
        stats = jnp.concatenate([run, total, jnp.zeros((head - 2, lines), F32)], axis=0)
        sst8[pl.ds(group * lines, lines), :] = jnp.transpose(stats)
        for j in range(GROUP // 2):
            weights = sufp[pl.ds(2 * j * heads, 2 * heads), :]
            for e in range(2):
                o = dot_nn(weights, ring[slot, 1, 2 * j + e])
                so8[pl.ds(group * lines + (2 * j + e) * heads, heads), :] = o[e * heads:(e + 1) * heads]
        if group + RING < n_groups:
            start(ring_copies(group + RING))

    def merge_prefix(chunk):
        base = 6 * chunk
        for i, where in ((base + 1, left), (base + 4, right), (base, right), (base + 5, left)):
            x_copies(i, where).wait_recv()
        merged = [functools.reduce(merge, [kept(own, chunk), arrived(base + 1), arrived(base + 4)]),
                  functools.reduce(merge, [kept(own, 2 + chunk), arrived(base), arrived(base + 5)])]
        for kv in range(kv_n):
            keep(own, 2 * kv + chunk, merged[kv])

    def att_copy(chunk):
        first, n = chunks[chunk]
        ref = att.at[core, pl.ds(first, n), :]
        return remote(ref, ref, s_as, s_ar.at[chunk], partner)

    def combine(chunk):
        first, n = chunks[chunk]
        at_rows = pl.ds(first, n)
        which, off = first // part_rows, first % part_rows
        for kv in range(kv_n):
            rest = []
            for g in range(grp):
                every = pl.ds(first * heads + kv * grp + g, n, stride=heads)
                stats = sst8[every, :]
                pre_at = pl.ds(g * part_rows + off, n)
                pre = own_st[2 * kv + which, pre_at, :]
                rest.append((so8[every, :], stats[:, 0:1], stats[:, 1:2], q8[every, :],
                             own_num[2 * kv + which, pre_at, :], pre[:, 0:1], pre[:, 1:2]))
            num, top, tot, qs, pre_num, pre_top, pre_tot = (jnp.concatenate(list(v), axis=0) for v in zip(*rest))
            state = merge((pre_num, pre_top, pre_tot), (num, top, tot))
            kn = jnp.concatenate([knew[at_rows, pl.ds(kv * head, head)]] * grp, axis=0)
            vn = jnp.concatenate([vnew[at_rows, pl.ds(kv * head, head)]] * grp, axis=0)
            s_new = jnp.sum(qs * kn, axis=1, keepdims=True) * scale
            state = merge(state, (vn, s_new, jnp.ones_like(s_new)))
            res = (state[0] / state[2]).astype(BF16)
            for g in range(grp):
                att[core, at_rows, pl.ds((kv * grp + g) * head, head)] = res[g * n:(g + 1) * n]
        att_copy(chunk).start()

    def y_copy(chunk, i, where):
        at = pl.ds(0, chunks[chunk][1])
        return remote(ys.at[i, at], yr.at[i, at], s_ys, s_yr.at[i], where)

    def y_post(chunk, val, i, where):
        ys[i, :val.shape[0]] = val
        y_copy(chunk, i, where).start()

    def project(chunk):
        base = 6 * chunk
        first, n = chunks[chunk]
        att_copy(chunk).wait_recv()
        both = jnp.concatenate([att[c, pl.ds(first, n), :] for c in range(2)], axis=0)

        def y_part(r):
            if chunk == 0:
                c_wo[r].wait()
            val = dot_nn(both, wo[r])
            return val[:n], val[n:]

        one, two = y_part(n_y // 2)
        y_post(chunk, one, base, up)
        y_post(chunk, two, base + 1, down)
        one, two = y_part(1)
        y_post(chunk, two, base + 2, up)
        yhold[chunk, 0, :n] = one
        one, two = y_part(n_y - 1)
        y_post(chunk, one, base + 3, down)
        yhold[chunk, 1, :n] = two
        one, two = y_part(0)
        yhold[chunk, 2, :n] = one
        yhold[chunk, 3, :n] = two

    def y_relay(chunk):
        base = 6 * chunk
        n = chunks[chunk][1]
        y_copy(chunk, base, up).wait_recv()
        y_post(chunk, yhold[chunk, 0, :n] + yr[base, :n], base + 4, up)
        y_copy(chunk, base + 1, down).wait_recv()
        y_post(chunk, yhold[chunk, 1, :n] + yr[base + 1, :n], base + 5, down)

    def region(chunk, dest, which):
        first, n = chunks[chunk]
        return out_v.at[pl.ds(first, n), pl.ds(pl.multiple_of(dest * blk + which * half, 128), half)]

    def g_start(src, dst, sem, where):
        remote(src, dst, s_gs, sem, where).start()

    def g_wait(chunk, slot):
        ref = region(chunk, ypos, 0)
        remote(ref, ref, s_gs, s_gr.at[chunk, slot], up).wait_recv()

    def g_first(src, dst, chunk, slot, where):
        @pl.when(core == slot)
        def _():
            g_start(src, dst, s_gr.at[chunk, slot], where)

        @pl.when(core != slot)
        def _():
            g_start(src, dst, s_gl, where)

    def finish(chunk):
        base = 6 * chunk
        first, n = chunks[chunk]
        mine = region(chunk, ypos, core)
        done = []
        for c, (near, merged) in enumerate(((base + 3, base + 4), (base + 2, base + 5))):
            val = yhold[chunk, 2 + c, :n]
            for i in (near, merged):
                y_copy(chunk, i, up if i % 2 == 0 else down).wait_recv()
                val = val + yr[i, :n]
            val = (val + xres[c, pl.ds(first, n), :].astype(F32)).astype(BF16)
            yblk[chunk, c, :n] = val
            src = yblk.at[chunk, c, pl.ds(0, n)]
            if c == 0:
                g_first(src, mine, chunk, 0, up_cores[c])
                g_first(src, mine, chunk, 1, down_cores[c])
            else:
                g_first(src, mine, chunk, 1, down_cores[c])
                g_first(src, mine, chunk, 0, up_cores[c])
            done.append(val)
        col = pl.multiple_of(ypos * blk + core * half, 128)
        out_v[pl.ds(first, n), pl.ds(col, half)] = jnp.where(core == 0, done[0], done[1])
        g_start(yblk.at[chunk, 1 - core, pl.ds(0, n)], mine, s_gl, partner)

    def forward(chunk):
        g_wait(chunk, 0)
        ref = region(chunk, below, 0)
        g_start(ref, ref, s_gl, up)
        g_wait(chunk, 1)
        ref = region(chunk, above, 1)
        g_start(ref, ref, s_gl, down)

    prefix_own()
    q_copies[0][0].wait_recv()
    fwd_right = remote(qg.at[1, 0], qg.at[3, 0], s_qs, s_qr.at[2, 0], right)
    fwd_right.start()
    wait(c_wkv)
    start(ring_copies(1))
    for r in (n_y // 2, 1, n_y - 1, 0):
        c_wo[r].start()
    knew[...] = dot_nn(hid[...], wk[...]).astype(BF16).astype(F32)
    vnew[...] = dot_nn(hid[...], wv[...]).astype(BF16).astype(F32)
    q_copies[1][1].wait_recv()
    fwd_left = remote(qg.at[2, 1], qg.at[3, 1], s_qs, s_qr.at[2, 1], left)
    fwd_left.start()
    q_copies[1][0].wait_recv()
    q_copies[0][1].wait_recv()
    prefix_near(0)
    prefix_near(1)
    fwd_right.wait_recv()
    fwd_left.wait_recv()
    prefix_far()

    suffix_group(0)
    suffix_group(1)
    relay(0)
    relay(1)
    suffix_group(2)
    merge_prefix(0)
    combine(0)
    wait(c_res)
    merge_prefix(1)
    project(0)
    for group in range(3, n_groups):
        suffix_group(group)
    combine(1)
    combine(2)
    y_relay(0)
    project(1)
    project(2)
    y_relay(1)
    y_relay(2)
    finish(0)
    finish(1)
    finish(2)
    remote(qg.at[pl.ds(0, 3)], qg.at[pl.ds(0, 3)], s_qs, s_qr.at[0, 0], right).wait_send()
    remote(xs, xr, s_xs, s_xr.at[0], right).wait_send()
    remote(att.at[0], att.at[0], s_as, s_ar.at[0], partner).wait_send()
    y_all = pl.ds(0, 12)
    remote(ys.at[y_all], yr.at[y_all], s_ys, s_yr.at[0], up).wait_send()
    forward(0)
    forward(1)
    forward(2)
    remote(yr.at[pl.ds(0, 5)], yr.at[pl.ds(0, 5)], s_gs, s_gl, up).wait_recv()
    remote(ys.at[pl.ds(0, 7)], yr.at[pl.ds(0, 7)], s_gs, s_gl, up).wait_send()


def store(src, dst, sem):
    c = pltpu.make_async_copy(src, dst, sem)
    c.start()
    c.wait()


def solution(mesh):
    n_ctx, n_y = mesh.shape['ctx'], mesh.shape['heads']
    row_spec = P(('dp', 'ctx'), None)
    col_spec = P(None, 'heads')
    pre_spec = P(('dp', 'ctx'), 'heads', None)
    suf_spec = P(('dp', 'ctx'), None, 'heads', None)

    def local_step(hidden, w_query, w_key, w_value, w_out, prefix_k, prefix_v, suffix_k, suffix_v, seq_lens):
        rows, width = hidden.shape
        pos, kv_n, head = prefix_k.shape
        slots = suffix_k.shape[1]
        grp = w_query.shape[1] // (kv_n * head)
        heads = kv_n * grp
        blk = width // n_y
        half_rows = rows // 2
        stack = grp * half_rows
        lines = GROUP * heads
        dma = pltpu.SemaphoreType.DMA
        scratch = dict(
            hid=pltpu.VMEM((rows, width), BF16),
            wq=pltpu.VMEM((kv_n, width, grp * head), BF16),
            wk=pltpu.VMEM((width, kv_n * head), BF16),
            wv=pltpu.VMEM((width, kv_n * head), BF16),
            wo=pltpu.VMEM((n_y, heads * head, blk // 2), BF16),
            raw=pltpu.VMEM((2, 2, pos * kv_n, head), BF16),
            flat=pltpu.VMEM((pos * kv_n, head), F32),
            kpre=pltpu.VMEM((kv_n, 2 * pos, head), BF16),
            vpre=pltpu.VMEM((kv_n, 2 * pos, head), BF16),
            qg=pltpu.VMEM((4, kv_n, rows, grp * head), BF16),
            q8=pltpu.VMEM((rows * heads, head), F32),
            knew=pltpu.VMEM((rows, kv_n * head), F32),
            vnew=pltpu.VMEM((rows, kv_n * head), F32),
            ring=pltpu.VMEM((RING, 2, GROUP, slots * kv_n, head), BF16),
            qbd=pltpu.VMEM((GROUP // 2, 2 * head, lines), BF16),
            sufs=pltpu.VMEM((slots * kv_n, lines), F32),
            sufp=pltpu.VMEM((lines, slots * kv_n), BF16),
            scores=pltpu.VMEM((2, 2 * stack, 2 * pos), F32),
            own_num=pltpu.VMEM((2 * kv_n, stack, head), F32),
            own_st=pltpu.VMEM((2 * kv_n, stack, 128), F32),
            hold_num=pltpu.VMEM((4, stack, head), F32),
            hold_st=pltpu.VMEM((4, stack, 128), F32),
            xres=pltpu.VMEM((2, rows, blk // 2), BF16),
            so8=pltpu.VMEM((rows * heads, head), F32),
            sst8=pltpu.VMEM((rows * heads, head), F32),
            xs=pltpu.VMEM((12, stack + 8, head), F32),
            xr=pltpu.VMEM((12, stack + 8, head), F32),
            att=pltpu.VMEM((2, rows, heads * head), BF16),
            yhold=pltpu.VMEM((3, 4, half_rows, blk // 2), F32),
            ys=pltpu.VMEM((18, half_rows, blk // 2), F32),
            yr=pltpu.VMEM((18, half_rows, blk // 2), F32),
            yblk=pltpu.VMEM((3, 2, half_rows, blk // 2), BF16),
            s_hid=dma(()), s_wq=dma((IN_FLIGHT + 1,)), s_wkv=dma((2,)), s_wo=dma((n_y,)),
            s_raw=dma(()), s_rawsend=dma(()), s_rawrecv=dma(()), s_ring=dma((RING,)),
            s_res=dma(()), s_ress=dma(()), s_resr=dma(()), s_as=dma(()), s_ar=dma((3,)),
            s_qs=dma(()), s_qr=dma((3, kv_n)),
            s_xs=dma(()), s_xr=dma((12,)),
            s_ys=dma(()), s_yr=dma((18,)), s_gs=dma(()), s_gr=dma((3, 2)), s_gl=dma(()),
        )
        hbm = pl.BlockSpec(memory_space=pl.ANY)
        out = pl.pallas_call(
            functools.partial(kernel, (n_ctx, n_y, kv_n, grp)),
            out_shape=pltpu.VMEM((rows, width), BF16),
            in_specs=[hbm] * 9 + [pl.BlockSpec(memory_space=pltpu.SMEM)],
            out_specs=pl.BlockSpec(memory_space=pltpu.VMEM),
            scratch_shapes=list(scratch.values()),
            compiler_params=pltpu.CompilerParams(collective_id=0, has_side_effects=True, vmem_limit_bytes=VMEM_BYTES),
        )(hidden, w_query, w_key, w_value, w_out,
          prefix_k.reshape(pos * kv_n, head), prefix_v.reshape(pos * kv_n, head),
          suffix_k.reshape(rows, slots * kv_n, head), suffix_v.reshape(rows, slots * kv_n, head), seq_lens)
        return pl.pallas_call(
            store,
            out_shape=jax.ShapeDtypeStruct((rows, width), BF16),
            in_specs=[pl.BlockSpec(memory_space=pltpu.VMEM)],
            out_specs=hbm,
            scratch_shapes=[dma(())],
            compiler_params=pltpu.CompilerParams(vmem_limit_bytes=1048576),
        )(out)

    return jax.shard_map(local_step, mesh=mesh, in_specs=(row_spec, col_spec, col_spec, col_spec, P('heads', None), pre_spec, pre_spec, suf_spec, suf_spec, P(('dp', 'ctx'))), out_specs=row_spec, check_vma=False)
```

```python
import functools
import math
import jax
import jax.numpy as jnp
from jax import lax
from jax.experimental import pallas as pl
from jax.experimental.pallas import tpu as pltpu
from jax.sharding import PartitionSpec as P

MESH = pl.DeviceIdType.MESH
F32 = jnp.float32
BF16 = jnp.bfloat16
LOW = -3.0e38
GROUP = 16
RING = 2
POS_CHUNK = 512
PIECES = 5
IN_FLIGHT = 6
VMEM_BYTES = 66000000


def dot_nt(a, b):
    return lax.dot_general(a, b, (((1,), (1,)), ((), ())), preferred_element_type=F32)


def dot_nn(a, b):
    return lax.dot_general(a, b, (((1,), (0,)), ((), ())), preferred_element_type=F32)


def pack_stats(row_max, row_sum):
    rows = row_max.shape[0]
    lane = lax.broadcasted_iota(jnp.int32, (rows, 128), 1)
    both = jnp.where(lane == 0, row_max, jnp.where(lane == 1, row_sum, 0.0))
    return jnp.transpose(both)[:8]


def unpack_stats(packed):
    rows = packed.shape[1]
    both = jnp.transpose(jnp.concatenate([packed, jnp.zeros((120, rows), F32)], axis=0))
    return both[:, 0:1], both[:, 1:2]


def merge(one, two):
    (num_a, max_a, sum_a), (num_b, max_b, sum_b) = one, two
    top = jnp.maximum(max_a, max_b)
    fac_a, fac_b = jnp.exp2(max_a - top), jnp.exp2(max_b - top)
    return num_a * fac_a + num_b * fac_b, top, sum_a * fac_a + sum_b * fac_b


def kernel(dims, hid_h, wq_h, wk_h, wv_h, wo_h, pk_h, pv_h, sk_h, sv_h, lens, out_v,
           hid, wq, wk, wv, wo, raw, flat, kpre, vpre, qg, q8, knew, vnew,
           ring, qbd, sufs, sufp, scores, own_num, own_st, hold_num, hold_st, xres,
           so8, sst8, xs, xr, att, yhold, ys, yr, yblk,
           s_hid, s_wq, s_wkv, s_wo, s_raw, s_rawsend, s_rawrecv, s_ring, s_res, s_ress, s_resr, s_as, s_ar,
           s_qs, s_qr, s_xs, s_xr, s_ys, s_yr, s_gs, s_gr, s_gl):
    n_ctx, n_y, kv_n, grp = dims
    rows = hid.shape[0]
    width = hid.shape[1]
    head = kpre.shape[-1]
    heads = kv_n * grp
    local_pos = raw.shape[2] // kv_n
    scale = head ** -0.5 * math.log2(math.e)
    blk = width // n_y
    half = blk // 2
    part_rows = rows // 2
    stack = grp * part_rows

    ctx = lax.axis_index('ctx')
    ypos = lax.axis_index('heads')
    right = {'ctx': lax.rem(ctx + 2, n_ctx)}
    left = {'ctx': lax.rem(ctx + n_ctx - 2, n_ctx)}
    core = lax.rem(ctx, 2)
    partner = {'ctx': ctx + 1 - 2 * core}
    below, above = lax.rem(ypos + n_y - 1, n_y), lax.rem(ypos + 1, n_y)
    up, down = {'heads': above}, {'heads': below}
    up_cores = [{'heads': above, 'ctx': ctx - core + c} for c in range(2)]
    down_cores = [{'heads': below, 'ctx': ctx - core + c} for c in range(2)]
    up_other = {'heads': above, 'ctx': ctx + 1 - 2 * core}
    down_other = {'heads': below, 'ctx': ctx + 1 - 2 * core}
    chunks = ((0, rows // 2), (rows // 2, rows // 4), (3 * rows // 4, rows // 4))

    def remote(src, dst, send, recv, where):
        return pltpu.make_async_remote_copy(src_ref=src, dst_ref=dst, send_sem=send, recv_sem=recv,
                                            device_id=where, device_id_type=MESH)

    c_hid = pltpu.make_async_copy(hid_h, hid, s_hid)
    c_raw = [pltpu.make_async_copy(src, raw.at[0, i], s_raw) for i, src in enumerate((pk_h, pv_h))]
    deep = width // PIECES
    c_wq = [pltpu.make_async_copy(wq_h.at[pl.ds(k * deep, deep), pl.ds(kv * grp * head, grp * head)],
                                  wq.at[kv, pl.ds(k * deep, deep), :], s_wq.at[(kv * PIECES + k) % (IN_FLIGHT + 1)])
            for kv in range(kv_n) for k in range(PIECES)]
    c_wkv = [pltpu.make_async_copy(src, dst, s_wkv.at[i]) for i, (src, dst) in enumerate(((wk_h, wk), (wv_h, wv)))]
    c_wo = []
    for r in range(n_y):
        col = pl.multiple_of(lax.rem(ypos + r, n_y) * blk + core * half, 128)
        c_wo.append(pltpu.make_async_copy(wo_h.at[:, pl.ds(col, half)], wo.at[r], s_wo.at[r]))
    n_groups = rows // GROUP

    def ring_copies(group):
        seqs = pl.ds(group * GROUP, GROUP)
        slot = group % RING
        return [pltpu.make_async_copy(src.at[seqs], ring.at[slot, i], s_ring.at[slot]) for i, src in enumerate((sk_h, sv_h))]

    def start(copies):
        for c in copies:
            c.start()

    def wait(copies):
        for c in copies:
            c.wait()

    queue = c_wq + c_raw + c_wkv

    def advance():
        if queue:
            queue.pop(0).start()

    c_hid.start()
    for _ in range(IN_FLIGHT):
        advance()

    barrier = pltpu.get_barrier_semaphore()
    for where in (partner, left, right, up, down, up_other, down_other):
        pl.semaphore_signal(barrier, inc=1, device_id=where, device_id_type=MESH)

    def deinterleave(which):
        for i, dst in enumerate((kpre, vpre)):
            flat[...] = raw[which, i].astype(F32)
            for kv in range(kv_n):
                dst[kv, pl.ds(which * local_pos, local_pos), :] = flat[pl.ds(kv, local_pos, stride=kv_n), :].astype(BF16)

    def queries(kv):
        total = None
        for k in range(PIECES):
            c_wq[kv * PIECES + k].wait()
            advance()
            at = pl.ds(k * deep, deep)
            term = dot_nn(hid[:, at], wq[kv, at, :])
            total = term if total is None else total + term
        part = total.astype(BF16)
        qg[0, kv] = part
        for g in range(grp):
            q8[pl.ds(kv * grp + g, rows, stride=heads), :] = part[:, g * head:(g + 1) * head].astype(F32)

    def send_queries(kv):
        pair = (remote(qg.at[0, kv], qg.at[1, kv], s_qs, s_qr.at[0, kv], right),
                remote(qg.at[0, kv], qg.at[2, kv], s_qs, s_qr.at[1, kv], left))
        start(pair)
        return pair

    c_hid.wait()
    queries(0)
    pl.semaphore_wait(barrier, 7)
    q_copies = [send_queries(0)]
    c_swap = [remote(src, raw.at[1, i], s_rawsend, s_rawrecv, partner) for i, src in enumerate((pk_h, pv_h))]
    start(c_swap)
    c_res = [pltpu.make_async_copy(hid_h.at[:, pl.ds(pl.multiple_of(ypos * blk + core * half, 128), half)], xres.at[core], s_res),
             remote(hid_h.at[:, pl.ds(pl.multiple_of(ypos * blk + (1 - core) * half, 128), half)], xres.at[core], s_ress, s_resr, partner)]
    start(c_res)
    queries(1)
    q_copies.append(send_queries(1))
    while queue:
        advance()
    pltpu.make_async_copy(raw.at[0], raw.at[0], s_raw).wait()
    deinterleave(0)

    remote(raw.at[1], raw.at[1], s_rawsend, s_rawrecv, partner).wait()
    deinterleave(1)
    start(ring_copies(0))

    n_pos = kpre.shape[1]

    n_pieces = n_pos // POS_CHUNK
    part_lanes = POS_CHUNK // 128

    def prefix_states(jobs):
        stacked, run, out = [None] * len(jobs), [None] * len(jobs), []

        def score(i, c):
            sources, kv = jobs[i]
            if c == 0:
                stacked[i] = jnp.concatenate([qg[slot, kv, pl.ds(chunk * part_rows, part_rows), pl.ds(g * head, head)]
                                              for slot, chunk in sources for g in range(grp)], axis=0)
            at = pl.ds(c * POS_CHUNK, POS_CHUNK)
            s = dot_nt(stacked[i], kpre[kv, at, :])
            scores[i % 2, :, at] = s
            for t in range(part_lanes):
                piece = s[:, t * 128:(t + 1) * 128]
                run[i] = piece if run[i] is None else jnp.maximum(run[i], piece)

        for c in range(n_pieces):
            score(0, c)
        for i, (sources, kv) in enumerate(jobs):
            row_max = jnp.max(run[i], axis=1, keepdims=True) * scale
            wide_max = jnp.broadcast_to(row_max, (2 * stack, 128))
            wide_max = jnp.concatenate([wide_max] * part_lanes, axis=1)
            total, num = None, None
            for c in range(n_pieces):
                if i + 1 < len(jobs):
                    score(i + 1, c)
                at = pl.ds(c * POS_CHUNK, POS_CHUNK)
                p = jnp.exp2(scores[i % 2, :, at] * scale - wide_max)
                for t in range(part_lanes):
                    piece = p[:, t * 128:(t + 1) * 128]
                    total = piece if total is None else total + piece
                term = dot_nn(p.astype(BF16), vpre[kv, at, :])
                num = term if num is None else num + term
            row_sum = jnp.sum(total, axis=1, keepdims=True)
            out += [(num[:stack], row_max[:stack], row_sum[:stack]), (num[stack:], row_max[stack:], row_sum[stack:])]
        return out

    def x_copies(i, where):
        return remote(xs.at[i], xr.at[i], s_xs, s_xr.at[i], where)

    def post(state, i, where):
        xs[i, :stack] = state[0]
        xs[i, stack:, :stack] = pack_stats(state[1], state[2])
        x_copies(i, where).start()

    def arrived(i):
        return (xr[i, :stack],) + unpack_stats(xr[i, stack:, :stack])

    def keep(refs, i, state):
        refs[0][i] = state[0]
        lane = lax.broadcasted_iota(jnp.int32, state[0].shape, 1)
        refs[1][i] = jnp.where(lane == 0, state[1], state[2])

    def kept(refs, i):
        return refs[0][i], refs[1][i][:, 0:1], refs[1][i][:, 1:2]

    own = (own_num, own_st)
    hold = (hold_num, hold_st)

    def prefix_near(chunk):
        base = 6 * chunk
        both = ((2, chunk), (1, chunk))
        right_1, left_1, right_0, left_0 = prefix_states([(both, 1), (both, 0)])
        post(right_1, base, right)
        post(left_0, base + 1, left)
        keep(hold, 2 * chunk + 1, left_1)
        keep(hold, 2 * chunk, right_0)

    def prefix_far():
        both = ((3, 0), (3, 1))
        states = prefix_states([(both, 0), (both, 1)])
        for chunk in range(2):
            post(states[chunk], 6 * chunk + 2, right)
            post(states[2 + chunk], 6 * chunk + 3, left)

    def prefix_own():
        both = ((0, 0), (0, 1))
        for i, state in enumerate(prefix_states([(both, 0), (both, 1)])):
            keep(own, i, state)

    def relay(chunk):
        base = 6 * chunk
        for i, where in ((base + 2, right), (base + 3, left)):
            x_copies(i, where).wait_recv()
        to_right, to_left = (merge(arrived(base + 2 + i), kept(hold, 2 * chunk + i)) for i in range(2))
        post(to_right, base + 4, right)
        post(to_left, base + 5, left)

    lines = GROUP * heads
    span = ring.shape[3]
    tile = span // 4

    def suffix_group(group):
        slot = group % RING
        lane = lax.broadcasted_iota(jnp.int32, (head, lines), 1)
        q_t = jnp.transpose(q8[pl.ds(group * lines, lines), :])
        for j in range(GROUP // 2):
            both = [jnp.where(lane // heads == 2 * j + e, q_t, 0.0) for e in range(2)]
            qbd[j] = jnp.concatenate(both, axis=0).astype(BF16)
        one = lax.broadcasted_iota(jnp.int32, (1, lines), 1)
        length = jnp.zeros((1, lines), jnp.int32)
        for b in range(GROUP):
            length = jnp.where(one // heads == b, lens[group * GROUP + b], length)
        line = lax.broadcasted_iota(jnp.int32, (tile, lines), 0)
        lane = lax.broadcasted_iota(jnp.int32, (tile, lines), 1)
        mine = lax.rem(line, kv_n) == lax.rem(lane, heads) // grp
        place = jnp.where(mine, line // kv_n, span)
        pltpu.make_async_copy(ring.at[slot], ring.at[slot], s_ring.at[slot]).wait()
        run = jnp.full((1, lines), LOW, F32)
        for c in range(4):
            at = pl.ds(c * tile, tile)
            s = None
            for j in range(GROUP // 2):
                keys = jnp.concatenate([ring[slot, 0, 2 * j, at, :], ring[slot, 0, 2 * j + 1, at, :]], axis=1)
                term = dot_nn(keys, qbd[j])
                s = term if s is None else s + term
            s = jnp.where(place < length - c * (tile // kv_n), s * scale, -jnp.inf)
            sufs[at, :] = s
            run = jnp.maximum(run, jnp.max(s, axis=0, keepdims=True))
        total = jnp.zeros((1, lines), F32)
        for c in range(4):
            p = jnp.exp2(sufs[pl.ds(c * tile, tile), :] - run)
            total = total + jnp.sum(p, axis=0, keepdims=True)
            sufp[:, pl.ds(c * tile, tile)] = jnp.transpose(p).astype(BF16)
        stats = jnp.concatenate([run, total, jnp.zeros((head - 2, lines), F32)], axis=0)
        sst8[pl.ds(group * lines, lines), :] = jnp.transpose(stats)
        for j in range(GROUP // 2):
            weights = sufp[pl.ds(2 * j * heads, 2 * heads), :]
            for e in range(2):
                o = dot_nn(weights, ring[slot, 1, 2 * j + e])
                so8[pl.ds(group * lines + (2 * j + e) * heads, heads), :] = o[e * heads:(e + 1) * heads]
        if group + RING < n_groups:
            start(ring_copies(group + RING))

    def merge_prefix(chunk):
        base = 6 * chunk
        for i, where in ((base + 1, left), (base + 4, right), (base, right), (base + 5, left)):
            x_copies(i, where).wait_recv()
        merged = [functools.reduce(merge, [kept(own, chunk), arrived(base + 1), arrived(base + 4)]),
                  functools.reduce(merge, [kept(own, 2 + chunk), arrived(base), arrived(base + 5)])]
        for kv in range(kv_n):
            keep(own, 2 * kv + chunk, merged[kv])

    def att_copy(chunk):
        first, n = chunks[chunk]
        ref = att.at[core, pl.ds(first, n), :]
        return remote(ref, ref, s_as, s_ar.at[chunk], partner)

    def combine(chunk):
        first, n = chunks[chunk]
        at_rows = pl.ds(first, n)
        which, off = first // part_rows, first % part_rows
        for kv in range(kv_n):
            rest = []
            for g in range(grp):
                every = pl.ds(first * heads + kv * grp + g, n, stride=heads)
                stats = sst8[every, :]
                pre_at = pl.ds(g * part_rows + off, n)
                pre = own_st[2 * kv + which, pre_at, :]
                rest.append((so8[every, :], stats[:, 0:1], stats[:, 1:2], q8[every, :],
                             own_num[2 * kv + which, pre_at, :], pre[:, 0:1], pre[:, 1:2]))
            num, top, tot, qs, pre_num, pre_top, pre_tot = (jnp.concatenate(list(v), axis=0) for v in zip(*rest))
            state = merge((pre_num, pre_top, pre_tot), (num, top, tot))
            kn = jnp.concatenate([knew[at_rows, pl.ds(kv * head, head)]] * grp, axis=0)
            vn = jnp.concatenate([vnew[at_rows, pl.ds(kv * head, head)]] * grp, axis=0)
            s_new = jnp.sum(qs * kn, axis=1, keepdims=True) * scale
            state = merge(state, (vn, s_new, jnp.ones_like(s_new)))
            res = (state[0] / state[2]).astype(BF16)
            for g in range(grp):
                att[core, at_rows, pl.ds((kv * grp + g) * head, head)] = res[g * n:(g + 1) * n]
        att_copy(chunk).start()

    def y_copy(chunk, i, where):
        at = pl.ds(0, chunks[chunk][1])
        return remote(ys.at[i, at], yr.at[i, at], s_ys, s_yr.at[i], where)

    def y_post(chunk, val, i, where, now=True):
        ys[i, :val.shape[0]] = val
        if now:
            y_copy(chunk, i, where).start()

    def y_near(chunk):
        y_copy(chunk, 6 * chunk + 2, up).start()
        y_copy(chunk, 6 * chunk + 3, down).start()

    def project(chunk):
        base = 6 * chunk
        first, n = chunks[chunk]
        att_copy(chunk).wait_recv()
        both = jnp.concatenate([att[c, pl.ds(first, n), :] for c in range(2)], axis=0)

        def y_part(r):
            if chunk == 0:
                c_wo[r].wait()
            val = dot_nn(both, wo[r])
            return val[:n], val[n:]

        one, two = y_part(n_y // 2)
        y_post(chunk, one, base, up)
        y_post(chunk, two, base + 1, down)
        one, two = y_part(1)
        y_post(chunk, two, base + 2, up, chunk == 0)
        yhold[chunk, 0, :n] = one
        one, two = y_part(n_y - 1)
        y_post(chunk, one, base + 3, down, chunk == 0)
        yhold[chunk, 1, :n] = two
        one, two = y_part(0)
        yhold[chunk, 2, :n] = one
        yhold[chunk, 3, :n] = two

    def y_relay(chunk):
        base = 6 * chunk
        n = chunks[chunk][1]
        y_copy(chunk, base, up).wait_recv()
        y_post(chunk, yhold[chunk, 0, :n] + yr[base, :n], base + 4, up)
        y_copy(chunk, base + 1, down).wait_recv()
        y_post(chunk, yhold[chunk, 1, :n] + yr[base + 1, :n], base + 5, down)

    def region(chunk, dest, which):
        first, n = chunks[chunk]
        return out_v.at[pl.ds(first, n), pl.ds(pl.multiple_of(dest * blk + which * half, 128), half)]

    def g_start(src, dst, sem, where):
        remote(src, dst, s_gs, sem, where).start()

    def g_wait(chunk, slot):
        ref = region(chunk, ypos, 0)
        remote(ref, ref, s_gs, s_gr.at[chunk, slot], up).wait_recv()

    def g_first(src, dst, chunk, slot, where):
        @pl.when(core == slot)
        def _():
            g_start(src, dst, s_gr.at[chunk, slot], where)

        @pl.when(core != slot)
        def _():
            g_start(src, dst, s_gl, where)

    def finish(chunk):
        base = 6 * chunk
        first, n = chunks[chunk]
        mine = region(chunk, ypos, core)
        done = []
        for c, (near, merged) in enumerate(((base + 3, base + 4), (base + 2, base + 5))):
            val = yhold[chunk, 2 + c, :n]
            for i in (near, merged):
                y_copy(chunk, i, up if i % 2 == 0 else down).wait_recv()
                val = val + yr[i, :n]
            val = (val + xres[c, pl.ds(first, n), :].astype(F32)).astype(BF16)
            yblk[chunk, c, :n] = val
            src = yblk.at[chunk, c, pl.ds(0, n)]
            if c == 0:
                g_first(src, mine, chunk, 0, up_cores[c])
                g_first(src, mine, chunk, 1, down_cores[c])
            else:
                g_first(src, mine, chunk, 1, down_cores[c])
                g_first(src, mine, chunk, 0, up_cores[c])
            done.append(val)
        col = pl.multiple_of(ypos * blk + core * half, 128)
        out_v[pl.ds(first, n), pl.ds(col, half)] = jnp.where(core == 0, done[0], done[1])
        g_start(yblk.at[chunk, 1 - core, pl.ds(0, n)], mine, s_gl, partner)

    def forward(chunk):
        g_wait(chunk, 0)
        ref = region(chunk, below, 0)
        g_start(ref, ref, s_gl, up)
        g_wait(chunk, 1)
        ref = region(chunk, above, 1)
        g_start(ref, ref, s_gl, down)

    prefix_own()
    q_copies[0][0].wait_recv()
    fwd_right = remote(qg.at[1, 0], qg.at[3, 0], s_qs, s_qr.at[2, 0], right)
    fwd_right.start()
    wait(c_wkv)
    start(ring_copies(1))
    for r in (n_y // 2, 1, n_y - 1, 0):
        c_wo[r].start()
    knew[...] = dot_nn(hid[...], wk[...]).astype(BF16).astype(F32)
    vnew[...] = dot_nn(hid[...], wv[...]).astype(BF16).astype(F32)
    q_copies[1][1].wait_recv()
    fwd_left = remote(qg.at[2, 1], qg.at[3, 1], s_qs, s_qr.at[2, 1], left)
    fwd_left.start()
    q_copies[1][0].wait_recv()
    q_copies[0][1].wait_recv()
    prefix_near(0)
    prefix_near(1)
    fwd_right.wait_recv()
    fwd_left.wait_recv()
    prefix_far()

    suffix_group(0)
    suffix_group(1)
    relay(0)
    relay(1)
    for group in range(2, n_groups):
        suffix_group(group)
    merge_prefix(0)
    combine(0)
    merge_prefix(1)
    combine(1)
    wait(c_res)
    project(0)
    combine(2)
    project(1)
    project(2)
    y_relay(0)
    y_near(1)
    y_near(2)
    y_relay(1)
    y_relay(2)
    finish(0)
    finish(1)
    finish(2)
    remote(qg.at[pl.ds(0, 3)], qg.at[pl.ds(0, 3)], s_qs, s_qr.at[0, 0], right).wait_send()
    remote(xs, xr, s_xs, s_xr.at[0], right).wait_send()
    remote(att.at[0], att.at[0], s_as, s_ar.at[0], partner).wait_send()
    y_all = pl.ds(0, 12)
    remote(ys.at[y_all], yr.at[y_all], s_ys, s_yr.at[0], up).wait_send()
    forward(0)
    forward(1)
    forward(2)
    remote(yr.at[pl.ds(0, 5)], yr.at[pl.ds(0, 5)], s_gs, s_gl, up).wait_recv()
    remote(ys.at[pl.ds(0, 7)], yr.at[pl.ds(0, 7)], s_gs, s_gl, up).wait_send()


def store(src, dst, sem):
    c = pltpu.make_async_copy(src, dst, sem)
    c.start()
    c.wait()


def solution(mesh):
    n_ctx, n_y = mesh.shape['ctx'], mesh.shape['heads']
    row_spec = P(('dp', 'ctx'), None)
    col_spec = P(None, 'heads')
    pre_spec = P(('dp', 'ctx'), 'heads', None)
    suf_spec = P(('dp', 'ctx'), None, 'heads', None)

    def local_step(hidden, w_query, w_key, w_value, w_out, prefix_k, prefix_v, suffix_k, suffix_v, seq_lens):
        rows, width = hidden.shape
        pos, kv_n, head = prefix_k.shape
        slots = suffix_k.shape[1]
        grp = w_query.shape[1] // (kv_n * head)
        heads = kv_n * grp
        blk = width // n_y
        half_rows = rows // 2
        stack = grp * half_rows
        lines = GROUP * heads
        dma = pltpu.SemaphoreType.DMA
        scratch = dict(
            hid=pltpu.VMEM((rows, width), BF16),
            wq=pltpu.VMEM((kv_n, width, grp * head), BF16),
            wk=pltpu.VMEM((width, kv_n * head), BF16),
            wv=pltpu.VMEM((width, kv_n * head), BF16),
            wo=pltpu.VMEM((n_y, heads * head, blk // 2), BF16),
            raw=pltpu.VMEM((2, 2, pos * kv_n, head), BF16),
            flat=pltpu.VMEM((pos * kv_n, head), F32),
            kpre=pltpu.VMEM((kv_n, 2 * pos, head), BF16),
            vpre=pltpu.VMEM((kv_n, 2 * pos, head), BF16),
            qg=pltpu.VMEM((4, kv_n, rows, grp * head), BF16),
            q8=pltpu.VMEM((rows * heads, head), F32),
            knew=pltpu.VMEM((rows, kv_n * head), F32),
            vnew=pltpu.VMEM((rows, kv_n * head), F32),
            ring=pltpu.VMEM((RING, 2, GROUP, slots * kv_n, head), BF16),
            qbd=pltpu.VMEM((GROUP // 2, 2 * head, lines), BF16),
            sufs=pltpu.VMEM((slots * kv_n, lines), F32),
            sufp=pltpu.VMEM((lines, slots * kv_n), BF16),
            scores=pltpu.VMEM((2, 2 * stack, 2 * pos), F32),
            own_num=pltpu.VMEM((2 * kv_n, stack, head), F32),
            own_st=pltpu.VMEM((2 * kv_n, stack, 128), F32),
            hold_num=pltpu.VMEM((4, stack, head), F32),
            hold_st=pltpu.VMEM((4, stack, 128), F32),
            xres=pltpu.VMEM((2, rows, blk // 2), BF16),
            so8=pltpu.VMEM((rows * heads, head), F32),
            sst8=pltpu.VMEM((rows * heads, head), F32),
            xs=pltpu.VMEM((12, stack + 8, head), F32),
            xr=pltpu.VMEM((12, stack + 8, head), F32),
            att=pltpu.VMEM((2, rows, heads * head), BF16),
            yhold=pltpu.VMEM((3, 4, half_rows, blk // 2), F32),
            ys=pltpu.VMEM((18, half_rows, blk // 2), F32),
            yr=pltpu.VMEM((18, half_rows, blk // 2), F32),
            yblk=pltpu.VMEM((3, 2, half_rows, blk // 2), BF16),
            s_hid=dma(()), s_wq=dma((IN_FLIGHT + 1,)), s_wkv=dma((2,)), s_wo=dma((n_y,)),
            s_raw=dma(()), s_rawsend=dma(()), s_rawrecv=dma(()), s_ring=dma((RING,)),
            s_res=dma(()), s_ress=dma(()), s_resr=dma(()), s_as=dma(()), s_ar=dma((3,)),
            s_qs=dma(()), s_qr=dma((3, kv_n)),
            s_xs=dma(()), s_xr=dma((12,)),
            s_ys=dma(()), s_yr=dma((18,)), s_gs=dma(()), s_gr=dma((3, 2)), s_gl=dma(()),
        )
        hbm = pl.BlockSpec(memory_space=pl.ANY)
        out = pl.pallas_call(
            functools.partial(kernel, (n_ctx, n_y, kv_n, grp)),
            out_shape=pltpu.VMEM((rows, width), BF16),
            in_specs=[hbm] * 9 + [pl.BlockSpec(memory_space=pltpu.SMEM)],
            out_specs=pl.BlockSpec(memory_space=pltpu.VMEM),
            scratch_shapes=list(scratch.values()),
            compiler_params=pltpu.CompilerParams(collective_id=0, has_side_effects=True, vmem_limit_bytes=VMEM_BYTES),
        )(hidden, w_query, w_key, w_value, w_out,
          prefix_k.reshape(pos * kv_n, head), prefix_v.reshape(pos * kv_n, head),
          suffix_k.reshape(rows, slots * kv_n, head), suffix_v.reshape(rows, slots * kv_n, head), seq_lens)
        return pl.pallas_call(
            store,
            out_shape=jax.ShapeDtypeStruct((rows, width), BF16),
            in_specs=[pl.BlockSpec(memory_space=pltpu.VMEM)],
            out_specs=hbm,
            scratch_shapes=[dma(())],
            compiler_params=pltpu.CompilerParams(vmem_limit_bytes=1048576),
        )(out)

    return jax.shard_map(local_step, mesh=mesh, in_specs=(row_spec, col_spec, col_spec, col_spec, P('heads', None), pre_spec, pre_spec, suf_spec, suf_spec, P(('dp', 'ctx'))), out_specs=row_spec, check_vma=False)
```

```python
import functools
import math
import jax
import jax.numpy as jnp
from jax import lax
from jax.experimental import pallas as pl
from jax.experimental.pallas import tpu as pltpu
from jax.sharding import PartitionSpec as P

MESH = pl.DeviceIdType.MESH
F32 = jnp.float32
BF16 = jnp.bfloat16
LOW = -3.0e38
GROUP = 16
RING = 2
POS_CHUNK = 512
PIECES = 2
SPLIT = 4
IN_FLIGHT = 2
VMEM_BYTES = 66000000


def dot_nt(a, b):
    return lax.dot_general(a, b, (((1,), (1,)), ((), ())), preferred_element_type=F32)


def dot_nn(a, b):
    return lax.dot_general(a, b, (((1,), (0,)), ((), ())), preferred_element_type=F32)


def pack_stats(row_max, row_sum):
    rows = row_max.shape[0]
    lane = lax.broadcasted_iota(jnp.int32, (rows, 128), 1)
    both = jnp.where(lane == 0, row_max, jnp.where(lane == 1, row_sum, 0.0))
    return jnp.transpose(both)[:8]


def unpack_stats(packed):
    rows = packed.shape[1]
    both = jnp.transpose(jnp.concatenate([packed, jnp.zeros((120, rows), F32)], axis=0))
    return both[:, 0:1], both[:, 1:2]


def merge(one, two):
    (num_a, max_a, sum_a), (num_b, max_b, sum_b) = one, two
    top = jnp.maximum(max_a, max_b)
    fac_a, fac_b = jnp.exp2(max_a - top), jnp.exp2(max_b - top)
    return num_a * fac_a + num_b * fac_b, top, sum_a * fac_a + sum_b * fac_b


def kernel(dims, hid_h, wq_h, wk_h, wv_h, wo_h, pk_h, pv_h, sk_h, sv_h, lens, out_v,
           hid, wq, wk, wv, wo, raw, flat, kpre, vpre, qg, q8, knew, vnew,
           ring, qbd, sufs, sufp, scores, own_num, own_st, hold_num, hold_st, xres,
           so8, sst8, xs, xr, att, yhold, ys, yr, yblk,
           s_hid, s_wq, s_wkv, s_wo, s_raw, s_rawsend, s_rawrecv, s_ring, s_res, s_ress, s_resr, s_as, s_ar,
           s_qs, s_qr, s_xs, s_xr, s_ys, s_yr, s_gs, s_gr, s_gl):
    n_ctx, n_y, kv_n, grp = dims
    rows = hid.shape[0]
    width = hid.shape[1]
    head = kpre.shape[-1]
    heads = kv_n * grp
    local_pos = raw.shape[2] // kv_n
    scale = head ** -0.5 * math.log2(math.e)
    blk = width // n_y
    half = blk // 2
    part_rows = rows // 2
    stack = grp * part_rows

    ctx = lax.axis_index('ctx')
    ypos = lax.axis_index('heads')
    right = {'ctx': lax.rem(ctx + 2, n_ctx)}
    left = {'ctx': lax.rem(ctx + n_ctx - 2, n_ctx)}
    core = lax.rem(ctx, 2)
    partner = {'ctx': ctx + 1 - 2 * core}
    below, above = lax.rem(ypos + n_y - 1, n_y), lax.rem(ypos + 1, n_y)
    up, down = {'heads': above}, {'heads': below}
    up_cores = [{'heads': above, 'ctx': ctx - core + c} for c in range(2)]
    down_cores = [{'heads': below, 'ctx': ctx - core + c} for c in range(2)]
    up_other = {'heads': above, 'ctx': ctx + 1 - 2 * core}
    down_other = {'heads': below, 'ctx': ctx + 1 - 2 * core}
    chunks = ((0, rows // 2), (rows // 2, rows // 4), (3 * rows // 4, rows // 4))

    def remote(src, dst, send, recv, where):
        return pltpu.make_async_remote_copy(src_ref=src, dst_ref=dst, send_sem=send, recv_sem=recv,
                                            device_id=where, device_id_type=MESH)

    c_hid = pltpu.make_async_copy(hid_h, hid, s_hid)
    c_raw = [pltpu.make_async_copy(src, raw.at[0, i], s_raw) for i, src in enumerate((pk_h, pv_h))]
    deep = width // PIECES
    fine = deep // SPLIT

    def wq_copies(kv, k):
        cols = pl.ds(kv * grp * head, grp * head)
        return [pltpu.make_async_copy(wq_h.at[pl.ds(k * deep + j * fine, fine), cols],
                                      wq.at[kv, pl.ds(k * deep + j * fine, fine), :], s_wq.at[kv, k]) for j in range(SPLIT)]

    c_wkv = [pltpu.make_async_copy(src, dst, s_wkv.at[i]) for i, (src, dst) in enumerate(((wk_h, wk), (wv_h, wv)))]
    c_wo = []
    for r in range(n_y):
        col = pl.multiple_of(lax.rem(ypos + r, n_y) * blk + core * half, 128)
        c_wo.append(pltpu.make_async_copy(wo_h.at[:, pl.ds(col, half)], wo.at[r], s_wo.at[r]))
    n_groups = rows // GROUP

    def ring_copies(group):
        seqs = pl.ds(group * GROUP, GROUP)
        slot = group % RING
        return [pltpu.make_async_copy(src.at[seqs], ring.at[slot, i], s_ring.at[slot]) for i, src in enumerate((sk_h, sv_h))]

    def start(copies):
        for c in copies:
            c.start()

    def wait(copies):
        for c in copies:
            c.wait()

    queue = [wq_copies(kv, k) for kv in range(kv_n) for k in range(PIECES)] + [c_raw] + [[c] for c in c_wkv]

    def advance():
        if queue:
            start(queue.pop(0))

    c_hid.start()
    for _ in range(IN_FLIGHT):
        advance()

    barrier = pltpu.get_barrier_semaphore()
    for where in (partner, left, right, up, down, up_other, down_other):
        pl.semaphore_signal(barrier, inc=1, device_id=where, device_id_type=MESH)

    def deinterleave(which):
        for i, dst in enumerate((kpre, vpre)):
            flat[...] = raw[which, i].astype(F32)
            for kv in range(kv_n):
                dst[kv, pl.ds(which * local_pos, local_pos), :] = flat[pl.ds(kv, local_pos, stride=kv_n), :].astype(BF16)

    def queries(kv):
        total = None
        for k in range(PIECES):
            at = pl.ds(k * deep, deep)
            pltpu.make_async_copy(wq.at[kv, at, :], wq.at[kv, at, :], s_wq.at[kv, k]).wait()
            advance()
            term = dot_nn(hid[:, at], wq[kv, at, :])
            total = term if total is None else total + term
        part = total.astype(BF16)
        qg[0, kv] = part
        for g in range(grp):
            q8[pl.ds(kv * grp + g, rows, stride=heads), :] = part[:, g * head:(g + 1) * head].astype(F32)

    def send_queries(kv):
        pair = (remote(qg.at[0, kv], qg.at[1, kv], s_qs, s_qr.at[0, kv], right),
                remote(qg.at[0, kv], qg.at[2, kv], s_qs, s_qr.at[1, kv], left))
        start(pair)
        return pair

    c_hid.wait()
    queries(0)
    pl.semaphore_wait(barrier, 7)
    q_copies = [send_queries(0)]
    c_swap = [remote(src, raw.at[1, i], s_rawsend, s_rawrecv, partner) for i, src in enumerate((pk_h, pv_h))]
    start(c_swap)
    c_res = [pltpu.make_async_copy(hid_h.at[:, pl.ds(pl.multiple_of(ypos * blk + core * half, 128), half)], xres.at[core], s_res),
             remote(hid_h.at[:, pl.ds(pl.multiple_of(ypos * blk + (1 - core) * half, 128), half)], xres.at[core], s_ress, s_resr, partner)]
    start(c_res)
    queries(1)
    q_copies.append(send_queries(1))
    while queue:
        advance()
    pltpu.make_async_copy(raw.at[0], raw.at[0], s_raw).wait()
    deinterleave(0)

    remote(raw.at[1], raw.at[1], s_rawsend, s_rawrecv, partner).wait()
    deinterleave(1)
    start(ring_copies(0))

    n_pos = kpre.shape[1]

    n_pieces = n_pos // POS_CHUNK
    part_lanes = POS_CHUNK // 128

    def prefix_states(jobs):
        stacked, run, out = [None] * len(jobs), [None] * len(jobs), []

        def score(i, c):
            sources, kv = jobs[i]
            if c == 0:
                stacked[i] = jnp.concatenate([qg[slot, kv, pl.ds(chunk * part_rows, part_rows), pl.ds(g * head, head)]
                                              for slot, chunk in sources for g in range(grp)], axis=0)
            at = pl.ds(c * POS_CHUNK, POS_CHUNK)
            s = dot_nt(stacked[i], kpre[kv, at, :])
            scores[i % 2, :, at] = s
            for t in range(part_lanes):
                piece = s[:, t * 128:(t + 1) * 128]
                run[i] = piece if run[i] is None else jnp.maximum(run[i], piece)

        for c in range(n_pieces):
            score(0, c)
        for i, (sources, kv) in enumerate(jobs):
            row_max = jnp.max(run[i], axis=1, keepdims=True) * scale
            wide_max = jnp.broadcast_to(row_max, (2 * stack, 128))
            wide_max = jnp.concatenate([wide_max] * part_lanes, axis=1)
            total, num = None, None
            for c in range(n_pieces):
                if i + 1 < len(jobs):
                    score(i + 1, c)
                at = pl.ds(c * POS_CHUNK, POS_CHUNK)
                p = jnp.exp2(scores[i % 2, :, at] * scale - wide_max)
                for t in range(part_lanes):
                    piece = p[:, t * 128:(t + 1) * 128]
                    total = piece if total is None else total + piece
                term = dot_nn(p.astype(BF16), vpre[kv, at, :])
                num = term if num is None else num + term
            row_sum = jnp.sum(total, axis=1, keepdims=True)
            out += [(num[:stack], row_max[:stack], row_sum[:stack]), (num[stack:], row_max[stack:], row_sum[stack:])]
        return out

    def x_copies(i, where):
        return remote(xs.at[i], xr.at[i], s_xs, s_xr.at[i], where)

    def post(state, i, where):
        xs[i, :stack] = state[0]
        xs[i, stack:, :stack] = pack_stats(state[1], state[2])
        x_copies(i, where).start()

    def arrived(i):
        return (xr[i, :stack],) + unpack_stats(xr[i, stack:, :stack])

    def keep(refs, i, state):
        refs[0][i] = state[0]
        lane = lax.broadcasted_iota(jnp.int32, state[0].shape, 1)
        refs[1][i] = jnp.where(lane == 0, state[1], state[2])

    def kept(refs, i):
        return refs[0][i], refs[1][i][:, 0:1], refs[1][i][:, 1:2]

    own = (own_num, own_st)
    hold = (hold_num, hold_st)

    def prefix_near(chunk):
        base = 6 * chunk
        both = ((2, chunk), (1, chunk))
        right_1, left_1, right_0, left_0 = prefix_states([(both, 1), (both, 0)])
        post(right_1, base, right)
        post(left_0, base + 1, left)
        keep(hold, 2 * chunk + 1, left_1)
        keep(hold, 2 * chunk, right_0)

    def prefix_far():
        both = ((3, 0), (3, 1))
        states = prefix_states([(both, 0), (both, 1)])
        for chunk in range(2):
            post(states[chunk], 6 * chunk + 2, right)
            post(states[2 + chunk], 6 * chunk + 3, left)

    def prefix_own():
        both = ((0, 0), (0, 1))
        for i, state in enumerate(prefix_states([(both, 0), (both, 1)])):
            keep(own, i, state)

    def relay():
        for base in (0, 6):
            for i, where in ((base + 2, right), (base + 3, left)):
                x_copies(i, where).wait_recv()
        ready = [merge(arrived(6 * (n // 2) + 2 + n % 2), kept(hold, n)) for n in range(4)]
        for n in range(4):
            post(ready[n], 6 * (n // 2) + 4 + n % 2, (right, left)[n % 2])

    lines = GROUP * heads
    span = ring.shape[3]
    tile = span // 4

    def suffix_group(group):
        slot = group % RING
        lane = lax.broadcasted_iota(jnp.int32, (head, lines), 1)
        q_t = jnp.transpose(q8[pl.ds(group * lines, lines), :])
        for j in range(GROUP // 2):
            both = [jnp.where(lane // heads == 2 * j + e, q_t, 0.0) for e in range(2)]
            qbd[j] = jnp.concatenate(both, axis=0).astype(BF16)
        one = lax.broadcasted_iota(jnp.int32, (1, lines), 1)
        length = jnp.zeros((1, lines), jnp.int32)
        for b in range(GROUP):
            length = jnp.where(one // heads == b, lens[group * GROUP + b], length)
        line = lax.broadcasted_iota(jnp.int32, (tile, lines), 0)
        lane = lax.broadcasted_iota(jnp.int32, (tile, lines), 1)
        mine = lax.rem(line, kv_n) == lax.rem(lane, heads) // grp
        place = jnp.where(mine, line // kv_n, span)
        pltpu.make_async_copy(ring.at[slot], ring.at[slot], s_ring.at[slot]).wait()
        run = jnp.full((1, lines), LOW, F32)
        for c in range(4):
            at = pl.ds(c * tile, tile)
            s = None
            for j in range(GROUP // 2):
                keys = jnp.concatenate([ring[slot, 0, 2 * j, at, :], ring[slot, 0, 2 * j + 1, at, :]], axis=1)
                term = dot_nn(keys, qbd[j])
                s = term if s is None else s + term
            s = jnp.where(place < length - c * (tile // kv_n), s * scale, -jnp.inf)
            sufs[at, :] = s
            run = jnp.maximum(run, jnp.max(s, axis=0, keepdims=True))
        total = jnp.zeros((1, lines), F32)
        for c in range(4):
            p = jnp.exp2(sufs[pl.ds(c * tile, tile), :] - run)
            total = total + jnp.sum(p, axis=0, keepdims=True)
            sufp[:, pl.ds(c * tile, tile)] = jnp.transpose(p).astype(BF16)
        stats = jnp.concatenate([run, total, jnp.zeros((head - 2, lines), F32)], axis=0)
        sst8[pl.ds(group * lines, lines), :] = jnp.transpose(stats)
        for j in range(GROUP // 2):
            weights = sufp[pl.ds(2 * j * heads, 2 * heads), :]
            for e in range(2):
                o = dot_nn(weights, ring[slot, 1, 2 * j + e])
                so8[pl.ds(group * lines + (2 * j + e) * heads, heads), :] = o[e * heads:(e + 1) * heads]
        if group + RING < n_groups:
            start(ring_copies(group + RING))

    def merge_prefix(chunk):
        base = 6 * chunk
        for i, where in ((base + 1, left), (base + 4, right), (base, right), (base + 5, left)):
            x_copies(i, where).wait_recv()
        merged = [functools.reduce(merge, [kept(own, chunk), arrived(base + 1), arrived(base + 4)]),
                  functools.reduce(merge, [kept(own, 2 + chunk), arrived(base), arrived(base + 5)])]
        for kv in range(kv_n):
            keep(own, 2 * kv + chunk, merged[kv])

    def att_copy(chunk):
        first, n = chunks[chunk]
        ref = att.at[core, pl.ds(first, n), :]
        return remote(ref, ref, s_as, s_ar.at[chunk], partner)

    def combine(chunk):
        first, n = chunks[chunk]
        at_rows = pl.ds(first, n)
        which, off = first // part_rows, first % part_rows
        for kv in range(kv_n):
            rest = []
            for g in range(grp):
                every = pl.ds(first * heads + kv * grp + g, n, stride=heads)
                stats = sst8[every, :]
                pre_at = pl.ds(g * part_rows + off, n)
                pre = own_st[2 * kv + which, pre_at, :]
                rest.append((so8[every, :], stats[:, 0:1], stats[:, 1:2], q8[every, :],
                             own_num[2 * kv + which, pre_at, :], pre[:, 0:1], pre[:, 1:2]))
            num, top, tot, qs, pre_num, pre_top, pre_tot = (jnp.concatenate(list(v), axis=0) for v in zip(*rest))
            state = merge((pre_num, pre_top, pre_tot), (num, top, tot))
            kn = jnp.concatenate([knew[at_rows, pl.ds(kv * head, head)]] * grp, axis=0)
            vn = jnp.concatenate([vnew[at_rows, pl.ds(kv * head, head)]] * grp, axis=0)
            s_new = jnp.sum(qs * kn, axis=1, keepdims=True) * scale
            state = merge(state, (vn, s_new, jnp.ones_like(s_new)))
            res = (state[0] / state[2]).astype(BF16)
            for g in range(grp):
                att[core, at_rows, pl.ds((kv * grp + g) * head, head)] = res[g * n:(g + 1) * n]
        att_copy(chunk).start()

    def y_copy(chunk, i, where):
        at = pl.ds(0, chunks[chunk][1])
        return remote(ys.at[i, at], yr.at[i, at], s_ys, s_yr.at[i], where)

    def y_post(chunk, val, i, where, now=True):
        ys[i, :val.shape[0]] = val
        if now:
            y_copy(chunk, i, where).start()

    def y_near(chunk):
        y_copy(chunk, 6 * chunk + 2, up).start()
        y_copy(chunk, 6 * chunk + 3, down).start()

    def project(chunk):
        base = 6 * chunk
        first, n = chunks[chunk]
        att_copy(chunk).wait_recv()
        both = jnp.concatenate([att[c, pl.ds(first, n), :] for c in range(2)], axis=0)

        def y_part(r):
            if chunk == 0:
                c_wo[r].wait()
            val = dot_nn(both, wo[r])
            return val[:n], val[n:]

        one, two = y_part(n_y // 2)
        y_post(chunk, one, base, up)
        y_post(chunk, two, base + 1, down)
        one, two = y_part(1)
        y_post(chunk, two, base + 2, up, chunk == 0)
        yhold[chunk, 0, :n] = one
        one, two = y_part(n_y - 1)
        y_post(chunk, one, base + 3, down, chunk == 0)
        yhold[chunk, 1, :n] = two
        one, two = y_part(0)
        yhold[chunk, 2, :n] = one
        yhold[chunk, 3, :n] = two

    def y_relay(chunk):
        base = 6 * chunk
        n = chunks[chunk][1]
        y_copy(chunk, base, up).wait_recv()
        y_post(chunk, yhold[chunk, 0, :n] + yr[base, :n], base + 4, up)
        y_copy(chunk, base + 1, down).wait_recv()
        y_post(chunk, yhold[chunk, 1, :n] + yr[base + 1, :n], base + 5, down)

    def region(chunk, dest, which):
        first, n = chunks[chunk]
        return out_v.at[pl.ds(first, n), pl.ds(pl.multiple_of(dest * blk + which * half, 128), half)]

    def g_start(src, dst, sem, where):
        remote(src, dst, s_gs, sem, where).start()

    def g_wait(chunk, slot):
        ref = region(chunk, ypos, 0)
        remote(ref, ref, s_gs, s_gr.at[chunk, slot], up).wait_recv()

    def g_first(src, dst, chunk, slot, where):
        @pl.when(core == slot)
        def _():
            g_start(src, dst, s_gr.at[chunk, slot], where)

        @pl.when(core != slot)
        def _():
            g_start(src, dst, s_gl, where)

    def finish(chunk):
        base = 6 * chunk
        first, n = chunks[chunk]
        mine = region(chunk, ypos, core)
        done = []
        for c, (near, merged) in enumerate(((base + 3, base + 4), (base + 2, base + 5))):
            val = yhold[chunk, 2 + c, :n]
            for i in (near, merged):
                y_copy(chunk, i, up if i % 2 == 0 else down).wait_recv()
                val = val + yr[i, :n]
            val = (val + xres[c, pl.ds(first, n), :].astype(F32)).astype(BF16)
            yblk[chunk, c, :n] = val
            src = yblk.at[chunk, c, pl.ds(0, n)]
            if c == 0:
                g_first(src, mine, chunk, 0, up_cores[c])
                g_first(src, mine, chunk, 1, down_cores[c])
            else:
                g_first(src, mine, chunk, 1, down_cores[c])
                g_first(src, mine, chunk, 0, up_cores[c])
            done.append(val)
        col = pl.multiple_of(ypos * blk + core * half, 128)
        out_v[pl.ds(first, n), pl.ds(col, half)] = jnp.where(core == 0, done[0], done[1])
        g_start(yblk.at[chunk, 1 - core, pl.ds(0, n)], mine, s_gl, partner)

    def forward(chunk):
        g_wait(chunk, 0)
        ref = region(chunk, below, 0)
        g_start(ref, ref, s_gl, up)
        g_wait(chunk, 1)
        ref = region(chunk, above, 1)
        g_start(ref, ref, s_gl, down)

    prefix_own()
    q_copies[0][0].wait_recv()
    fwd_right = remote(qg.at[1, 0], qg.at[3, 0], s_qs, s_qr.at[2, 0], right)
    fwd_right.start()
    wait(c_wkv)
    start(ring_copies(1))
    for r in (n_y // 2, 1, n_y - 1, 0):
        c_wo[r].start()
    knew[...] = dot_nn(hid[...], wk[...]).astype(BF16).astype(F32)
    vnew[...] = dot_nn(hid[...], wv[...]).astype(BF16).astype(F32)
    q_copies[1][1].wait_recv()
    fwd_left = remote(qg.at[2, 1], qg.at[3, 1], s_qs, s_qr.at[2, 1], left)
    fwd_left.start()
    q_copies[1][0].wait_recv()
    q_copies[0][1].wait_recv()
    prefix_near(0)
    prefix_near(1)
    fwd_right.wait_recv()
    fwd_left.wait_recv()
    prefix_far()

    suffix_group(0)
    suffix_group(1)
    relay()
    for group in range(2, n_groups):
        suffix_group(group)
    merge_prefix(0)
    combine(0)
    merge_prefix(1)
    combine(1)
    wait(c_res)
    project(0)
    combine(2)
    project(1)
    project(2)
    y_relay(0)
    y_near(1)
    y_near(2)
    y_relay(1)
    y_relay(2)
    finish(0)
    finish(1)
    finish(2)
    remote(qg.at[pl.ds(0, 3)], qg.at[pl.ds(0, 3)], s_qs, s_qr.at[0, 0], right).wait_send()
    remote(xs, xr, s_xs, s_xr.at[0], right).wait_send()
    remote(att.at[0], att.at[0], s_as, s_ar.at[0], partner).wait_send()
    y_all = pl.ds(0, 12)
    remote(ys.at[y_all], yr.at[y_all], s_ys, s_yr.at[0], up).wait_send()
    forward(0)
    forward(1)
    forward(2)
    remote(yr.at[pl.ds(0, 5)], yr.at[pl.ds(0, 5)], s_gs, s_gl, up).wait_recv()
    remote(ys.at[pl.ds(0, 7)], yr.at[pl.ds(0, 7)], s_gs, s_gl, up).wait_send()


def store(src, dst, sem):
    c = pltpu.make_async_copy(src, dst, sem)
    c.start()
    c.wait()


def solution(mesh):
    n_ctx, n_y = mesh.shape['ctx'], mesh.shape['heads']
    row_spec = P(('dp', 'ctx'), None)
    col_spec = P(None, 'heads')
    pre_spec = P(('dp', 'ctx'), 'heads', None)
    suf_spec = P(('dp', 'ctx'), None, 'heads', None)

    def local_step(hidden, w_query, w_key, w_value, w_out, prefix_k, prefix_v, suffix_k, suffix_v, seq_lens):
        rows, width = hidden.shape
        pos, kv_n, head = prefix_k.shape
        slots = suffix_k.shape[1]
        grp = w_query.shape[1] // (kv_n * head)
        heads = kv_n * grp
        blk = width // n_y
        half_rows = rows // 2
        stack = grp * half_rows
        lines = GROUP * heads
        dma = pltpu.SemaphoreType.DMA
        scratch = dict(
            hid=pltpu.VMEM((rows, width), BF16),
            wq=pltpu.VMEM((kv_n, width, grp * head), BF16),
            wk=pltpu.VMEM((width, kv_n * head), BF16),
            wv=pltpu.VMEM((width, kv_n * head), BF16),
            wo=pltpu.VMEM((n_y, heads * head, blk // 2), BF16),
            raw=pltpu.VMEM((2, 2, pos * kv_n, head), BF16),
            flat=pltpu.VMEM((pos * kv_n, head), F32),
            kpre=pltpu.VMEM((kv_n, 2 * pos, head), BF16),
            vpre=pltpu.VMEM((kv_n, 2 * pos, head), BF16),
            qg=pltpu.VMEM((4, kv_n, rows, grp * head), BF16),
            q8=pltpu.VMEM((rows * heads, head), F32),
            knew=pltpu.VMEM((rows, kv_n * head), F32),
            vnew=pltpu.VMEM((rows, kv_n * head), F32),
            ring=pltpu.VMEM((RING, 2, GROUP, slots * kv_n, head), BF16),
            qbd=pltpu.VMEM((GROUP // 2, 2 * head, lines), BF16),
            sufs=pltpu.VMEM((slots * kv_n, lines), F32),
            sufp=pltpu.VMEM((lines, slots * kv_n), BF16),
            scores=pltpu.VMEM((2, 2 * stack, 2 * pos), F32),
            own_num=pltpu.VMEM((2 * kv_n, stack, head), F32),
            own_st=pltpu.VMEM((2 * kv_n, stack, 128), F32),
            hold_num=pltpu.VMEM((4, stack, head), F32),
            hold_st=pltpu.VMEM((4, stack, 128), F32),
            xres=pltpu.VMEM((2, rows, blk // 2), BF16),
            so8=pltpu.VMEM((rows * heads, head), F32),
            sst8=pltpu.VMEM((rows * heads, head), F32),
            xs=pltpu.VMEM((12, stack + 8, head), F32),
            xr=pltpu.VMEM((12, stack + 8, head), F32),
            att=pltpu.VMEM((2, rows, heads * head), BF16),
            yhold=pltpu.VMEM((3, 4, half_rows, blk // 2), F32),
            ys=pltpu.VMEM((18, half_rows, blk // 2), F32),
            yr=pltpu.VMEM((18, half_rows, blk // 2), F32),
            yblk=pltpu.VMEM((3, 2, half_rows, blk // 2), BF16),
            s_hid=dma(()), s_wq=dma((kv_n, PIECES)), s_wkv=dma((2,)), s_wo=dma((n_y,)),
            s_raw=dma(()), s_rawsend=dma(()), s_rawrecv=dma(()), s_ring=dma((RING,)),
            s_res=dma(()), s_ress=dma(()), s_resr=dma(()), s_as=dma(()), s_ar=dma((3,)),
            s_qs=dma(()), s_qr=dma((3, kv_n)),
            s_xs=dma(()), s_xr=dma((12,)),
            s_ys=dma(()), s_yr=dma((18,)), s_gs=dma(()), s_gr=dma((3, 2)), s_gl=dma(()),
        )
        hbm = pl.BlockSpec(memory_space=pl.ANY)
        out = pl.pallas_call(
            functools.partial(kernel, (n_ctx, n_y, kv_n, grp)),
            out_shape=pltpu.VMEM((rows, width), BF16),
            in_specs=[hbm] * 9 + [pl.BlockSpec(memory_space=pltpu.SMEM)],
            out_specs=pl.BlockSpec(memory_space=pltpu.VMEM),
            scratch_shapes=list(scratch.values()),
            compiler_params=pltpu.CompilerParams(collective_id=0, has_side_effects=True, vmem_limit_bytes=VMEM_BYTES),
        )(hidden, w_query, w_key, w_value, w_out,
          prefix_k.reshape(pos * kv_n, head), prefix_v.reshape(pos * kv_n, head),
          suffix_k.reshape(rows, slots * kv_n, head), suffix_v.reshape(rows, slots * kv_n, head), seq_lens)
        return pl.pallas_call(
            store,
            out_shape=jax.ShapeDtypeStruct((rows, width), BF16),
            in_specs=[pl.BlockSpec(memory_space=pltpu.VMEM)],
            out_specs=hbm,
            scratch_shapes=[dma(())],
            compiler_params=pltpu.CompilerParams(vmem_limit_bytes=1048576),
        )(out)

    return jax.shard_map(local_step, mesh=mesh, in_specs=(row_spec, col_spec, col_spec, col_spec, P('heads', None), pre_spec, pre_spec, suf_spec, suf_spec, P(('dp', 'ctx'))), out_specs=row_spec, check_vma=False)
```
